128 devices in a mesh: inst: 8 (over y_hi, x), head: 16 (over y_lo, z, core).
Axes of the slice: x: 4, y: 4 (y_hi: 2, y_lo: 2; y = y_hi * 2 + y_lo), z: 4, core: 2. Of those that a mesh axis runs over, the one named last changes fastest.
Arguments:
- old_keys: bfloat16 [1024, 16, 64, 128], P('inst', 'head'), may hold values from -6 to 6
- old_values: bfloat16 [1024, 16, 64, 128], P('inst', 'head'), may hold values from -6 to 6
- old_block: int32 [1024], P('inst'), may hold values from -1 to 255, as said below
- new_slot: int32 [256], replicated, may hold values from 0 to 255, as said below
- lengths: int32 [64], replicated, may hold values from 1 to 16384, as said below
- queries: bfloat16 [64, 16, 8192], P(None, None, 'head'), may hold values from -240 to 240
- draft_keys: bfloat16 [64, 16, 1024], P('inst'), may hold values from -6 to 6
- draft_values: bfloat16 [64, 16, 1024], P('inst'), may hold values from -6 to 6
Outputs:
- moved_keys: bfloat16 [256, 16, 64, 128], P('inst', 'head')
- moved_values: bfloat16 [256, 16, 64, 128], P('inst', 'head')
- attended: bfloat16 [64, 16, 8192], P(None, None, 'head')
The draws below stay inside these ranges and needn't reach their ends.
Inputs may be any that keep to these rules, and one draw needn't show every extreme that they name: ceil(lengths / 128) summed over the requests is exactly 256; the longest request has exactly 16384 tokens. `old_block`: every block 0 to 255 stands in exactly one old slot; the blocks fill all slots of 2 instances and all other slots hold -1. A permutation; block g goes to instance new_slot[g] // 32. At most 32 blocks go from one old instance to one new one, and in every draw some new instance receives all its 32 blocks from a single old instance.
All inputs are finite; a program needn't handle non-finite values.
Results may differ from the reference program's by a relative error of at most 0.004.
Values may be sent and summed in bfloat16 or wider, within the bound.
No kernel may reach another device: no remote copies, remote signals or barrier semaphores. Data moves between devices by JAX's collectives and lax.ppermute only.
A program may use at most 64 MiB of HBM per device.

```python
import math
import jax
import jax.numpy as jnp
from jax import lax

KVH = 8
HD = 128
GROUP = 8
BLK = 128
REQ = 64
DRAFT = 16
BLOCKS_PER_RANK = 32
QH = 64
HALF = 64
OLD_INST = 2
SLOTS = 128
TOTAL_BLOCKS = 256
MAX_BLOCKS = 128
N_INST = 8


def build_tables(key):
    base = jax.random.fold_in(key, 11)
    key_old, key_shuffle, foreign_key_rows, key_owners = jax.random.split(base, 4)
    chosen = jnp.sort(jax.random.permutation(key_old, N_INST)[:OLD_INST]).astype(jnp.int32)
    shuffle = jax.random.permutation(key_shuffle, TOTAL_BLOCKS).astype(jnp.int32)
    places = jnp.arange(TOTAL_BLOCKS, dtype=jnp.int32)
    old_position = chosen[places // SLOTS] * SLOTS + places % SLOTS
    old_table = jnp.full((N_INST * SLOTS,), -1, jnp.int32).at[old_position].set(shuffle)
    peer_replicas = (BLOCKS_PER_RANK + jax.random.permutation(foreign_key_rows, TOTAL_BLOCKS - BLOCKS_PER_RANK)).astype(jnp.int32)
    token_position = jnp.concatenate([jnp.arange(BLOCKS_PER_RANK, dtype=jnp.int32), peer_replicas])
    block_owner_list = jax.random.permutation(key_owners, N_INST).astype(jnp.int32)
    destination_replica = block_owner_list[token_position // BLOCKS_PER_RANK] * BLOCKS_PER_RANK + token_position % BLOCKS_PER_RANK
    new_table = jnp.zeros((TOTAL_BLOCKS,), jnp.int32).at[shuffle].set(destination_replica)
    return (old_table, new_table)


def draw_old_block(key, part):
    return build_tables(key)[0]


def draw_new_slot(key, part):
    return build_tables(key)[1]


def draw_lengths(key, part):
    base = jax.random.fold_in(key, 23)
    key_long, key_weight, key_fill = jax.random.split(base, 3)
    longest = jax.random.randint(key_long, (), 0, REQ)
    request_ids = jnp.arange(REQ, dtype=jnp.int32)
    peer_replicas = request_ids != longest
    weights = jnp.where(peer_replicas, jax.random.randint(key_weight, (REQ,), 1, 5), 0).astype(jnp.int32)
    weight_sum = jnp.sum(weights)
    excess = TOTAL_BLOCKS - MAX_BLOCKS - (REQ - 1)
    shares = excess * weights // weight_sum
    leftover = excess - jnp.sum(shares)
    ranking = jnp.cumsum(peer_replicas.astype(jnp.int32)) - 1
    counts = jnp.where(peer_replicas, 1 + shares + (ranking < leftover).astype(jnp.int32), MAX_BLOCKS)
    filling = jnp.where(peer_replicas, jax.random.randint(key_fill, (REQ,), 1, BLK + 1), BLK)
    return ((counts - 1) * BLK + filling).astype(jnp.int32)


def draw_queries(key, part):
    base = jax.random.fold_in(key, 37)
    key_value, key_scale = jax.random.split(base)
    entries_drawn = jax.random.normal(key_value, (REQ, DRAFT, QH, HD), jnp.float32)
    scales = jnp.exp(jax.random.uniform(key_scale, (REQ, 1, QH, 1), jnp.float32, math.log(1.0), math.log(6.0)))
    return jnp.clip(entries_drawn * scales, -240.0, 240.0).reshape(REQ, DRAFT, QH * HD).astype(jnp.bfloat16)


def block_levels(rng, dims, cuts, least, largest):
    level = 1.0
    for axis_at, blocks in cuts:
        heights = jax.random.uniform(jax.random.fold_in(jax.random.fold_in(rng, 6), axis_at), (blocks,), jnp.float32, least / len(cuts), largest / len(cuts))
        level = level * jnp.repeat(jnp.exp(heights), dims[axis_at] // blocks).reshape((-1,) + (1,) * (len(dims) - 1 - axis_at))
    return level


def noise(own_key, dims, spread, most, cuts=(), kind=jnp.bfloat16):
    entries = spread * jax.random.normal(own_key, dims, jnp.float32)
    if cuts:
        entries = entries * block_levels(own_key, dims, cuts, -0.22, 0.18)
    return jnp.clip(entries, -most, most).astype(kind)


def setup_inputs(seed: int = 0) -> dict:
    streams_of = jax.random.split(jax.random.key(seed), 9)
    old_keys = noise(streams_of[0], (N_INST * SLOTS, 2 * KVH, HALF, HD), 1.0, 6.0, ((0, 8), (1, 16)))
    old_values = noise(streams_of[1], (N_INST * SLOTS, 2 * KVH, HALF, HD), 1.0, 6.0, ((0, 8), (1, 16)))
    old_block = draw_old_block(jax.random.fold_in(streams_of[8], 71), 0)
    new_slot = draw_new_slot(jax.random.fold_in(streams_of[8], 71), 0)
    lengths = draw_lengths(jax.random.fold_in(streams_of[8], 71), 0)
    queries = draw_queries(jax.random.fold_in(streams_of[8], 71), 0)
    draft_keys = noise(streams_of[6], (REQ, DRAFT, KVH * HD), 1.0, 6.0, ((0, 8),))
    draft_values = noise(streams_of[7], (REQ, DRAFT, KVH * HD), 1.0, 6.0, ((0, 8),))
    return {"old_keys": old_keys, "old_values": old_values, "old_block": old_block, "new_slot": new_slot, "lengths": lengths, "queries": queries, "draft_keys": draft_keys, "draft_values": draft_values}


masked = -1e+30

def reference(old_keys, old_values, old_block, new_slot, lengths, queries, draft_keys, draft_values):
    slot_count = old_keys.shape[0]
    block_capacity = new_slot.shape[0]
    block_ids = jnp.arange(block_capacity, dtype=jnp.int32)
    holder = jnp.zeros((block_capacity,), jnp.int32).at[jnp.where(old_block >= 0, old_block, block_capacity)].set(jnp.arange(slot_count, dtype=jnp.int32), mode='drop')
    locally_present = jnp.zeros((block_capacity,), jnp.int32).at[new_slot].set(block_ids)
    source = holder[locally_present]
    moved_keys = old_keys[source]
    moved_values = old_values[source]
    inv_root = 1.0 / math.sqrt(HD)
    counts = (lengths + BLK - 1) // BLK
    starts = jnp.cumsum(counts) - counts
    block_owner_list = (lax.optimization_barrier(jnp.sum((starts[None, :] <= locally_present[:, None]).astype(jnp.int32), axis=1)) - 1).astype(jnp.int32)
    offset = locally_present - starts[block_owner_list]
    positions = offset[:, None] * BLK + jnp.arange(BLK, dtype=jnp.int32)[None, :]
    usable = positions < lengths[block_owner_list][:, None]
    qcount = DRAFT * GROUP
    split_q = queries.reshape(REQ, DRAFT, KVH, GROUP, HD)
    grouped = split_q.transpose(0, 2, 1, 3, 4).reshape(REQ, KVH, qcount, HD)
    dkeys = draft_keys.reshape(REQ, DRAFT, KVH, HD).astype(jnp.float32)
    dvals = draft_values.reshape(REQ, DRAFT, KVH, HD).astype(jnp.float32)
    dscore = jnp.einsum('rikgd,rjkd->rkigj', split_q.astype(jnp.float32), dkeys) * inv_root
    causal = jnp.arange(DRAFT)[None, :] <= jnp.arange(DRAFT)[:, None]
    causal_flat = jnp.broadcast_to(causal[:, None, :], (DRAFT, GROUP, DRAFT)).reshape(qcount, DRAFT)
    dscore = jnp.where(causal_flat, dscore.reshape(REQ, KVH, qcount, DRAFT), masked)
    stride = math.gcd(block_capacity, 64)
    nsteps = block_capacity // stride
    key_blocks = moved_keys.reshape(nsteps, stride, KVH, BLK, HD)
    value_blocks = moved_values.reshape(nsteps, stride, KVH, BLK, HD)
    owner_blocks = block_owner_list.reshape(nsteps, stride)
    usable_blocks = usable.reshape(nsteps, stride, BLK)
    request_ids = jnp.arange(REQ, dtype=jnp.int32)

    def scores_of(key_rows, rows_owner, rows_usable):
        picked = grouped[rows_owner].astype(jnp.float32)
        scores = jnp.einsum('skqd,sktd->skqt', picked, key_rows.astype(jnp.float32)) * inv_root
        return jnp.where(rows_usable[:, None, None, :], scores, masked)

    def first_pass(peaks, pieces):
        key_rows, rows_owner, rows_usable = pieces
        scores = scores_of(key_rows, rows_owner, rows_usable)
        belongs = rows_owner[:, None] == request_ids[None, :]
        slot_peaks = lax.optimization_barrier(jnp.max(scores, axis=-1))
        block_peak = lax.optimization_barrier(jnp.max(jnp.where(belongs[:, :, None, None], slot_peaks[:, None], masked), axis=0))
        return (jnp.maximum(peaks, block_peak), None)
    peaks = lax.scan(first_pass, lax.optimization_barrier(jnp.max(dscore, axis=-1)), (key_blocks, owner_blocks, usable_blocks))[0]

    def second_pass(state_now, pieces):
        totals, weighted = state_now
        key_rows, value_rows, rows_owner, rows_usable = pieces
        scores = scores_of(key_rows, rows_owner, rows_usable)
        weights = jnp.where(rows_usable[:, None, None, :], jnp.exp(scores - peaks[rows_owner][..., None]), 0.0)
        belongs = (rows_owner[:, None] == request_ids[None, :]).astype(jnp.float32)
        totals = totals + jnp.einsum('sr,skq->rkq', belongs, lax.optimization_barrier(jnp.sum(weights, axis=-1)), precision=lax.Precision.HIGHEST)
        rounded = weights.astype(jnp.bfloat16).astype(jnp.float32)
        blended = jnp.einsum('skqt,sktd->skqd', rounded, value_rows.astype(jnp.float32))
        weighted = weighted + jnp.einsum('sr,skqd->rkqd', belongs, blended, precision=lax.Precision.HIGHEST)
        return ((totals, weighted), None)
    start_state = (jnp.zeros((REQ, KVH, qcount), jnp.float32), jnp.zeros((REQ, KVH, qcount, HD), jnp.float32))
    totals, weighted = lax.scan(second_pass, start_state, (key_blocks, value_blocks, owner_blocks, usable_blocks))[0]
    dweights = jnp.where(causal_flat, jnp.exp(dscore - peaks[..., None]), 0.0)
    totals = totals + lax.optimization_barrier(jnp.sum(dweights, axis=-1))
    drounded = dweights.astype(jnp.bfloat16).astype(jnp.float32)
    weighted = weighted + jnp.einsum('rkqj,rjkd->rkqd', drounded, dvals)
    result = weighted / totals[..., None]
    result = result.reshape(REQ, KVH, DRAFT, GROUP, HD).transpose(0, 2, 1, 3, 4).reshape(REQ, DRAFT, QH * HD)
    return (moved_keys, moved_values, result.astype(jnp.bfloat16))
```

```python
import math

import jax
import jax.numpy as jnp
from jax import lax
from jax.experimental import pallas as pl
from jax.experimental.pallas import tpu as pltpu
from jax.sharding import PartitionSpec as P

BLK = 128
DRAFT = 16
masked = -1e30


def pack_body(old_block, new_slot, keys, values, out_k, out_v, zeros, owned, sem_k, sem_v):
    slots = keys.shape[0]
    total = out_k.shape[0]
    chunk = zeros.shape[0]
    zeros[...] = jnp.zeros(zeros.shape, zeros.dtype)
    is_source = old_block[0] >= 0

    @pl.when(is_source)
    def _():
        def clear(t, c):
            owned[t] = 0
            return c

        lax.fori_loop(0, total, clear, 0, unroll=8)

        def send(i, c):
            t = new_slot[jnp.maximum(old_block[i], 0)]
            owned[t] = 1
            pltpu.make_async_copy(keys.at[i], out_k.at[t], sem_k).start()
            pltpu.make_async_copy(values.at[i], out_v.at[t], sem_v).start()
            return c

        lax.fori_loop(0, slots, send, 0)

        def fill(t, c):
            @pl.when(owned[t] == 0)
            def _():
                pltpu.make_async_copy(zeros.at[0], out_k.at[t], sem_k).start()
                pltpu.make_async_copy(zeros.at[0], out_v.at[t], sem_v).start()

            return c

        lax.fori_loop(0, total, fill, 0)

    @pl.when(jnp.logical_not(is_source))
    def _():
        for j in range(total // chunk):
            pltpu.make_async_copy(zeros, out_k.at[pl.ds(j * chunk, chunk)], sem_k).start()
            pltpu.make_async_copy(zeros, out_v.at[pl.ds(j * chunk, chunk)], sem_v).start()

    pltpu.make_async_copy(out_k, out_k, sem_k).wait()
    pltpu.make_async_copy(out_v, out_v, sem_v).wait()


def pack(old_block, new_slot, keys, values):
    total = new_slot.shape[0]
    out = jax.ShapeDtypeStruct((total,) + keys.shape[1:], keys.dtype)
    anyspace = pl.BlockSpec(memory_space=pl.ANY)
    smem = pl.BlockSpec(memory_space=pltpu.SMEM)
    return pl.pallas_call(
        pack_body,
        in_specs=[smem, smem, anyspace, anyspace],
        out_specs=[anyspace, anyspace],
        out_shape=[out, out],
        scratch_shapes=[
            pltpu.VMEM((32,) + keys.shape[1:], keys.dtype),
            pltpu.SMEM((total,), jnp.int32),
            pltpu.SemaphoreType.DMA,
            pltpu.SemaphoreType.DMA,
        ],
        name="pack",
    )(old_block, new_slot, keys, values)


def split3(x):
    hi = lax.reduce_precision(x, 8, 7)
    rest = x - hi
    mid = lax.reduce_precision(rest, 8, 7)
    low = lax.reduce_precision(rest - mid, 8, 7)
    return jnp.stack([hi, mid, low], axis=1).astype(jnp.bfloat16)


def cache_partial(keys, values, old_block, lengths, grouped, me_head):
    other = [(i, i ^ 1) for i in range(lax.axis_size("head"))]
    other_k = lax.ppermute(keys, "head", other)
    other_v = lax.ppermute(values, "head", other)
    slots, half, head_dim = keys.shape
    requests, qcount, _ = grouped.shape
    inv_root = 1.0 / math.sqrt(head_dim)
    counts = (lengths + BLK - 1) // BLK
    starts = jnp.cumsum(counts) - counts
    filled = old_block >= 0
    owner = jnp.sum((starts[None, :] <= old_block[:, None]).astype(jnp.int32), axis=1) - 1
    owner = jnp.clip(owner, 0, requests - 1)
    owned = (owner[:, None] == jnp.arange(requests)[None, :]) & filled[:, None]
    offset = old_block - jnp.sum(jnp.where(owned, starts[None, :], 0), axis=1)
    limit = jnp.sum(jnp.where(owned, lengths[None, :], 0), axis=1)
    token = jnp.arange(2 * half, dtype=jnp.int32)
    within = jnp.where(me_head % 2 == 0, token, (token + half) % (2 * half))
    usable = filled[:, None] & (offset[:, None] * BLK + within[None, :] < limit[:, None])
    key_rows = jnp.concatenate([keys, other_k], axis=1)
    value_rows = jnp.concatenate([values, other_v], axis=1)
    picked = grouped[owner]
    scores = (
        jnp.einsum("sqd,std->sqt", picked, key_rows, preferred_element_type=jnp.float32) * inv_root
    )
    scores = jnp.where(usable[:, None, :], scores, masked)
    slot_peaks = jnp.max(scores, axis=-1)
    peaks = jnp.max(jnp.where(owned[:, :, None], slot_peaks[:, None, :], masked), axis=0)
    own_peak = jnp.max(jnp.where(owned[:, :, None], peaks[None], masked), axis=1)
    weights = jnp.where(usable[:, None, :], jnp.exp(scores - own_peak[:, :, None]), 0.0)
    owned_f = owned.astype(jnp.float32)
    totals = jnp.dot(
        owned_f.T,
        jnp.sum(weights, axis=-1),
        precision=lax.Precision.HIGHEST,
        preferred_element_type=jnp.float32,
    )
    blended = jnp.einsum(
        "sqt,std->sqd",
        weights.astype(jnp.bfloat16),
        value_rows,
        preferred_element_type=jnp.float32,
    )
    weighted = jnp.einsum("sr,sqd->rqd", owned_f, blended, precision=lax.Precision.HIGHEST)
    return peaks, totals, weighted


def draft_partial(grouped, draft_keys, draft_values, inst, me_head):
    requests, qcount, head_dim = grouped.shape
    per_token = qcount // DRAFT
    rows = draft_keys.shape[0]
    kv_head = me_head // 2
    own_keys = lax.dynamic_slice_in_dim(draft_keys, kv_head * head_dim, head_dim, 2)
    own_vals = lax.dynamic_slice_in_dim(draft_values, kv_head * head_dim, head_dim, 2)
    own_q = lax.dynamic_slice_in_dim(grouped, inst * rows, rows, 0)
    inv_root = 1.0 / math.sqrt(head_dim)
    scores = (
        jnp.einsum("rqd,rjd->rqj", own_q, own_keys, preferred_element_type=jnp.float32) * inv_root
    )
    causal = jnp.arange(DRAFT)[None, :] <= (jnp.arange(qcount) // per_token)[:, None]
    scores = jnp.where(causal, scores, masked)
    peaks = jnp.max(scores, axis=-1)
    weights = jnp.where(causal, jnp.exp(scores - peaks[..., None]), 0.0)
    totals = jnp.sum(weights, axis=-1)
    weighted = jnp.einsum(
        "rqj,rjd->rqd", weights.astype(jnp.bfloat16), own_vals, preferred_element_type=jnp.float32
    )
    return peaks, totals, weighted


def spread(x):
    return lax.all_to_all(x, "inst", split_axis=0, concat_axis=0, tiled=True)


def shards(old_keys, old_values, old_block, new_slot, lengths, queries, draft_keys, draft_values):
    insts = lax.axis_size("inst")
    inst = lax.axis_index("inst")
    me_head = lax.axis_index("head")
    _, entries, half, head_dim = old_keys.shape
    keys = old_keys.reshape(-1, half, head_dim)
    values = old_values.reshape(-1, half, head_dim)
    blocks = new_slot.shape[0]
    requests = queries.shape[0]
    local_heads = queries.shape[2] // head_dim
    qcount = DRAFT * local_heads
    rows = requests // insts

    out_k, out_v = pack(old_block, new_slot, keys, values)
    inbox_k = spread(out_k)
    inbox_v = spread(out_v)

    grouped = queries.reshape(requests, qcount, head_dim)
    peaks, totals, weighted = cache_partial(keys, values, old_block, lengths, grouped, me_head)
    level = jnp.where(totals > 0, peaks + jnp.log(jnp.where(totals > 0, totals, 1.0)), masked)
    mean = weighted / jnp.where(totals > 0, totals, 1.0)[..., None]
    parts = split3(level.reshape(insts, rows * qcount)).reshape(insts, -1, head_dim)
    parts = jnp.pad(parts, ((0, 0), (0, -parts.shape[1] % 16), (0, 0)))
    packet = jnp.concatenate(
        [mean.astype(jnp.bfloat16).reshape(insts, rows * qcount, head_dim), parts], axis=1
    )
    got = spread(packet)
    got_mean = got[:, : rows * qcount].reshape(insts, rows, qcount, head_dim).astype(jnp.float32)
    got_parts = got[:, rows * qcount : rows * qcount + 3 * rows * qcount // head_dim]
    got_level = jnp.sum(
        got_parts.reshape(insts, 3, rows, qcount).astype(jnp.float32), axis=1
    )
    d_peaks, d_totals, d_weighted = draft_partial(grouped, draft_keys, draft_values, inst, me_head)
    top = jnp.maximum(jnp.max(got_level, axis=0), d_peaks)
    share = jnp.exp(got_level - top[None])
    d_share = jnp.exp(d_peaks - top)
    total = jnp.sum(share, axis=0) + d_totals * d_share
    acc = jnp.sum(got_mean * share[..., None], axis=0) + d_weighted * d_share[..., None]
    mine = (acc / total[..., None]).astype(jnp.bfloat16)
    full = spread(jnp.broadcast_to(mine[None], (insts,) + mine.shape))
    attended = full.reshape(requests, DRAFT, local_heads * head_dim)

    shape = (insts, blocks // insts, entries, half, head_dim)
    moved_keys = jnp.sum(inbox_k.reshape(shape), axis=0)
    moved_values = jnp.sum(inbox_v.reshape(shape), axis=0)
    return moved_keys, moved_values, attended


def solution(mesh):
    placed = (
        P("inst", "head", None, None),
        P("inst", "head", None, None),
        P("inst"),
        P(),
        P(),
        P(None, None, "head"),
        P("inst", None, None),
        P("inst", None, None),
    )
    return jax.shard_map(
        shards,
        mesh=mesh,
        in_specs=placed,
        out_specs=(
            P("inst", "head", None, None),
            P("inst", "head", None, None),
            P(None, None, "head"),
        ),
        check_vma=False,
    )
```

```python
import math

import jax
import jax.numpy as jnp
from jax import lax
from jax.experimental import pallas as pl
from jax.experimental.pallas import tpu as pltpu
from jax.sharding import PartitionSpec as P

BLK = 128
DRAFT = 16
masked = -1e30


COLS = 4


def pack_body(old_block, new_slot, base, keys, values, *rest):
    pieces = len(rest) - 6
    out_k = rest[: pieces // 2]
    out_v = rest[pieces // 2 : pieces]
    vk, vv, zeros, origin, sems, load_sem = rest[pieces:]
    slots = keys.shape[0]
    total = new_slot.shape[0]
    per = zeros.shape[0]
    is_source = old_block[0] >= 0

    @pl.when(is_source)
    def _():
        load_k = pltpu.make_async_copy(keys, vk, load_sem.at[0])
        load_v = pltpu.make_async_copy(values, vv, load_sem.at[1])
        load_k.start()
        load_v.start()
        zeros[0] = jnp.zeros(zeros.shape[1:], zeros.dtype)

        def clear(t, c):
            origin[t] = -1
            return c

        lax.fori_loop(0, total, clear, 0, unroll=8)

        def note(i, c):
            origin[new_slot[jnp.maximum(old_block[i], 0)]] = i
            return c

        lax.fori_loop(0, slots, note, 0, unroll=8)
        load_k.wait()
        load_v.wait()
        for p in range(pieces // 2):
            start = base[p]

            def send(j, c, p=p, start=start):
                i = origin[start + j]

                @pl.when(i >= 0)
                def _():
                    pltpu.make_async_copy(vk.at[i], out_k[p].at[j], sems.at[0, p]).start()
                    pltpu.make_async_copy(vv.at[i], out_v[p].at[j], sems.at[1, p]).start()

                @pl.when(i < 0)
                def _():
                    pltpu.make_async_copy(zeros.at[0], out_k[p].at[j], sems.at[0, p]).start()
                    pltpu.make_async_copy(zeros.at[0], out_v[p].at[j], sems.at[1, p]).start()

                return c

            lax.fori_loop(0, per, send, 0, unroll=4)

    @pl.when(jnp.logical_not(is_source))
    def _():
        zeros[...] = jnp.zeros(zeros.shape, zeros.dtype)
        for p in range(pieces // 2):
            pltpu.make_async_copy(zeros, out_k[p], sems.at[0, p]).start()
            pltpu.make_async_copy(zeros, out_v[p], sems.at[1, p]).start()

    for p in range(pieces // 2):
        pltpu.make_async_copy(zeros, out_k[p], sems.at[0, p]).wait()
        pltpu.make_async_copy(zeros, out_v[p], sems.at[1, p]).wait()


def pack(old_block, new_slot, keys, values, inst, insts):
    total = new_slot.shape[0]
    per = total // insts
    step = jnp.arange(insts, dtype=jnp.int32)
    away = (inst // COLS) ^ (step % 2)
    column = (inst % COLS + step // 2) % COLS
    base = (away * COLS + column) * per
    out = jax.ShapeDtypeStruct((per,) + keys.shape[1:], keys.dtype)
    anyspace = pl.BlockSpec(memory_space=pl.ANY)
    smem = pl.BlockSpec(memory_space=pltpu.SMEM)
    got = pl.pallas_call(
        pack_body,
        in_specs=[smem, smem, smem, anyspace, anyspace],
        out_specs=[anyspace] * (2 * insts),
        out_shape=[out] * (2 * insts),
        scratch_shapes=[
            pltpu.VMEM(keys.shape, keys.dtype),
            pltpu.VMEM(keys.shape, keys.dtype),
            pltpu.VMEM((per,) + keys.shape[1:], keys.dtype),
            pltpu.SMEM((total,), jnp.int32),
            pltpu.SemaphoreType.DMA((2, insts)),
            pltpu.SemaphoreType.DMA((2,)),
        ],
        name="pack",
    )(old_block, new_slot, base, keys, values)
    return got[:insts], got[insts:]


def right(x):
    rows = lax.axis_size("inst") // COLS
    route = [(r * COLS + c, r * COLS + (c + 1) % COLS) for r in range(rows) for c in range(COLS)]
    return lax.ppermute(x, "inst", route)


def left(x):
    rows = lax.axis_size("inst") // COLS
    route = [(r * COLS + (c + 1) % COLS, r * COLS + c) for r in range(rows) for c in range(COLS)]
    return lax.ppermute(x, "inst", route)


def across(x):
    return lax.ppermute(x, "inst", [(i, i ^ COLS) for i in range(lax.axis_size("inst"))])


def move_keys(pieces):
    k0n, k0f, k1n, k1f, k2n, k2f, k3n, k3f = pieces
    a1, b1 = right(k2n), left(k2f)
    f1, n3 = right(k1f), left(k3n)
    a2, b2 = right(k1n + a1), left(k3f + b1)
    return k0n + n3 + a2 + across(k0f + f1 + b2)


def move_values(pieces):
    v0n, v0f, v1n, v1f, v2n, v2f, v3n, v3f = pieces
    y2, y1, y3, y0 = across(v2f), across(v1f), across(v3f), across(v0f)
    cut = v2n.shape[0] // 2
    w2 = v2n + y2
    c1, d1 = right(w2[:cut]), left(w2[cut:])
    w1 = v1n + y1
    w3 = v3n + y3
    e_hi, g_lo = right(w1[cut:]), left(w3[:cut])
    e_lo, g_hi = right(w1[:cut] + c1), left(w3[cut:] + d1)
    return v0n + y0 + jnp.concatenate([e_lo + g_lo, e_hi + g_hi])


def split3(x):
    hi = lax.reduce_precision(x, 8, 7)
    rest = x - hi
    mid = lax.reduce_precision(rest, 8, 7)
    low = lax.reduce_precision(rest - mid, 8, 7)
    return jnp.stack([hi, mid, low], axis=1).astype(jnp.bfloat16)


def cache_partial(keys, values, old_block, lengths, grouped, me_head):
    other = [(i, i ^ 1) for i in range(lax.axis_size("head"))]
    other_k = lax.ppermute(keys, "head", other)
    other_v = lax.ppermute(values, "head", other)
    slots, half, head_dim = keys.shape
    requests, qcount, _ = grouped.shape
    inv_root = 1.0 / math.sqrt(head_dim)
    counts = (lengths + BLK - 1) // BLK
    starts = jnp.cumsum(counts) - counts
    filled = old_block >= 0
    owner = jnp.sum((starts[None, :] <= old_block[:, None]).astype(jnp.int32), axis=1) - 1
    owner = jnp.clip(owner, 0, requests - 1)
    owned = (owner[:, None] == jnp.arange(requests)[None, :]) & filled[:, None]
    offset = old_block - jnp.sum(jnp.where(owned, starts[None, :], 0), axis=1)
    limit = jnp.sum(jnp.where(owned, lengths[None, :], 0), axis=1)
    token = jnp.arange(2 * half, dtype=jnp.int32)
    within = jnp.where(me_head % 2 == 0, token, (token + half) % (2 * half))
    usable = filled[:, None] & (offset[:, None] * BLK + within[None, :] < limit[:, None])
    key_rows = jnp.concatenate([keys, other_k], axis=1)
    value_rows = jnp.concatenate([values, other_v], axis=1)
    picked = grouped[owner]
    scores = (
        jnp.einsum("sqd,std->sqt", picked, key_rows, preferred_element_type=jnp.float32) * inv_root
    )
    scores = jnp.where(usable[:, None, :], scores, masked)
    slot_peaks = jnp.max(scores, axis=-1)
    peaks = jnp.max(jnp.where(owned[:, :, None], slot_peaks[:, None, :], masked), axis=0)
    own_peak = jnp.max(jnp.where(owned[:, :, None], peaks[None], masked), axis=1)
    weights = jnp.where(usable[:, None, :], jnp.exp(scores - own_peak[:, :, None]), 0.0)
    owned_f = owned.astype(jnp.float32)
    totals = jnp.dot(
        owned_f.T,
        jnp.sum(weights, axis=-1),
        precision=lax.Precision.HIGHEST,
        preferred_element_type=jnp.float32,
    )
    blended = jnp.einsum(
        "sqt,std->sqd",
        weights.astype(jnp.bfloat16),
        value_rows,
        preferred_element_type=jnp.float32,
    )
    weighted = jnp.einsum("sr,sqd->rqd", owned_f, blended, precision=lax.Precision.HIGHEST)
    return peaks, totals, weighted


def draft_partial(grouped, draft_keys, draft_values, inst, me_head):
    requests, qcount, head_dim = grouped.shape
    per_token = qcount // DRAFT
    rows = draft_keys.shape[0]
    kv_head = me_head // 2
    own_keys = lax.dynamic_slice_in_dim(draft_keys, kv_head * head_dim, head_dim, 2)
    own_vals = lax.dynamic_slice_in_dim(draft_values, kv_head * head_dim, head_dim, 2)
    own_q = lax.dynamic_slice_in_dim(grouped, inst * rows, rows, 0)
    inv_root = 1.0 / math.sqrt(head_dim)
    scores = (
        jnp.einsum("rqd,rjd->rqj", own_q, own_keys, preferred_element_type=jnp.float32) * inv_root
    )
    causal = jnp.arange(DRAFT)[None, :] <= (jnp.arange(qcount) // per_token)[:, None]
    scores = jnp.where(causal, scores, masked)
    peaks = jnp.max(scores, axis=-1)
    weights = jnp.where(causal, jnp.exp(scores - peaks[..., None]), 0.0)
    totals = jnp.sum(weights, axis=-1)
    weighted = jnp.einsum(
        "rqj,rjd->rqd", weights.astype(jnp.bfloat16), own_vals, preferred_element_type=jnp.float32
    )
    return peaks, totals, weighted


def spread(x):
    return lax.all_to_all(x, "inst", split_axis=0, concat_axis=0, tiled=True)


def shards(old_keys, old_values, old_block, new_slot, lengths, queries, draft_keys, draft_values):
    insts = lax.axis_size("inst")
    inst = lax.axis_index("inst")
    me_head = lax.axis_index("head")
    _, entries, half, head_dim = old_keys.shape
    keys = old_keys.reshape(-1, half, head_dim)
    values = old_values.reshape(-1, half, head_dim)
    blocks = new_slot.shape[0]
    requests = queries.shape[0]
    local_heads = queries.shape[2] // head_dim
    qcount = DRAFT * local_heads
    rows = requests // insts

    out_k, out_v = pack(old_block, new_slot, keys, values, inst, insts)
    queries, out_k, out_v = lax.optimization_barrier((queries, out_k, out_v))
    shape = (blocks // insts, entries, half, head_dim)
    moved_values = move_values(out_v).reshape(shape)
    moved_keys = move_keys(out_k).reshape(shape)

    grouped = queries.reshape(requests, qcount, head_dim)
    peaks, totals, weighted = cache_partial(keys, values, old_block, lengths, grouped, me_head)
    level = jnp.where(totals > 0, peaks + jnp.log(jnp.where(totals > 0, totals, 1.0)), masked)
    mean = weighted / jnp.where(totals > 0, totals, 1.0)[..., None]
    parts = split3(level.reshape(insts, rows * qcount)).reshape(insts, -1, head_dim)
    parts = jnp.pad(parts, ((0, 0), (0, -parts.shape[1] % 16), (0, 0)))
    packet = jnp.concatenate(
        [mean.astype(jnp.bfloat16).reshape(insts, rows * qcount, head_dim), parts], axis=1
    )
    got = spread(packet)
    got_mean = got[:, : rows * qcount].reshape(insts, rows, qcount, head_dim).astype(jnp.float32)
    got_parts = got[:, rows * qcount : rows * qcount + 3 * rows * qcount // head_dim]
    got_level = jnp.sum(
        got_parts.reshape(insts, 3, rows, qcount).astype(jnp.float32), axis=1
    )
    d_peaks, d_totals, d_weighted = draft_partial(grouped, draft_keys, draft_values, inst, me_head)
    top = jnp.maximum(jnp.max(got_level, axis=0), d_peaks)
    share = jnp.exp(got_level - top[None])
    d_share = jnp.exp(d_peaks - top)
    total = jnp.sum(share, axis=0) + d_totals * d_share
    acc = jnp.sum(got_mean * share[..., None], axis=0) + d_weighted * d_share[..., None]
    mine = (acc / total[..., None]).astype(jnp.bfloat16)
    full = spread(jnp.broadcast_to(mine[None], (insts,) + mine.shape))
    attended = full.reshape(requests, DRAFT, local_heads * head_dim)

    return moved_keys, moved_values, attended


def solution(mesh):
    placed = (
        P("inst", "head", None, None),
        P("inst", "head", None, None),
        P("inst"),
        P(),
        P(),
        P(None, None, "head"),
        P("inst", None, None),
        P("inst", None, None),
    )
    return jax.shard_map(
        shards,
        mesh=mesh,
        in_specs=placed,
        out_specs=(
            P("inst", "head", None, None),
            P("inst", "head", None, None),
            P(None, None, "head"),
        ),
        check_vma=False,
    )
```

```python
import math

import jax
import jax.numpy as jnp
from jax import lax
from jax.experimental import pallas as pl
from jax.experimental.pallas import tpu as pltpu
from jax.sharding import PartitionSpec as P

BLK = 128
DRAFT = 16
masked = -1e30


COLS = 4


GROUPS_K = ((4, 3), (5, 6), (2,), (7,), (0,), (1,))
GROUPS_V = ((5, 3, 7), (1,), (4,), (2,), (6,), (0,))


def pack_body(old_block, new_slot, base, keys, values, *rest):
    count = len(GROUPS_K) + len(GROUPS_V)
    outs = rest[:count]
    vk, vv, zeros, origin, sems, load_sem = rest[count:]
    slots = keys.shape[0]
    total = new_slot.shape[0]
    per = zeros.shape[0]
    is_source = old_block[0] >= 0
    jobs = [(vk, out, group) for out, group in zip(outs, GROUPS_K)]
    jobs += [(vv, out, group) for out, group in zip(outs[len(GROUPS_K) :], GROUPS_V)]

    @pl.when(is_source)
    def _():
        load_k = pltpu.make_async_copy(keys, vk, load_sem.at[0])
        load_v = pltpu.make_async_copy(values, vv, load_sem.at[1])
        load_k.start()
        load_v.start()
        zeros[0] = jnp.zeros(zeros.shape[1:], zeros.dtype)

        def clear(t, c):
            origin[t] = -1
            return c

        lax.fori_loop(0, total, clear, 0, unroll=8)

        def note(i, c):
            origin[new_slot[jnp.maximum(old_block[i], 0)]] = i
            return c

        lax.fori_loop(0, slots, note, 0, unroll=8)
        load_k.wait()
        load_v.wait()
        for at, (cache, out, group) in enumerate(jobs):
            for g, p in enumerate(group):
                start = base[p]

                def send(j, c, cache=cache, out=out, at=at, g=g, start=start):
                    i = origin[start + j]

                    @pl.when(i >= 0)
                    def _():
                        pltpu.make_async_copy(cache.at[i], out.at[g * per + j], sems.at[at]).start()

                    @pl.when(i < 0)
                    def _():
                        pltpu.make_async_copy(zeros.at[0], out.at[g * per + j], sems.at[at]).start()

                    return c

                lax.fori_loop(0, per, send, 0, unroll=4)

    @pl.when(jnp.logical_not(is_source))
    def _():
        zeros[...] = jnp.zeros(zeros.shape, zeros.dtype)
        for at, (cache, out, group) in enumerate(jobs):
            for g in range(len(group)):
                pltpu.make_async_copy(zeros, out.at[pl.ds(g * per, per)], sems.at[at]).start()

    for at, (cache, out, group) in enumerate(jobs):
        pltpu.make_async_copy(out, out, sems.at[at]).wait()


def pack(old_block, new_slot, keys, values, inst, insts):
    total = new_slot.shape[0]
    per = total // insts
    step = jnp.arange(insts, dtype=jnp.int32)
    away = (inst // COLS) ^ (step % 2)
    column = (inst % COLS + step // 2) % COLS
    base = (away * COLS + column) * per
    groups = GROUPS_K + GROUPS_V
    anyspace = pl.BlockSpec(memory_space=pl.ANY)
    smem = pl.BlockSpec(memory_space=pltpu.SMEM)
    got = pl.pallas_call(
        pack_body,
        in_specs=[smem, smem, smem, anyspace, anyspace],
        out_specs=[anyspace] * len(groups),
        out_shape=[
            jax.ShapeDtypeStruct((per * len(g),) + keys.shape[1:], keys.dtype) for g in groups
        ],
        scratch_shapes=[
            pltpu.VMEM(keys.shape, keys.dtype),
            pltpu.VMEM(keys.shape, keys.dtype),
            pltpu.VMEM((per,) + keys.shape[1:], keys.dtype),
            pltpu.SMEM((total,), jnp.int32),
            pltpu.SemaphoreType.DMA((len(groups),)),
            pltpu.SemaphoreType.DMA((2,)),
        ],
        name="pack",
    )(old_block, new_slot, base, keys, values)
    return got[: len(GROUPS_K)], got[len(GROUPS_K) :]


def right(x):
    rows = lax.axis_size("inst") // COLS
    route = [(r * COLS + c, r * COLS + (c + 1) % COLS) for r in range(rows) for c in range(COLS)]
    return lax.ppermute(x, "inst", route)


def left(x):
    rows = lax.axis_size("inst") // COLS
    route = [(r * COLS + (c + 1) % COLS, r * COLS + c) for r in range(rows) for c in range(COLS)]
    return lax.ppermute(x, "inst", route)


def across(x):
    return lax.ppermute(x, "inst", [(i, i ^ COLS) for i in range(lax.axis_size("inst"))])


def move_keys(groups):
    to_right, to_left, k1n, k3f, k0n, k0f = groups
    per = k1n.shape[0]
    from_left, from_right = right(to_right), left(to_left)
    a2 = right(k1n + from_left[:per])
    b2 = left(k3f + from_right[:per])
    return k0n + from_right[per:] + a2 + across(k0f + from_left[per:] + b2)


def move_values(groups):
    far, v0f, v2n, v1n, v3n, v0n = groups
    per = v1n.shape[0]
    cut = per // 2
    got = across(far)
    y0 = across(v0f)
    w2 = v2n + got[:per]
    w1 = v1n + got[per : 2 * per]
    w3 = v3n + got[2 * per :]
    from_left = right(jnp.concatenate([w2[:cut], w1[cut:]]))
    from_right = left(jnp.concatenate([w2[cut:], w3[:cut]]))
    e_lo = right(w1[:cut] + from_left[:cut])
    g_hi = left(w3[cut:] + from_right[:cut])
    return v0n + y0 + jnp.concatenate([e_lo + from_right[cut:], from_left[cut:] + g_hi])


def dot_t(x, y):
    return lax.dot_general(x, y, (((1,), (1,)), ((), ())), preferred_element_type=jnp.float32)


def attend_body(
    old_block, lengths, meta, q, k, v, ok, ov, dk, dv, packet,
    vq, vk, vv, vok, vov, scores, drafted, peak, total, acc, owner, live, sems,
):
    requests, draft, width = vq.shape
    head_dim = vk.shape[2]
    half = vk.shape[1]
    slots = vk.shape[0]
    heads = width // head_dim
    qrows = draft * heads
    insts = packet.shape[0]
    rows = requests // insts
    inv_root = 1.0 / math.sqrt(head_dim)
    is_source = old_block[0] >= 0
    first = meta[0]
    shift = meta[1]
    load_q = pltpu.make_async_copy(q, vq, sems.at[0])
    load_q.start()
    loads = [
        pltpu.make_async_copy(x, y, sems.at[1 + n])
        for n, (x, y) in enumerate(((k, vk), (ok, vok), (v, vv), (ov, vov)))
    ]

    @pl.when(is_source)
    def _():
        for load in loads:
            load.start()

        def per_request(r, g):
            size = lengths[r]

            def per_block(j, c):
                owner[g + j] = r
                live[g + j] = jnp.minimum(size - j * BLK, BLK)
                return c

            n = (size + BLK - 1) // BLK
            lax.fori_loop(0, n, per_block, 0)
            return g + n

        lax.fori_loop(0, requests, per_request, 0)

    def q_of(r):
        return jnp.concatenate(
            [vq[r, :, h * head_dim : (h + 1) * head_dim] for h in range(heads)], axis=0
        )

    lane = lax.broadcasted_iota(jnp.int32, (qrows, head_dim), 1)
    row = lax.broadcasted_iota(jnp.int32, (qrows, head_dim), 0)
    place = (lane + shift) % (2 * half)
    causal = lane <= row % draft
    blank = jnp.full((qrows, head_dim), masked, jnp.float32)

    def reset(r, c):
        peak[r] = blank
        return c

    lax.fori_loop(0, requests, reset, 0, unroll=4)
    load_q.wait()
    pad = jnp.zeros((2 * half - draft, head_dim), dk.dtype)
    for a in range(rows):
        s = dot_t(q_of(first + a), jnp.concatenate([dk[a], pad], axis=0)) * inv_root
        s = jnp.where(causal, s, masked)
        drafted[a] = s
        peak[first + a] = s

    @pl.when(is_source)
    def _():
        loads[0].wait()
        loads[1].wait()

        def score(n, c):
            for u in range(UNROLL):
                i = n * UNROLL + u
                g = jnp.maximum(old_block[i], 0)
                r = owner[g]
                key = jnp.concatenate([vk[i], vok[i]], axis=0)
                s = dot_t(q_of(r), key) * inv_root
                s = jnp.where(place < live[g], s, masked)
                scores[i] = s
                peak[r] = jnp.maximum(peak[r], s)
            return c

        lax.fori_loop(0, slots // UNROLL, score, 0)

    def settle(r, c):
        peak[r] = jnp.broadcast_to(jnp.max(peak[r], axis=1, keepdims=True), (qrows, head_dim))
        total[r] = jnp.zeros((qrows, head_dim), jnp.float32)
        acc[r] = jnp.zeros((qrows, head_dim), jnp.float32)
        return c

    lax.fori_loop(0, requests, settle, 0, unroll=2)
    for a in range(rows):
        w = jnp.exp(drafted[a] - peak[first + a])
        total[first + a] = w
        acc[first + a] = jnp.dot(
            w.astype(dv.dtype),
            jnp.concatenate([dv[a], pad], axis=0),
            preferred_element_type=jnp.float32,
        )

    @pl.when(is_source)
    def _():
        loads[2].wait()
        loads[3].wait()

        def gather(n, c):
            for u in range(UNROLL):
                i = n * UNROLL + u
                r = owner[jnp.maximum(old_block[i], 0)]
                w = jnp.exp(scores[i] - peak[r])
                value = jnp.concatenate([vv[i], vov[i]], axis=0)
                out = jnp.dot(w.astype(vv.dtype), value, preferred_element_type=jnp.float32)
                total[r] += w
                acc[r] += out
            return c

        lax.fori_loop(0, slots // UNROLL, gather, 0)

    def finish(d, c):
        stat = jnp.zeros((qrows, head_dim), jnp.float32)
        for a in range(rows):
            r = d * rows + a
            l = jnp.sum(total[r], axis=1, keepdims=True)
            seen = l > 0
            safe = jnp.where(seen, l, 1.0)
            packet[d, a * qrows : (a + 1) * qrows, :] = (acc[r] / safe).astype(packet.dtype)
            level = jnp.where(seen, peak[r] + jnp.log(safe), masked)
            hi = level.astype(jnp.bfloat16).astype(jnp.float32)
            mid = (level - hi).astype(jnp.bfloat16).astype(jnp.float32)
            low = level - hi - mid
            stat = jnp.where(lane == 3 * a, hi, stat)
            stat = jnp.where(lane == 3 * a + 1, mid, stat)
            stat = jnp.where(lane == 3 * a + 2, low, stat)
        packet[d, rows * qrows :, :] = stat.astype(packet.dtype)
        return c

    lax.fori_loop(0, insts, finish, 0)


UNROLL = 4


def attend(old_block, lengths, meta, queries, keys, values, other_k, other_v, dk, dv, insts):
    requests, draft, width = queries.shape
    head_dim = keys.shape[2]
    qrows = draft * width // head_dim
    rows = requests // insts
    anyspace = pl.BlockSpec(memory_space=pl.ANY)
    smem = pl.BlockSpec(memory_space=pltpu.SMEM)
    vmem = pl.BlockSpec(memory_space=pltpu.VMEM)
    bf16 = jnp.bfloat16
    state = pltpu.VMEM((requests, qrows, head_dim), jnp.float32)
    return pl.pallas_call(
        attend_body,
        in_specs=[smem] * 3 + [anyspace] * 5 + [vmem] * 2,
        out_specs=vmem,
        out_shape=jax.ShapeDtypeStruct((insts, (rows + 1) * qrows, head_dim), bf16),
        scratch_shapes=[pltpu.VMEM(queries.shape, bf16)]
        + [pltpu.VMEM(keys.shape, bf16)] * 4
        + [
            pltpu.VMEM((keys.shape[0], qrows, head_dim), jnp.float32),
            pltpu.VMEM((rows, qrows, head_dim), jnp.float32),
            state,
            state,
            state,
            pltpu.SMEM((TOTAL,), jnp.int32),
            pltpu.SMEM((TOTAL,), jnp.int32),
            pltpu.SemaphoreType.DMA((5,)),
        ],
        name="attend",
    )(old_block, lengths, meta, queries, keys, values, other_k, other_v, dk, dv)


TOTAL = 256


def join_body(got, out):
    insts, _, head_dim = got.shape
    rows = out.shape[1]
    draft = out.shape[2]
    heads = out.shape[3] // head_dim
    qrows = draft * heads
    lane = lax.broadcasted_iota(jnp.int32, (qrows, head_dim), 1)
    stats = [got[s, rows * qrows :, :].astype(jnp.float32) for s in range(insts)]
    for a in range(rows):
        mine = (lane >= 3 * a) & (lane < 3 * a + 3)
        level = [
            jnp.sum(jnp.where(mine, stat, 0.0), axis=1, keepdims=True) for stat in stats
        ]
        top = level[0]
        for x in level[1:]:
            top = jnp.maximum(top, x)
        total = jnp.zeros((qrows, 1), jnp.float32)
        acc = jnp.zeros((qrows, head_dim), jnp.float32)
        for s in range(insts):
            share = jnp.exp(level[s] - top)
            total = total + share
            acc = acc + share * got[s, a * qrows : (a + 1) * qrows, :].astype(jnp.float32)
        res = (acc / total).astype(out.dtype)
        for d in range(insts):
            for h in range(heads):
                out[d, a, :, h * head_dim : (h + 1) * head_dim] = res[h * draft : (h + 1) * draft]


def join(got, rows, draft, width):
    insts = got.shape[0]
    vmem = pl.BlockSpec(memory_space=pltpu.VMEM)
    return pl.pallas_call(
        join_body,
        in_specs=[vmem],
        out_specs=vmem,
        out_shape=jax.ShapeDtypeStruct((insts, rows, draft, width), got.dtype),
        name="join",
    )(got)


def spread(x):
    return lax.all_to_all(x, "inst", split_axis=0, concat_axis=0, tiled=True)


def shards(old_keys, old_values, old_block, new_slot, lengths, queries, draft_keys, draft_values):
    insts = lax.axis_size("inst")
    inst = lax.axis_index("inst")
    me_head = lax.axis_index("head")
    _, entries, half, head_dim = old_keys.shape
    keys = old_keys.reshape(-1, half, head_dim)
    values = old_values.reshape(-1, half, head_dim)
    blocks = new_slot.shape[0]
    requests = queries.shape[0]
    rows = requests // insts
    swap = [(i, i ^ 1) for i in range(lax.axis_size("head"))]
    other_k = lax.ppermute(keys, "head", swap)
    other_v = lax.ppermute(values, "head", swap)

    out_k, out_v = pack(old_block, new_slot, keys, values, inst, insts)
    queries, out_k, out_v = lax.optimization_barrier((queries, out_k, out_v))
    shape = (blocks // insts, entries, half, head_dim)
    moved_values = move_values(out_v).reshape(shape)
    moved_keys = move_keys(out_k).reshape(shape)

    kv_head = me_head // 2
    dk = lax.dynamic_slice_in_dim(draft_keys, kv_head * head_dim, head_dim, 2)
    dv = lax.dynamic_slice_in_dim(draft_values, kv_head * head_dim, head_dim, 2)
    meta = jnp.stack([inst * rows, me_head % 2 * half])
    packet = attend(
        old_block, lengths, meta, queries, keys, values, other_k, other_v, dk, dv, insts
    )
    mine = join(spread(packet), rows, queries.shape[1], queries.shape[2])
    attended = spread(mine).reshape(queries.shape)
    return moved_keys, moved_values, attended


def solution(mesh):
    placed = (
        P("inst", "head", None, None),
        P("inst", "head", None, None),
        P("inst"),
        P(),
        P(),
        P(None, None, "head"),
        P("inst", None, None),
        P("inst", None, None),
    )
    return jax.shard_map(
        shards,
        mesh=mesh,
        in_specs=placed,
        out_specs=(
            P("inst", "head", None, None),
            P("inst", "head", None, None),
            P(None, None, "head"),
        ),
        check_vma=False,
    )
```

```python
import math

import jax
import jax.numpy as jnp
from jax import lax
from jax.experimental import pallas as pl
from jax.experimental.pallas import tpu as pltpu
from jax.sharding import PartitionSpec as P


BLK = 128
masked = -1e30


COLS = 4


GROUPS_K = ((4, 3), (5, 6), (2,), (7,), (0,), (1,))
GROUPS_V = ((5, 3, 7), (1,), (4,), (2,), (6,), (0,))


def pack_body(old_block, new_slot, base, keys, values, *rest):
    count = len(GROUPS_K) + len(GROUPS_V)
    outs = rest[:count]
    vk, vv, zeros, origin, sems, load_sem = rest[count:]
    slots = keys.shape[0]
    total = new_slot.shape[0]
    per = zeros.shape[0]
    is_source = old_block[0] >= 0
    jobs = [(vk, out, group) for out, group in zip(outs, GROUPS_K)]
    jobs += [(vv, out, group) for out, group in zip(outs[len(GROUPS_K) :], GROUPS_V)]

    @pl.when(is_source)
    def _():
        load_k = pltpu.make_async_copy(keys, vk, load_sem.at[0])
        load_v = pltpu.make_async_copy(values, vv, load_sem.at[1])
        load_k.start()
        load_v.start()
        zeros[0] = jnp.zeros(zeros.shape[1:], zeros.dtype)

        def clear(t, c):
            origin[t] = -1
            return c

        lax.fori_loop(0, total, clear, 0, unroll=8)

        def note(i, c):
            origin[new_slot[jnp.maximum(old_block[i], 0)]] = i
            return c

        lax.fori_loop(0, slots, note, 0, unroll=8)
        load_k.wait()
        load_v.wait()
        for at, (cache, out, group) in enumerate(jobs):
            for g, p in enumerate(group):
                start = base[p]

                def send(j, c, cache=cache, out=out, at=at, g=g, start=start):
                    i = origin[start + j]

                    @pl.when(i >= 0)
                    def _():
                        pltpu.make_async_copy(cache.at[i], out.at[g * per + j], sems.at[at]).start()

                    @pl.when(i < 0)
                    def _():
                        pltpu.make_async_copy(zeros.at[0], out.at[g * per + j], sems.at[at]).start()

                    return c

                lax.fori_loop(0, per, send, 0, unroll=4)

    @pl.when(jnp.logical_not(is_source))
    def _():
        zeros[...] = jnp.zeros(zeros.shape, zeros.dtype)
        for at, (cache, out, group) in enumerate(jobs):
            for g in range(len(group)):
                pltpu.make_async_copy(zeros, out.at[pl.ds(g * per, per)], sems.at[at]).start()

    for at, (cache, out, group) in enumerate(jobs):
        pltpu.make_async_copy(out, out, sems.at[at]).wait()


def pack(old_block, new_slot, keys, values, inst, insts):
    total = new_slot.shape[0]
    per = total // insts
    step = jnp.arange(insts, dtype=jnp.int32)
    away = (inst // COLS) ^ (step % 2)
    column = (inst % COLS + step // 2) % COLS
    base = (away * COLS + column) * per
    groups = GROUPS_K + GROUPS_V
    anyspace = pl.BlockSpec(memory_space=pl.ANY)
    smem = pl.BlockSpec(memory_space=pltpu.SMEM)
    got = pl.pallas_call(
        pack_body,
        in_specs=[smem, smem, smem, anyspace, anyspace],
        out_specs=[anyspace] * len(groups),
        out_shape=[
            jax.ShapeDtypeStruct((per * len(g),) + keys.shape[1:], keys.dtype) for g in groups
        ],
        scratch_shapes=[
            pltpu.VMEM(keys.shape, keys.dtype),
            pltpu.VMEM(keys.shape, keys.dtype),
            pltpu.VMEM((per,) + keys.shape[1:], keys.dtype),
            pltpu.SMEM((total,), jnp.int32),
            pltpu.SemaphoreType.DMA((len(groups),)),
            pltpu.SemaphoreType.DMA((2,)),
        ],
        name="pack",
    )(old_block, new_slot, base, keys, values)
    return got[: len(GROUPS_K)], got[len(GROUPS_K) :]


def right(x):
    rows = lax.axis_size("inst") // COLS
    route = [(r * COLS + c, r * COLS + (c + 1) % COLS) for r in range(rows) for c in range(COLS)]
    return lax.ppermute(x, "inst", route)


def left(x):
    rows = lax.axis_size("inst") // COLS
    route = [(r * COLS + (c + 1) % COLS, r * COLS + c) for r in range(rows) for c in range(COLS)]
    return lax.ppermute(x, "inst", route)


def across(x):
    return lax.ppermute(x, "inst", [(i, i ^ COLS) for i in range(lax.axis_size("inst"))])


def vmem_call(body, outs, *args):
    vmem = pl.BlockSpec(memory_space=pltpu.VMEM)
    return pl.pallas_call(
        body,
        in_specs=[vmem] * len(args),
        out_specs=[vmem] * len(outs),
        out_shape=[jax.ShapeDtypeStruct(shape, args[0].dtype) for shape in outs],
    )(*args)


def merge_keys_body(from_left, from_right, k1n, k3f, k0n, k0f, o_right, o_left, near, cross):
    per = k1n.shape[0]
    o_right[...] = k1n[...] + from_left[:per]
    o_left[...] = k3f[...] + from_right[:per]
    near[...] = k0n[...] + from_right[per:]
    cross[...] = k0f[...] + from_left[per:]


def move_keys(from_left, from_right, groups):
    piece = groups[0].shape
    o_right, o_left, near, cross = vmem_call(
        merge_keys_body, [piece] * 4, from_left, from_right, *groups
    )
    a2 = right(o_right)
    b2 = left(o_left)
    crossed = across(cross + b2)
    return near + a2 + crossed


def merge_values_body(far, v2n, v1n, v3n, o_right, o_left, low, high):
    per = v1n.shape[0]
    cut = per // 2
    o_right[:cut] = v2n[:cut] + far[:cut]
    o_left[:cut] = v2n[cut:] + far[cut:per]
    low[...] = v1n[:cut] + far[per : per + cut]
    o_right[cut:] = v1n[cut:] + far[per + cut : 2 * per]
    o_left[cut:] = v3n[:cut] + far[2 * per : 2 * per + cut]
    high[...] = v3n[cut:] + far[2 * per + cut :]


def second_body(low, high, from_left, from_right, o_right, o_left):
    cut = low.shape[0]
    o_right[...] = low[...] + from_left[:cut]
    o_left[...] = high[...] + from_right[:cut]


def move_values(got, y0, groups):
    v2n, v1n, v3n, v0n = groups
    cut = v1n.shape[0] // 2
    piece = v1n.shape
    part = (cut,) + piece[1:]
    o_right, o_left, low, high = vmem_call(
        merge_values_body, [piece, piece, part, part], got, v2n, v1n, v3n
    )
    from_left = right(o_right)
    from_right = left(o_left)
    o_right, o_left = vmem_call(second_body, [part, part], low, high, from_left, from_right)
    e_lo = right(o_right)
    g_hi = left(o_left)
    return v0n + y0 + jnp.concatenate([e_lo + from_right[cut:], from_left[cut:] + g_hi])


def dot_t(x, y):
    return lax.dot_general(x, y, (((1,), (1,)), ((), ())), preferred_element_type=jnp.float32)


def attend_body(
    old_block, lengths, meta, q, k, v, ok, ov, dk, dv, packet,
    vq, vk, vv, vok, vov, scores, drafted, peak, total, acc, owner, live, sems,
):
    requests, draft, width = vq.shape
    head_dim = vk.shape[2]
    half = vk.shape[1]
    slots = vk.shape[0]
    heads = width // head_dim
    qrows = draft * heads
    insts = packet.shape[0]
    rows = requests // insts
    inv_root = 1.0 / math.sqrt(head_dim)
    is_source = old_block[0] >= 0
    first = meta[0]
    shift = meta[1]
    load_q = pltpu.make_async_copy(q, vq, sems.at[0])
    load_q.start()
    loads = [
        pltpu.make_async_copy(x, y, sems.at[1 + n])
        for n, (x, y) in enumerate(((k, vk), (ok, vok), (v, vv), (ov, vov)))
    ]

    @pl.when(is_source)
    def _():
        for load in loads:
            load.start()

        def per_request(r, g):
            size = lengths[r]

            def per_block(j, c):
                owner[g + j] = r
                live[g + j] = jnp.minimum(size - j * BLK, BLK)
                return c

            n = (size + BLK - 1) // BLK
            lax.fori_loop(0, n, per_block, 0)
            return g + n

        lax.fori_loop(0, requests, per_request, 0)

    def q_of(r):
        return jnp.concatenate(
            [vq[r, :, h * head_dim : (h + 1) * head_dim] for h in range(heads)], axis=0
        )

    lane = lax.broadcasted_iota(jnp.int32, (qrows, head_dim), 1)
    row = lax.broadcasted_iota(jnp.int32, (qrows, head_dim), 0)
    place = (lane + shift) % (2 * half)
    causal = lane <= row % draft
    blank = jnp.full((qrows, head_dim), masked, jnp.float32)

    def reset(r, c):
        peak[r] = blank
        return c

    lax.fori_loop(0, requests, reset, 0, unroll=4)
    load_q.wait()
    pad = jnp.zeros((2 * half - draft, head_dim), dk.dtype)
    for a in range(rows):
        s = dot_t(q_of(first + a), jnp.concatenate([dk[a], pad], axis=0)) * inv_root
        s = jnp.where(causal, s, masked)
        drafted[a] = s
        peak[first + a] = s

    @pl.when(is_source)
    def _():
        loads[0].wait()
        loads[1].wait()

        def score(n, c):
            for u in range(UNROLL):
                i = n * UNROLL + u
                g = jnp.maximum(old_block[i], 0)
                r = owner[g]
                key = jnp.concatenate([vk[i], vok[i]], axis=0)
                s = dot_t(q_of(r), key) * inv_root
                s = jnp.where(place < live[g], s, masked)
                scores[i] = s
                peak[r] = jnp.maximum(peak[r], s)
            return c

        lax.fori_loop(0, slots // UNROLL, score, 0)

    def settle(r, c):
        peak[r] = jnp.broadcast_to(jnp.max(peak[r], axis=1, keepdims=True), (qrows, head_dim))
        total[r] = jnp.zeros((qrows, head_dim), jnp.float32)
        acc[r] = jnp.zeros((qrows, head_dim), jnp.float32)
        return c

    lax.fori_loop(0, requests, settle, 0, unroll=2)
    for a in range(rows):
        w = jnp.exp(drafted[a] - peak[first + a])
        total[first + a] = w
        acc[first + a] = jnp.dot(
            w.astype(dv.dtype),
            jnp.concatenate([dv[a], pad], axis=0),
            preferred_element_type=jnp.float32,
        )

    @pl.when(is_source)
    def _():
        loads[2].wait()
        loads[3].wait()

        def gather(n, c):
            for u in range(UNROLL):
                i = n * UNROLL + u
                r = owner[jnp.maximum(old_block[i], 0)]
                w = jnp.exp(scores[i] - peak[r])
                value = jnp.concatenate([vv[i], vov[i]], axis=0)
                out = jnp.dot(w.astype(vv.dtype), value, preferred_element_type=jnp.float32)
                total[r] += w
                acc[r] += out
            return c

        lax.fori_loop(0, slots // UNROLL, gather, 0)

    def finish(d, c):
        stat = jnp.zeros((qrows, head_dim), jnp.float32)
        for a in range(rows):
            r = d * rows + a
            l = jnp.sum(total[r], axis=1, keepdims=True)
            seen = l > 0
            safe = jnp.where(seen, l, 1.0)
            packet[d, a * qrows : (a + 1) * qrows, :] = (acc[r] / safe).astype(packet.dtype)
            level = jnp.where(seen, peak[r] + jnp.log(safe), masked)
            hi = level.astype(jnp.bfloat16).astype(jnp.float32)
            mid = (level - hi).astype(jnp.bfloat16).astype(jnp.float32)
            low = level - hi - mid
            stat = jnp.where(lane == 3 * a, hi, stat)
            stat = jnp.where(lane == 3 * a + 1, mid, stat)
            stat = jnp.where(lane == 3 * a + 2, low, stat)
        packet[d, rows * qrows :, :] = stat.astype(packet.dtype)
        return c

    lax.fori_loop(0, insts, finish, 0)


UNROLL = 4


def attend(old_block, lengths, meta, queries, keys, values, other_k, other_v, dk, dv, insts):
    requests, draft, width = queries.shape
    head_dim = keys.shape[2]
    qrows = draft * width // head_dim
    rows = requests // insts
    anyspace = pl.BlockSpec(memory_space=pl.ANY)
    smem = pl.BlockSpec(memory_space=pltpu.SMEM)
    vmem = pl.BlockSpec(memory_space=pltpu.VMEM)
    bf16 = jnp.bfloat16
    state = pltpu.VMEM((requests, qrows, head_dim), jnp.float32)
    return pl.pallas_call(
        attend_body,
        in_specs=[smem] * 3 + [anyspace] * 5 + [vmem] * 2,
        out_specs=vmem,
        out_shape=jax.ShapeDtypeStruct((insts, (rows + 1) * qrows, head_dim), bf16),
        scratch_shapes=[pltpu.VMEM(queries.shape, bf16)]
        + [pltpu.VMEM(keys.shape, bf16)] * 4
        + [
            pltpu.VMEM((keys.shape[0], qrows, head_dim), jnp.float32),
            pltpu.VMEM((rows, qrows, head_dim), jnp.float32),
            state,
            state,
            state,
            pltpu.SMEM((TOTAL,), jnp.int32),
            pltpu.SMEM((TOTAL,), jnp.int32),
            pltpu.SemaphoreType.DMA((5,)),
        ],
        name="attend",
    )(old_block, lengths, meta, queries, keys, values, other_k, other_v, dk, dv)


TOTAL = 256


def join_body(got, out):
    insts, _, head_dim = got.shape
    rows = out.shape[1]
    draft = out.shape[2]
    heads = out.shape[3] // head_dim
    qrows = draft * heads
    lane = lax.broadcasted_iota(jnp.int32, (qrows, head_dim), 1)
    stats = [got[s, rows * qrows :, :].astype(jnp.float32) for s in range(insts)]
    for a in range(rows):
        mine = (lane >= 3 * a) & (lane < 3 * a + 3)
        level = [
            jnp.sum(jnp.where(mine, stat, 0.0), axis=1, keepdims=True) for stat in stats
        ]
        top = level[0]
        for x in level[1:]:
            top = jnp.maximum(top, x)
        total = jnp.zeros((qrows, 1), jnp.float32)
        acc = jnp.zeros((qrows, head_dim), jnp.float32)
        for s in range(insts):
            share = jnp.exp(level[s] - top)
            total = total + share
            acc = acc + share * got[s, a * qrows : (a + 1) * qrows, :].astype(jnp.float32)
        res = (acc / total).astype(out.dtype)
        for d in range(insts):
            for h in range(heads):
                out[d, a, :, h * head_dim : (h + 1) * head_dim] = res[h * draft : (h + 1) * draft]


def join(got, rows, draft, width):
    insts = got.shape[0]
    vmem = pl.BlockSpec(memory_space=pltpu.VMEM)
    return pl.pallas_call(
        join_body,
        in_specs=[vmem],
        out_specs=vmem,
        out_shape=jax.ShapeDtypeStruct((insts, rows, draft, width), got.dtype),
        name="join",
    )(got)


def spread(x):
    return lax.all_to_all(x, "inst", split_axis=0, concat_axis=0, tiled=True)


def move_and_attend(
    old_keys, old_values, old_block, new_slot, lengths, queries, draft_keys, draft_values
):
    insts = lax.axis_size("inst")
    inst = lax.axis_index("inst")
    me_head = lax.axis_index("head")
    _, entries, half, head_dim = old_keys.shape
    keys = old_keys.reshape(-1, half, head_dim)
    values = old_values.reshape(-1, half, head_dim)
    blocks = new_slot.shape[0]
    requests = queries.shape[0]
    rows = requests // insts
    swap = [(i, i ^ 1) for i in range(lax.axis_size("head"))]
    other_k = lax.ppermute(keys, "head", swap)
    other_v = lax.ppermute(values, "head", swap)

    out_k, out_v = pack(old_block, new_slot, keys, values, inst, insts)
    queries, out_k, out_v = lax.optimization_barrier((queries, out_k, out_v))
    shape = (blocks // insts, entries, half, head_dim)
    far = across(out_v[0])
    from_left = right(out_k[0])
    from_right = left(out_k[1])
    near = across(out_v[1])

    kv_head = me_head // 2
    dk = lax.dynamic_slice_in_dim(draft_keys, kv_head * head_dim, head_dim, 2)
    dv = lax.dynamic_slice_in_dim(draft_values, kv_head * head_dim, head_dim, 2)
    meta = jnp.stack([inst * rows, me_head % 2 * half])
    packet = attend(
        old_block, lengths, meta, queries, keys, values, other_k, other_v, dk, dv, insts
    )
    packet, rest_k, rest_v = lax.optimization_barrier((packet, out_k[2:], out_v[2:]))
    moved_keys = move_keys(from_left, from_right, rest_k).reshape(shape)
    moved_values = move_values(far, near, rest_v).reshape(shape)
    got = spread(packet)
    mine = join(got, rows, queries.shape[1], queries.shape[2])
    attended = spread(mine).reshape(queries.shape)
    return moved_keys, moved_values, attended


def solution(mesh):
    placed = (
        P("inst", "head", None, None),
        P("inst", "head", None, None),
        P("inst"),
        P(),
        P(),
        P(None, None, "head"),
        P("inst", None, None),
        P("inst", None, None),
    )
    return jax.shard_map(
        move_and_attend,
        mesh=mesh,
        in_specs=placed,
        out_specs=(
            P("inst", "head", None, None),
            P("inst", "head", None, None),
            P(None, None, "head"),
        ),
        check_vma=False,
    )
```

```python
import math

import jax
import jax.numpy as jnp
from jax import lax
from jax.experimental import pallas as pl
from jax.experimental.pallas import tpu as pltpu
from jax.sharding import PartitionSpec as P


BLK = 128
masked = -1e30


COLS = 4


GROUPS_K = ((4, 3), (5, 6), (2,), (7,), (0,), (1,))
GROUPS_V = ((5, 3, 7), (1,), (4,), (2,), (6,), (0,))


def pack_body(old_block, new_slot, base, keys, values, *rest):
    count = len(GROUPS_K) + len(GROUPS_V)
    outs = rest[:count]
    vk, vv, zeros, origin, sems, load_sem = rest[count:]
    slots = keys.shape[0]
    total = new_slot.shape[0]
    per = zeros.shape[0]
    is_source = old_block[0] >= 0
    jobs = [(vk, out, group) for out, group in zip(outs, GROUPS_K)]
    jobs += [(vv, out, group) for out, group in zip(outs[len(GROUPS_K) :], GROUPS_V)]

    @pl.when(is_source)
    def _():
        load_k = pltpu.make_async_copy(keys, vk, load_sem.at[0])
        load_v = pltpu.make_async_copy(values, vv, load_sem.at[1])
        load_k.start()
        load_v.start()
        zeros[0] = jnp.zeros(zeros.shape[1:], zeros.dtype)

        def clear(t, c):
            origin[t] = -1
            return c

        lax.fori_loop(0, total, clear, 0, unroll=8)

        def note(i, c):
            origin[new_slot[jnp.maximum(old_block[i], 0)]] = i
            return c

        lax.fori_loop(0, slots, note, 0, unroll=8)
        load_k.wait()
        load_v.wait()
        for at, (cache, out, group) in enumerate(jobs):
            for g, p in enumerate(group):
                start = base[p]

                def send(j, c, cache=cache, out=out, at=at, g=g, start=start):
                    i = origin[start + j]

                    @pl.when(i >= 0)
                    def _():
                        pltpu.make_async_copy(cache.at[i], out.at[g * per + j], sems.at[at]).start()

                    @pl.when(i < 0)
                    def _():
                        pltpu.make_async_copy(zeros.at[0], out.at[g * per + j], sems.at[at]).start()

                    return c

                lax.fori_loop(0, per, send, 0, unroll=4)

    @pl.when(jnp.logical_not(is_source))
    def _():
        zeros[...] = jnp.zeros(zeros.shape, zeros.dtype)
        for at, (cache, out, group) in enumerate(jobs):
            for g in range(len(group)):
                pltpu.make_async_copy(zeros, out.at[pl.ds(g * per, per)], sems.at[at]).start()

    for at, (cache, out, group) in enumerate(jobs):
        pltpu.make_async_copy(out, out, sems.at[at]).wait()


def table_of(per, rows, half, head_dim):
    insts = lax.axis_size("inst")
    inst = lax.axis_index("inst")
    me_head = lax.axis_index("head")
    step = jnp.arange(16, dtype=jnp.int32)
    away = (inst // COLS) ^ (step % 2)
    column = (inst % COLS + step // 2) % COLS
    base = (away * COLS + column) * per
    rest = jnp.where(
        step == insts,
        inst * rows,
        jnp.where(step == insts + 1, me_head % 2 * half, me_head // 2 * head_dim),
    )
    return jnp.where(step < insts, base, rest)


def pack(old_block, new_slot, base, keys, values, insts):
    total = new_slot.shape[0]
    per = total // insts
    groups = GROUPS_K + GROUPS_V
    anyspace = pl.BlockSpec(memory_space=pl.ANY)
    smem = pl.BlockSpec(memory_space=pltpu.SMEM)
    got = pl.pallas_call(
        pack_body,
        in_specs=[smem, smem, smem, anyspace, anyspace],
        out_specs=[anyspace] * len(groups),
        out_shape=[
            jax.ShapeDtypeStruct((per * len(g),) + keys.shape[1:], keys.dtype) for g in groups
        ],
        scratch_shapes=[
            pltpu.VMEM(keys.shape, keys.dtype),
            pltpu.VMEM(keys.shape, keys.dtype),
            pltpu.VMEM((per,) + keys.shape[1:], keys.dtype),
            pltpu.SMEM((total,), jnp.int32),
            pltpu.SemaphoreType.DMA((len(groups),)),
            pltpu.SemaphoreType.DMA((2,)),
        ],
        name="pack",
    )(old_block, new_slot, base, keys, values)
    return got[: len(GROUPS_K)], got[len(GROUPS_K) :]


def right(x):
    rows = lax.axis_size("inst") // COLS
    route = [(r * COLS + c, r * COLS + (c + 1) % COLS) for r in range(rows) for c in range(COLS)]
    return lax.ppermute(x, "inst", route)


def left(x):
    rows = lax.axis_size("inst") // COLS
    route = [(r * COLS + (c + 1) % COLS, r * COLS + c) for r in range(rows) for c in range(COLS)]
    return lax.ppermute(x, "inst", route)


def across(x):
    return lax.ppermute(x, "inst", [(i, i ^ COLS) for i in range(lax.axis_size("inst"))])


def vmem_call(body, outs, *args):
    vmem = pl.BlockSpec(memory_space=pltpu.VMEM)
    return pl.pallas_call(
        body,
        in_specs=[vmem] * len(args),
        out_specs=[vmem] * len(outs),
        out_shape=[jax.ShapeDtypeStruct(shape, args[0].dtype) for shape in outs],
    )(*args)


def merge_keys_body(from_left, from_right, k1n, k3f, k0n, k0f, o_right, o_left, near, cross):
    per = k1n.shape[0]
    o_right[...] = k1n[...] + from_left[:per]
    o_left[...] = k3f[...] + from_right[:per]
    near[...] = k0n[...] + from_right[per:]
    cross[...] = k0f[...] + from_left[per:]


def move_keys(from_left, from_right, groups):
    piece = groups[0].shape
    o_right, o_left, near, cross = vmem_call(
        merge_keys_body, [piece] * 4, from_left, from_right, *groups
    )
    a2 = right(o_right)
    b2 = left(o_left)
    crossed = across(cross + b2)
    return near + a2 + crossed


def merge_values_body(far, v2n, v1n, v3n, o_right, o_left, low, high):
    per = v1n.shape[0]
    cut = per // 2
    o_right[:cut] = v2n[:cut] + far[:cut]
    o_left[:cut] = v2n[cut:] + far[cut:per]
    low[...] = v1n[:cut] + far[per : per + cut]
    o_right[cut:] = v1n[cut:] + far[per + cut : 2 * per]
    o_left[cut:] = v3n[:cut] + far[2 * per : 2 * per + cut]
    high[...] = v3n[cut:] + far[2 * per + cut :]


def second_body(low, high, from_left, from_right, o_right, o_left):
    cut = low.shape[0]
    o_right[...] = low[...] + from_left[:cut]
    o_left[...] = high[...] + from_right[:cut]


def move_values(got, y0, groups):
    v2n, v1n, v3n, v0n = groups
    cut = v1n.shape[0] // 2
    piece = v1n.shape
    part = (cut,) + piece[1:]
    o_right, o_left, low, high = vmem_call(
        merge_values_body, [piece, piece, part, part], got, v2n, v1n, v3n
    )
    from_left = right(o_right)
    from_right = left(o_left)
    o_right, o_left = vmem_call(second_body, [part, part], low, high, from_left, from_right)
    e_lo = right(o_right)
    g_hi = left(o_left)
    return v0n + y0 + jnp.concatenate([e_lo + from_right[cut:], from_left[cut:] + g_hi])


def dot_t(x, y):
    return lax.dot_general(x, y, (((1,), (1,)), ((), ())), preferred_element_type=jnp.float32)


def attend_body(
    old_block, lengths, meta, q, k, v, ok, ov, dks, dvs, packet,
    vq, dk, dv, vk, vv, vok, vov, scores, drafted, peak, total, acc, owner, live, sems,
):
    requests, draft, width = vq.shape
    head_dim = vk.shape[2]
    half = vk.shape[1]
    slots = vk.shape[0]
    heads = width // head_dim
    qrows = draft * heads
    insts = packet.shape[0]
    rows = requests // insts
    inv_root = 1.0 / math.sqrt(head_dim)
    is_source = old_block[0] >= 0
    first = meta[insts]
    shift = meta[insts + 1]
    kv = pl.ds(pl.multiple_of(meta[insts + 2], head_dim), head_dim)
    early = [
        pltpu.make_async_copy(q, vq, sems.at[0]),
        pltpu.make_async_copy(dks.at[:, :, kv], dk, sems.at[5]),
        pltpu.make_async_copy(dvs.at[:, :, kv], dv, sems.at[6]),
    ]
    for load in early:
        load.start()
    loads = [
        pltpu.make_async_copy(x, y, sems.at[1 + n])
        for n, (x, y) in enumerate(((k, vk), (ok, vok), (v, vv), (ov, vov)))
    ]

    @pl.when(is_source)
    def _():
        for load in loads:
            load.start()

        def per_request(r, g):
            size = lengths[r]

            def per_block(j, c):
                owner[g + j] = r
                live[g + j] = jnp.minimum(size - j * BLK, BLK)
                return c

            n = (size + BLK - 1) // BLK
            lax.fori_loop(0, n, per_block, 0)
            return g + n

        lax.fori_loop(0, requests, per_request, 0)

    def q_of(r):
        return jnp.concatenate(
            [vq[r, :, h * head_dim : (h + 1) * head_dim] for h in range(heads)], axis=0
        )

    lane = lax.broadcasted_iota(jnp.int32, (qrows, head_dim), 1)
    row = lax.broadcasted_iota(jnp.int32, (qrows, head_dim), 0)
    place = (lane + shift) % (2 * half)
    causal = lane <= row % draft
    blank = jnp.full((qrows, head_dim), masked, jnp.float32)

    def reset(r, c):
        peak[r] = blank
        return c

    lax.fori_loop(0, requests, reset, 0, unroll=4)
    for load in early:
        load.wait()
    pad = jnp.zeros((2 * half - draft, head_dim), dk.dtype)
    for a in range(rows):
        s = dot_t(q_of(first + a), jnp.concatenate([dk[a], pad], axis=0)) * inv_root
        s = jnp.where(causal, s, masked)
        drafted[a] = s
        peak[first + a] = s

    @pl.when(is_source)
    def _():
        loads[0].wait()
        loads[1].wait()

        def score(n, c):
            found = []
            for u in range(UNROLL):
                i = n * UNROLL + u
                g = jnp.maximum(old_block[i], 0)
                r = owner[g]
                key = jnp.concatenate([vk[i], vok[i]], axis=0)
                s = dot_t(q_of(r), key) * inv_root
                found.append((i, r, jnp.where(place < live[g], s, masked)))
            for i, r, s in found:
                scores[i] = s
                peak[r] = jnp.maximum(peak[r], s)
            return c

        lax.fori_loop(0, slots // UNROLL, score, 0)

    def settle(r, c):
        peak[r] = jnp.broadcast_to(jnp.max(peak[r], axis=1, keepdims=True), (qrows, head_dim))
        total[r] = jnp.zeros((qrows, head_dim), jnp.float32)
        acc[r] = jnp.zeros((qrows, head_dim), jnp.float32)
        return c

    lax.fori_loop(0, requests, settle, 0, unroll=SETTLE)
    for a in range(rows):
        w = jnp.exp(drafted[a] - peak[first + a])
        total[first + a] = w
        acc[first + a] = jnp.dot(
            w.astype(dv.dtype),
            jnp.concatenate([dv[a], pad], axis=0),
            preferred_element_type=jnp.float32,
        )

    @pl.when(is_source)
    def _():
        loads[2].wait()
        loads[3].wait()

        def gather(n, c):
            found = []
            for u in range(UNROLL):
                i = n * UNROLL + u
                r = owner[jnp.maximum(old_block[i], 0)]
                w = jnp.exp(scores[i] - peak[r])
                value = jnp.concatenate([vv[i], vov[i]], axis=0)
                out = jnp.dot(w.astype(vv.dtype), value, preferred_element_type=jnp.float32)
                found.append((r, w, out))
            for r, w, out in found:
                total[r] += w
                acc[r] += out
            return c

        lax.fori_loop(0, slots // UNROLL, gather, 0)

    def finish(d, c):
        sums = jnp.zeros((qrows, head_dim), jnp.float32)
        tops = jnp.zeros((qrows, head_dim), jnp.float32)
        for a in range(rows):
            r = d * rows + a
            l = jnp.sum(total[r], axis=1, keepdims=True)
            scale = 1.0 / jnp.where(l > 0, l, 1.0)
            packet[d, a * qrows : (a + 1) * qrows, :] = (acc[r] * scale).astype(packet.dtype)
            sums = jnp.where(lane % rows == a, l, sums)
            tops = jnp.where(lane % rows == a, peak[r], tops)
        level = jnp.where(sums > 0, tops + jnp.log(jnp.where(sums > 0, sums, 1.0)), masked)
        hi = level.astype(jnp.bfloat16).astype(jnp.float32)
        mid = (level - hi).astype(jnp.bfloat16).astype(jnp.float32)
        stat = jnp.where(lane < rows, hi, jnp.where(lane < 2 * rows, mid, level - hi - mid))
        packet[d, rows * qrows :, :] = stat.astype(packet.dtype)
        return c

    lax.fori_loop(0, insts, finish, 0)


UNROLL = 16
SETTLE = 16


def attend(old_block, lengths, meta, queries, keys, values, other_k, other_v, dk, dv, insts):
    requests, draft, width = queries.shape
    head_dim = keys.shape[2]
    qrows = draft * width // head_dim
    rows = requests // insts
    anyspace = pl.BlockSpec(memory_space=pl.ANY)
    smem = pl.BlockSpec(memory_space=pltpu.SMEM)
    vmem = pl.BlockSpec(memory_space=pltpu.VMEM)
    bf16 = jnp.bfloat16
    state = pltpu.VMEM((requests, qrows, head_dim), jnp.float32)
    return pl.pallas_call(
        attend_body,
        in_specs=[smem] * 3 + [anyspace] * 7,
        out_specs=vmem,
        out_shape=jax.ShapeDtypeStruct((insts, (rows + 1) * qrows, head_dim), bf16),
        scratch_shapes=[pltpu.VMEM(queries.shape, bf16)]
        + [pltpu.VMEM((rows, draft, head_dim), bf16)] * 2
        + [pltpu.VMEM(keys.shape, bf16)] * 4
        + [
            pltpu.VMEM((keys.shape[0], qrows, head_dim), jnp.float32),
            pltpu.VMEM((rows, qrows, head_dim), jnp.float32),
            state,
            state,
            state,
            pltpu.SMEM((TOTAL,), jnp.int32),
            pltpu.SMEM((TOTAL,), jnp.int32),
            pltpu.SemaphoreType.DMA((7,)),
        ],
        name="attend",
    )(old_block, lengths, meta, queries, keys, values, other_k, other_v, dk, dv)


TOTAL = 256


def join_body(got, out):
    insts, _, head_dim = got.shape
    rows = out.shape[1]
    draft = out.shape[2]
    heads = out.shape[3] // head_dim
    qrows = draft * heads
    lane = lax.broadcasted_iota(jnp.int32, (qrows, head_dim), 1)
    stats = [got[s, rows * qrows :, :].astype(jnp.float32) for s in range(insts)]
    for a in range(rows):
        mine = (lane % rows == a) & (lane < 3 * rows)
        level = [
            jnp.sum(jnp.where(mine, stat, 0.0), axis=1, keepdims=True) for stat in stats
        ]
        top = level[0]
        for x in level[1:]:
            top = jnp.maximum(top, x)
        total = jnp.zeros((qrows, 1), jnp.float32)
        acc = jnp.zeros((qrows, head_dim), jnp.float32)
        for s in range(insts):
            share = jnp.exp(level[s] - top)
            total = total + share
            acc = acc + share * got[s, a * qrows : (a + 1) * qrows, :].astype(jnp.float32)
        res = (acc / total).astype(out.dtype)
        for d in range(insts):
            for h in range(heads):
                out[d, a, :, h * head_dim : (h + 1) * head_dim] = res[h * draft : (h + 1) * draft]


def join(got, rows, draft, width):
    insts = got.shape[0]
    vmem = pl.BlockSpec(memory_space=pltpu.VMEM)
    return pl.pallas_call(
        join_body,
        in_specs=[vmem],
        out_specs=vmem,
        out_shape=jax.ShapeDtypeStruct((insts, rows, draft, width), got.dtype),
        name="join",
    )(got)


def spread(x):
    return lax.all_to_all(x, "inst", split_axis=0, concat_axis=0, tiled=True)


def move_and_attend(
    old_keys, old_values, old_block, new_slot, lengths, queries, draft_keys, draft_values
):
    insts = lax.axis_size("inst")
    _, entries, half, head_dim = old_keys.shape
    keys = old_keys.reshape(-1, half, head_dim)
    values = old_values.reshape(-1, half, head_dim)
    blocks = new_slot.shape[0]
    requests = queries.shape[0]
    rows = requests // insts
    swap = [(i, i ^ 1) for i in range(lax.axis_size("head"))]
    other_k = lax.ppermute(keys, "head", swap)
    other_v = lax.ppermute(values, "head", swap)

    table = table_of(blocks // insts, rows, half, head_dim)
    out_k, out_v = pack(old_block, new_slot, table, keys, values, insts)
    queries, out_k, out_v = lax.optimization_barrier((queries, out_k, out_v))
    shape = (blocks // insts, entries, half, head_dim)
    far = across(out_v[0])
    from_left = right(out_k[0])
    from_right = left(out_k[1])
    near = across(out_v[1])

    packet = attend(
        old_block, lengths, table, queries, keys, values, other_k, other_v,
        draft_keys, draft_values, insts,
    )
    packet, rest_k, rest_v = lax.optimization_barrier((packet, out_k[2:], out_v[2:]))
    moved_keys = move_keys(from_left, from_right, rest_k).reshape(shape)
    moved_values = move_values(far, near, rest_v).reshape(shape)
    got = spread(packet)
    mine = join(got, rows, queries.shape[1], queries.shape[2])
    attended = spread(mine).reshape(queries.shape)
    return moved_keys, moved_values, attended


def solution(mesh):
    placed = (
        P("inst", "head", None, None),
        P("inst", "head", None, None),
        P("inst"),
        P(),
        P(),
        P(None, None, "head"),
        P("inst", None, None),
        P("inst", None, None),
    )
    return jax.shard_map(
        move_and_attend,
        mesh=mesh,
        in_specs=placed,
        out_specs=(
            P("inst", "head", None, None),
            P("inst", "head", None, None),
            P(None, None, "head"),
        ),
        check_vma=False,
    )
```

```python
import math

import jax
import jax.numpy as jnp
from jax import lax
from jax.experimental import pallas as pl
from jax.experimental.pallas import tpu as pltpu
from jax.sharding import PartitionSpec as P


BLK = 128
masked = -1e30


COLS = 4
GROUPS_K = ((4, 3), (5, 6), (2,), (7,), (0,), (1,))
GROUPS_V = ((5,), (3, 7), (1,), (4,), (2,), (6,), (0,))


def pack_body(old_block, new_slot, base, keys, values, *rest):
    count = len(GROUPS_K) + len(GROUPS_V)
    outs = rest[:count]
    vk, vv, zeros, origin, sems, load_sem = rest[count:]
    slots = keys.shape[0]
    total = new_slot.shape[0]
    per = zeros.shape[0]
    is_source = old_block[0] >= 0
    jobs = [(vk, out, group) for out, group in zip(outs, GROUPS_K)]
    jobs += [(vv, out, group) for out, group in zip(outs[len(GROUPS_K) :], GROUPS_V)]

    @pl.when(is_source)
    def _():
        load_k = pltpu.make_async_copy(keys, vk, load_sem.at[0])
        load_v = pltpu.make_async_copy(values, vv, load_sem.at[1])
        load_k.start()
        load_v.start()
        zeros[0] = jnp.zeros(zeros.shape[1:], zeros.dtype)

        def clear(t, c):
            origin[t] = -1
            return c

        lax.fori_loop(0, total, clear, 0, unroll=8)

        def note(i, c):
            origin[new_slot[jnp.maximum(old_block[i], 0)]] = i
            return c

        lax.fori_loop(0, slots, note, 0, unroll=8)
        load_k.wait()
        load_v.wait()
        for at, (cache, out, group) in enumerate(jobs):
            for g, p in enumerate(group):
                start = base[p]

                def send(j, c, cache=cache, out=out, at=at, g=g, start=start):
                    i = origin[start + j]

                    @pl.when(i >= 0)
                    def _():
                        pltpu.make_async_copy(cache.at[i], out.at[g * per + j], sems.at[at]).start()

                    @pl.when(i < 0)
                    def _():
                        pltpu.make_async_copy(zeros.at[0], out.at[g * per + j], sems.at[at]).start()

                    return c

                lax.fori_loop(0, per, send, 0, unroll=4)

    @pl.when(jnp.logical_not(is_source))
    def _():
        zeros[...] = jnp.zeros(zeros.shape, zeros.dtype)
        for at, (cache, out, group) in enumerate(jobs):
            for g in range(len(group)):
                pltpu.make_async_copy(zeros, out.at[pl.ds(g * per, per)], sems.at[at]).start()

    for at, (cache, out, group) in enumerate(jobs):
        pltpu.make_async_copy(out, out, sems.at[at]).wait()


def table_of(per, rows, half, head_dim):
    insts = lax.axis_size("inst")
    inst = lax.axis_index("inst")
    me_head = lax.axis_index("head")
    step = jnp.arange(16, dtype=jnp.int32)
    away = (inst // COLS) ^ (step % 2)
    column = (inst % COLS + step // 2) % COLS
    base = (away * COLS + column) * per
    rest = jnp.where(
        step == insts,
        inst * rows,
        jnp.where(step == insts + 1, me_head % 2 * half, me_head // 2 * head_dim),
    )
    return jnp.where(step < insts, base, rest)


def pack(old_block, new_slot, base, keys, values, insts):
    total = new_slot.shape[0]
    per = total // insts
    groups = GROUPS_K + GROUPS_V
    anyspace = pl.BlockSpec(memory_space=pl.ANY)
    smem = pl.BlockSpec(memory_space=pltpu.SMEM)
    got = pl.pallas_call(
        pack_body,
        in_specs=[smem, smem, smem, anyspace, anyspace],
        out_specs=[anyspace] * len(groups),
        out_shape=[
            jax.ShapeDtypeStruct((per * len(g),) + keys.shape[1:], keys.dtype) for g in groups
        ],
        scratch_shapes=[
            pltpu.VMEM(keys.shape, keys.dtype),
            pltpu.VMEM(keys.shape, keys.dtype),
            pltpu.VMEM((per,) + keys.shape[1:], keys.dtype),
            pltpu.SMEM((total,), jnp.int32),
            pltpu.SemaphoreType.DMA((len(groups),)),
            pltpu.SemaphoreType.DMA((2,)),
        ],
        name="pack",
    )(old_block, new_slot, base, keys, values)
    return got[: len(GROUPS_K)], got[len(GROUPS_K) :]


def right(x):
    rows = lax.axis_size("inst") // COLS
    route = [(r * COLS + c, r * COLS + (c + 1) % COLS) for r in range(rows) for c in range(COLS)]
    return lax.ppermute(x, "inst", route)


def left(x):
    rows = lax.axis_size("inst") // COLS
    route = [(r * COLS + (c + 1) % COLS, r * COLS + c) for r in range(rows) for c in range(COLS)]
    return lax.ppermute(x, "inst", route)


def across(x):
    return lax.ppermute(x, "inst", [(i, i ^ COLS) for i in range(lax.axis_size("inst"))])


def add_call(sums, split=None):
    per = sums[0][0][0].shape[0]
    tail = sums[0][0][0].shape[1:]
    step = per // 4
    steps = per // step
    args = [x for terms in sums for x, _ in terms]
    where = [
        pl.BlockSpec((step,) + tail, lambda i, at=first // step: (i + at, 0, 0))
        for terms in sums
        for _, first in terms
    ]
    if split:
        args += split
        where += [
            pl.BlockSpec((step,) + tail, lambda i: (jnp.minimum(i, steps // 2 - 1), 0, 0)),
            pl.BlockSpec((step,) + tail, lambda i: (jnp.maximum(i - steps // 2, 0), 0, 0)),
        ]

    def body(*refs):
        i = pl.program_id(0)
        outs = refs[len(args) :]
        at = 0
        for terms, out in zip(sums, outs):
            value = refs[at][...]
            for n in range(1, len(terms)):
                value = value + refs[at + n][...]
            at += len(terms)
            out[...] = value
        if split:

            @pl.when(i < steps // 2)
            def _():
                outs[0][...] += refs[at][...]

            @pl.when(i >= steps // 2)
            def _():
                outs[1][...] += refs[at + 1][...]

    return pl.pallas_call(
        body,
        grid=(steps,),
        in_specs=where,
        out_specs=[pl.BlockSpec((step,) + tail, lambda i: (i, 0, 0))] * len(sums),
        out_shape=[jax.ShapeDtypeStruct((per,) + tail, args[0].dtype)] * len(sums),
    )(*args)


def move_keys(from_left, from_right, groups):
    k1n, k3f, k0n, k0f = groups
    per = k1n.shape[0]
    o_right, o_left = add_call([[(k1n, 0), (from_left, 0)], [(k3f, 0), (from_right, 0)]])
    a2 = right(o_right)
    b2 = left(o_left)
    crossed = across(k0f + from_left[per:] + b2)
    return k0n + from_right[per:] + a2 + crossed


def move_values(got2, got, y0, groups):
    v2n, v1n, v3n, v0n = groups
    per = v1n.shape[0]
    cut = per // 2
    from_left = right(v2n[:cut] + got2[:cut])
    from_right = left(v2n[cut:] + got2[cut:])
    o_right, o_left = add_call(
        [[(v1n, 0), (got, 0)], [(v3n, 0), (got, per)]], [from_left, from_right]
    )
    a2 = right(o_right)
    b2 = left(o_left)
    return v0n + y0 + a2 + b2


def dot_t(x, y):
    return lax.dot_general(x, y, (((1,), (1,)), ((), ())), preferred_element_type=jnp.float32)


def attend_body(
    old_block, lengths, meta, q, k, v, ok, ov, dks, dvs, packet,
    vq, dk, dv, vk, vv, vok, vov, scores, drafted, peak, total, acc, owner, live, sems,
):
    requests, draft, width = vq.shape
    head_dim = vk.shape[2]
    half = vk.shape[1]
    slots = vk.shape[0]
    heads = width // head_dim
    qrows = draft * heads
    insts = packet.shape[0]
    rows = requests // insts
    inv_root = 1.0 / math.sqrt(head_dim)
    is_source = old_block[0] >= 0
    first = meta[insts]
    shift = meta[insts + 1]
    kv = pl.ds(pl.multiple_of(meta[insts + 2], head_dim), head_dim)
    early = [
        pltpu.make_async_copy(q, vq, sems.at[0]),
        pltpu.make_async_copy(dks.at[:, :, kv], dk, sems.at[5]),
        pltpu.make_async_copy(dvs.at[:, :, kv], dv, sems.at[6]),
    ]
    for load in early:
        load.start()
    loads = [
        pltpu.make_async_copy(x, y, sems.at[1 + n])
        for n, (x, y) in enumerate(((k, vk), (ok, vok), (v, vv), (ov, vov)))
    ]

    @pl.when(is_source)
    def _():
        for load in loads:
            load.start()

        def per_request(r, g):
            size = lengths[r]

            def per_block(j, c):
                owner[g + j] = r
                live[g + j] = jnp.minimum(size - j * BLK, BLK)
                return c

            n = (size + BLK - 1) // BLK
            lax.fori_loop(0, n, per_block, 0)
            return g + n

        lax.fori_loop(0, requests, per_request, 0)

    def q_of(r):
        return jnp.concatenate(
            [vq[r, :, h * head_dim : (h + 1) * head_dim] for h in range(heads)], axis=0
        )

    lane = lax.broadcasted_iota(jnp.int32, (qrows, head_dim), 1)
    row = lax.broadcasted_iota(jnp.int32, (qrows, head_dim), 0)
    place = (lane + shift) % (2 * half)
    causal = lane <= row % draft
    blank = jnp.full((qrows, head_dim), masked, jnp.float32)

    def reset(r, c):
        peak[r] = blank
        return c

    lax.fori_loop(0, requests, reset, 0, unroll=4)
    for load in early:
        load.wait()
    pad = jnp.zeros((2 * half - draft, head_dim), dk.dtype)
    for a in range(rows):
        s = dot_t(q_of(first + a), jnp.concatenate([dk[a], pad], axis=0)) * inv_root
        s = jnp.where(causal, s, masked)
        drafted[a] = s
        peak[first + a] = s

    @pl.when(is_source)
    def _():
        loads[0].wait()
        loads[1].wait()

        def score(n, c):
            found = []
            for u in range(UNROLL):
                i = n * UNROLL + u
                g = jnp.maximum(old_block[i], 0)
                r = owner[g]
                key = jnp.concatenate([vk[i], vok[i]], axis=0)
                s = dot_t(q_of(r), key) * inv_root
                found.append((i, r, jnp.where(place < live[g], s, masked)))
            for i, r, s in found:
                scores[i] = s
                peak[r] = jnp.maximum(peak[r], s)
            return c

        lax.fori_loop(0, slots // UNROLL, score, 0)

    def settle(r, c):
        peak[r] = jnp.broadcast_to(jnp.max(peak[r], axis=1, keepdims=True), (qrows, head_dim))
        total[r] = jnp.zeros((qrows, head_dim), jnp.float32)
        acc[r] = jnp.zeros((qrows, head_dim), jnp.float32)
        return c

    lax.fori_loop(0, requests, settle, 0, unroll=SETTLE)
    for a in range(rows):
        w = jnp.exp(drafted[a] - peak[first + a])
        total[first + a] = w
        acc[first + a] = jnp.dot(
            w.astype(dv.dtype),
            jnp.concatenate([dv[a], pad], axis=0),
            preferred_element_type=jnp.float32,
        )

    @pl.when(is_source)
    def _():
        loads[2].wait()
        loads[3].wait()

        def gather(n, c):
            found = []
            for u in range(UNROLL):
                i = n * UNROLL + u
                r = owner[jnp.maximum(old_block[i], 0)]
                w = jnp.exp(scores[i] - peak[r])
                value = jnp.concatenate([vv[i], vov[i]], axis=0)
                out = jnp.dot(w.astype(vv.dtype), value, preferred_element_type=jnp.float32)
                found.append((r, w, out))
            for r, w, out in found:
                total[r] += w
                acc[r] += out
            return c

        lax.fori_loop(0, slots // UNROLL, gather, 0)

    def finish(d, c):
        sums = jnp.zeros((qrows, head_dim), jnp.float32)
        tops = jnp.zeros((qrows, head_dim), jnp.float32)
        for a in range(rows):
            r = d * rows + a
            l = jnp.sum(total[r], axis=1, keepdims=True)
            scale = 1.0 / jnp.where(l > 0, l, 1.0)
            packet[d, a * qrows : (a + 1) * qrows, :] = (acc[r] * scale).astype(packet.dtype)
            sums = jnp.where(lane % rows == a, l, sums)
            tops = jnp.where(lane % rows == a, peak[r], tops)
        level = jnp.where(sums > 0, tops + jnp.log(jnp.where(sums > 0, sums, 1.0)), masked)
        hi = level.astype(jnp.bfloat16).astype(jnp.float32)
        mid = (level - hi).astype(jnp.bfloat16).astype(jnp.float32)
        stat = jnp.where(lane < rows, hi, jnp.where(lane < 2 * rows, mid, level - hi - mid))
        packet[d, rows * qrows :, :] = stat.astype(packet.dtype)
        return c

    lax.fori_loop(0, insts, finish, 0)


UNROLL = 16
SETTLE = 16


def attend(old_block, lengths, meta, queries, keys, values, other_k, other_v, dk, dv, insts):
    requests, draft, width = queries.shape
    head_dim = keys.shape[2]
    qrows = draft * width // head_dim
    rows = requests // insts
    anyspace = pl.BlockSpec(memory_space=pl.ANY)
    smem = pl.BlockSpec(memory_space=pltpu.SMEM)
    vmem = pl.BlockSpec(memory_space=pltpu.VMEM)
    bf16 = jnp.bfloat16
    state = pltpu.VMEM((requests, qrows, head_dim), jnp.float32)
    return pl.pallas_call(
        attend_body,
        in_specs=[smem] * 3 + [anyspace] * 7,
        out_specs=vmem,
        out_shape=jax.ShapeDtypeStruct((insts, (rows + 1) * qrows, head_dim), bf16),
        scratch_shapes=[pltpu.VMEM(queries.shape, bf16)]
        + [pltpu.VMEM((rows, draft, head_dim), bf16)] * 2
        + [pltpu.VMEM(keys.shape, bf16)] * 4
        + [
            pltpu.VMEM((keys.shape[0], qrows, head_dim), jnp.float32),
            pltpu.VMEM((rows, qrows, head_dim), jnp.float32),
            state,
            state,
            state,
            pltpu.SMEM((TOTAL,), jnp.int32),
            pltpu.SMEM((TOTAL,), jnp.int32),
            pltpu.SemaphoreType.DMA((7,)),
        ],
        name="attend",
    )(old_block, lengths, meta, queries, keys, values, other_k, other_v, dk, dv)


TOTAL = 256


def join_body(got, out):
    insts, _, head_dim = got.shape
    rows = out.shape[1]
    draft = out.shape[2]
    heads = out.shape[3] // head_dim
    qrows = draft * heads
    lane = lax.broadcasted_iota(jnp.int32, (qrows, head_dim), 1)
    stats = [got[s, rows * qrows :, :].astype(jnp.float32) for s in range(insts)]
    for a in range(rows):
        mine = (lane % rows == a) & (lane < 3 * rows)
        level = [
            jnp.sum(jnp.where(mine, stat, 0.0), axis=1, keepdims=True) for stat in stats
        ]
        top = level[0]
        for x in level[1:]:
            top = jnp.maximum(top, x)
        total = jnp.zeros((qrows, 1), jnp.float32)
        acc = jnp.zeros((qrows, head_dim), jnp.float32)
        for s in range(insts):
            share = jnp.exp(level[s] - top)
            total = total + share
            acc = acc + share * got[s, a * qrows : (a + 1) * qrows, :].astype(jnp.float32)
        res = (acc / total).astype(out.dtype)
        for d in range(insts):
            for h in range(heads):
                out[d, a, :, h * head_dim : (h + 1) * head_dim] = res[h * draft : (h + 1) * draft]


def join(got, rows, draft, width):
    insts = got.shape[0]
    vmem = pl.BlockSpec(memory_space=pltpu.VMEM)
    return pl.pallas_call(
        join_body,
        in_specs=[vmem],
        out_specs=vmem,
        out_shape=jax.ShapeDtypeStruct((insts, rows, draft, width), got.dtype),
        name="join",
    )(got)


def spread(x):
    return lax.all_to_all(x, "inst", split_axis=0, concat_axis=0, tiled=True)


def move_and_attend(
    old_keys, old_values, old_block, new_slot, lengths, queries, draft_keys, draft_values
):
    insts = lax.axis_size("inst")
    _, entries, half, head_dim = old_keys.shape
    keys = old_keys.reshape(-1, half, head_dim)
    values = old_values.reshape(-1, half, head_dim)
    blocks = new_slot.shape[0]
    requests = queries.shape[0]
    rows = requests // insts
    swap = [(i, i ^ 1) for i in range(lax.axis_size("head"))]
    other_k = lax.ppermute(keys, "head", swap)
    other_v = lax.ppermute(values, "head", swap)

    table = table_of(blocks // insts, rows, half, head_dim)
    out_k, out_v = pack(old_block, new_slot, table, keys, values, insts)
    queries, out_k, out_v = lax.optimization_barrier((queries, out_k, out_v))
    shape = (blocks // insts, entries, half, head_dim)
    far2 = across(out_v[0])
    from_left = right(out_k[0])
    from_right = left(out_k[1])
    far = across(out_v[1])
    near = across(out_v[2])
    packet = attend(
        old_block, lengths, table, queries, keys, values, other_k, other_v,
        draft_keys, draft_values, insts,
    )
    packet, rest_k, rest_v = lax.optimization_barrier((packet, out_k[2:], out_v[3:]))
    moved_keys = move_keys(from_left, from_right, rest_k).reshape(shape)
    moved_values = move_values(far2, far, near, rest_v).reshape(shape)
    got = spread(packet)
    mine = join(got, rows, queries.shape[1], queries.shape[2])
    attended = spread(mine).reshape(queries.shape)
    return moved_keys, moved_values, attended


def solution(mesh):
    placed = (
        P("inst", "head", None, None),
        P("inst", "head", None, None),
        P("inst"),
        P(),
        P(),
        P(None, None, "head"),
        P("inst", None, None),
        P("inst", None, None),
    )
    return jax.shard_map(
        move_and_attend,
        mesh=mesh,
        in_specs=placed,
        out_specs=(
            P("inst", "head", None, None),
            P("inst", "head", None, None),
            P(None, None, "head"),
        ),
        check_vma=False,
    )
```

```python
import functools
import math

import jax
import jax.numpy as jnp
from jax import lax
from jax.experimental import pallas as pl
from jax.experimental.pallas import tpu as pltpu
from jax.sharding import PartitionSpec as P


BLK = 128
masked = -1e30


COLS = 4
SENT_K = ((4, 3), (5, 6))
SENT_V = ((5,), (3, 7))
KEPT_K = ((2,), (7,), (0,), (1,))
KEPT_V = ((1,), (4,), (2,), (6,), (0,))


def pack_body(groups_k, groups_v, old_block, new_slot, base, keys, values, *rest):
    count = len(groups_k) + len(groups_v)
    outs = rest[:count]
    vk, vv, zeros, origin, sems, load_sem = rest[count:]
    slots = keys.shape[0]
    total = new_slot.shape[0]
    per = zeros.shape[0]
    is_source = old_block[0] >= 0
    jobs = [(vk, out, group) for out, group in zip(outs, groups_k)]
    jobs += [(vv, out, group) for out, group in zip(outs[len(groups_k) :], groups_v)]

    @pl.when(is_source)
    def _():
        load_k = pltpu.make_async_copy(keys, vk, load_sem.at[0])
        load_v = pltpu.make_async_copy(values, vv, load_sem.at[1])
        load_k.start()
        load_v.start()
        zeros[0] = jnp.zeros(zeros.shape[1:], zeros.dtype)

        def clear(t, c):
            origin[t] = -1
            return c

        lax.fori_loop(0, total, clear, 0, unroll=8)

        def note(i, c):
            origin[new_slot[jnp.maximum(old_block[i], 0)]] = i
            return c

        lax.fori_loop(0, slots, note, 0, unroll=8)
        load_k.wait()
        load_v.wait()
        for at, (cache, out, group) in enumerate(jobs):
            for g, p in enumerate(group):
                start = base[p]

                def send(j, c, cache=cache, out=out, at=at, g=g, start=start):
                    i = origin[start + j]

                    @pl.when(i >= 0)
                    def _():
                        pltpu.make_async_copy(cache.at[i], out.at[g * per + j], sems.at[at]).start()

                    @pl.when(i < 0)
                    def _():
                        pltpu.make_async_copy(zeros.at[0], out.at[g * per + j], sems.at[at]).start()

                    return c

                lax.fori_loop(0, per, send, 0, unroll=4)

    @pl.when(jnp.logical_not(is_source))
    def _():
        zeros[...] = jnp.zeros(zeros.shape, zeros.dtype)
        for at, (cache, out, group) in enumerate(jobs):
            for g in range(len(group)):
                pltpu.make_async_copy(zeros, out.at[pl.ds(g * per, per)], sems.at[at]).start()

    for at, (cache, out, group) in enumerate(jobs):
        pltpu.make_async_copy(out, out, sems.at[at]).wait()


def table_of(per, rows, half, head_dim):
    insts = lax.axis_size("inst")
    inst = lax.axis_index("inst")
    me_head = lax.axis_index("head")
    step = jnp.arange(16, dtype=jnp.int32)
    away = (inst // COLS) ^ (step % 2)
    column = (inst % COLS + step // 2) % COLS
    base = (away * COLS + column) * per
    rest = jnp.where(
        step == insts,
        inst * rows,
        jnp.where(step == insts + 1, me_head % 2 * half, me_head // 2 * head_dim),
    )
    return jnp.where(step < insts, base, rest)


def pack(old_block, new_slot, base, keys, values, insts, groups_k, groups_v):
    total = new_slot.shape[0]
    per = total // insts
    groups = groups_k + groups_v
    anyspace = pl.BlockSpec(memory_space=pl.ANY)
    smem = pl.BlockSpec(memory_space=pltpu.SMEM)
    got = pl.pallas_call(
        functools.partial(pack_body, groups_k, groups_v),
        in_specs=[smem, smem, smem, anyspace, anyspace],
        out_specs=[anyspace] * len(groups),
        out_shape=[
            jax.ShapeDtypeStruct((per * len(g),) + keys.shape[1:], keys.dtype) for g in groups
        ],
        scratch_shapes=[
            pltpu.VMEM(keys.shape, keys.dtype),
            pltpu.VMEM(keys.shape, keys.dtype),
            pltpu.VMEM((per,) + keys.shape[1:], keys.dtype),
            pltpu.SMEM((total,), jnp.int32),
            pltpu.SemaphoreType.DMA((len(groups),)),
            pltpu.SemaphoreType.DMA((2,)),
        ],
    )(old_block, new_slot, base, keys, values)
    return got[: len(groups_k)], got[len(groups_k) :]


def right(x):
    rows = lax.axis_size("inst") // COLS
    route = [(r * COLS + c, r * COLS + (c + 1) % COLS) for r in range(rows) for c in range(COLS)]
    return lax.ppermute(x, "inst", route)


def left(x):
    rows = lax.axis_size("inst") // COLS
    route = [(r * COLS + (c + 1) % COLS, r * COLS + c) for r in range(rows) for c in range(COLS)]
    return lax.ppermute(x, "inst", route)


def across(x):
    return lax.ppermute(x, "inst", [(i, i ^ COLS) for i in range(lax.axis_size("inst"))])


def move_keys(from_left, from_right, groups):
    k1n, k3f, k0n, k0f = groups
    per = k1n.shape[0]
    a2 = right(k1n + from_left[:per])
    b2 = left(k3f + from_right[:per])
    b2, from_left = lax.optimization_barrier((b2, from_left))
    crossed = across(k0f + from_left[per:] + b2)
    return k0n + from_right[per:] + a2 + crossed


def move_values(got2, got, y0, groups):
    v2n, v1n, v3n, v0n = groups
    per = v1n.shape[0]
    cut = per // 2
    from_left = right(v2n[:cut] + got2[:cut])
    from_right = left(v2n[cut:] + got2[cut:])
    rest = jnp.zeros((per - cut,) + v1n.shape[1:], v1n.dtype)
    a2 = right(v1n + got[:per] + jnp.concatenate([from_left, rest]))
    b2 = left(v3n + got[per:] + jnp.concatenate([rest, from_right]))
    return v0n + y0 + a2 + b2


def dot_t(x, y):
    return lax.dot_general(x, y, (((1,), (1,)), ((), ())), preferred_element_type=jnp.float32)


def attend_body(
    old_block, lengths, meta, q, k, v, ok, ov, dks, dvs, packet,
    vq, dk, dv, vk, vv, vok, vov, scores, drafted, peak, total, acc, owner, live, sems,
):
    requests, draft, width = vq.shape
    head_dim = vk.shape[2]
    half = vk.shape[1]
    slots = vk.shape[0]
    heads = width // head_dim
    qrows = draft * heads
    insts = packet.shape[0]
    rows = requests // insts
    inv_root = 1.0 / math.sqrt(head_dim)
    is_source = old_block[0] >= 0
    first = meta[insts]
    shift = meta[insts + 1]
    kv = pl.ds(pl.multiple_of(meta[insts + 2], head_dim), head_dim)
    early = [
        pltpu.make_async_copy(q, vq, sems.at[0]),
        pltpu.make_async_copy(dks.at[:, :, kv], dk, sems.at[5]),
        pltpu.make_async_copy(dvs.at[:, :, kv], dv, sems.at[6]),
    ]
    for load in early:
        load.start()
    loads = [
        pltpu.make_async_copy(x, y, sems.at[1 + n])
        for n, (x, y) in enumerate(((k, vk), (ok, vok), (v, vv), (ov, vov)))
    ]

    @pl.when(is_source)
    def _():
        for load in loads:
            load.start()

        def per_request(r, g):
            size = lengths[r]

            def per_block(j, c):
                owner[g + j] = r
                live[g + j] = jnp.minimum(size - j * BLK, BLK)
                return c

            n = (size + BLK - 1) // BLK
            lax.fori_loop(0, n, per_block, 0)
            return g + n

        lax.fori_loop(0, requests, per_request, 0)

    def q_of(r):
        return jnp.concatenate(
            [vq[r, :, h * head_dim : (h + 1) * head_dim] for h in range(heads)], axis=0
        )

    lane = lax.broadcasted_iota(jnp.int32, (qrows, head_dim), 1)
    row = lax.broadcasted_iota(jnp.int32, (qrows, head_dim), 0)
    place = (lane + shift) % (2 * half)
    causal = lane <= row % draft
    blank = jnp.full((qrows, head_dim), masked, jnp.float32)

    def reset(r, c):
        peak[r] = blank
        return c

    lax.fori_loop(0, requests, reset, 0, unroll=4)
    for load in early:
        load.wait()
    pad = jnp.zeros((2 * half - draft, head_dim), dk.dtype)
    for a in range(rows):
        s = dot_t(q_of(first + a), jnp.concatenate([dk[a], pad], axis=0)) * inv_root
        s = jnp.where(causal, s, masked)
        drafted[a] = s
        peak[first + a] = s

    @pl.when(is_source)
    def _():
        loads[0].wait()
        loads[1].wait()

        def score(n, c):
            found = []
            for u in range(UNROLL):
                i = n * UNROLL + u
                g = jnp.maximum(old_block[i], 0)
                r = owner[g]
                key = jnp.concatenate([vk[i], vok[i]], axis=0)
                s = dot_t(q_of(r), key) * inv_root
                found.append((i, r, jnp.where(place < live[g], s, masked)))
            for i, r, s in found:
                scores[i] = s
                peak[r] = jnp.maximum(peak[r], s)
            return c

        lax.fori_loop(0, slots // UNROLL, score, 0)

    def settle(r, c):
        peak[r] = jnp.broadcast_to(jnp.max(peak[r], axis=1, keepdims=True), (qrows, head_dim))
        total[r] = jnp.zeros((qrows, head_dim), jnp.float32)
        acc[r] = jnp.zeros((qrows, head_dim), jnp.float32)
        return c

    lax.fori_loop(0, requests, settle, 0, unroll=SETTLE)
    for a in range(rows):
        w = jnp.exp(drafted[a] - peak[first + a])
        total[first + a] = w
        acc[first + a] = jnp.dot(
            w.astype(dv.dtype),
            jnp.concatenate([dv[a], pad], axis=0),
            preferred_element_type=jnp.float32,
        )

    @pl.when(is_source)
    def _():
        loads[2].wait()
        loads[3].wait()

        def gather(n, c):
            found = []
            for u in range(UNROLL):
                i = n * UNROLL + u
                r = owner[jnp.maximum(old_block[i], 0)]
                w = jnp.exp(scores[i] - peak[r])
                value = jnp.concatenate([vv[i], vov[i]], axis=0)
                out = jnp.dot(w.astype(vv.dtype), value, preferred_element_type=jnp.float32)
                found.append((r, w, out))
            for r, w, out in found:
                total[r] += w
                acc[r] += out
            return c

        lax.fori_loop(0, slots // UNROLL, gather, 0)

    def finish(d, c):
        sums = jnp.zeros((qrows, head_dim), jnp.float32)
        tops = jnp.zeros((qrows, head_dim), jnp.float32)
        for a in range(rows):
            r = d * rows + a
            l = jnp.sum(total[r], axis=1, keepdims=True)
            scale = 1.0 / jnp.where(l > 0, l, 1.0)
            packet[d, a * qrows : (a + 1) * qrows, :] = (acc[r] * scale).astype(packet.dtype)
            sums = jnp.where(lane % rows == a, l, sums)
            tops = jnp.where(lane % rows == a, peak[r], tops)
        level = jnp.where(sums > 0, tops + jnp.log(jnp.where(sums > 0, sums, 1.0)), masked)
        hi = level.astype(jnp.bfloat16).astype(jnp.float32)
        mid = (level - hi).astype(jnp.bfloat16).astype(jnp.float32)
        stat = jnp.where(lane < rows, hi, jnp.where(lane < 2 * rows, mid, level - hi - mid))
        packet[d, rows * qrows :, :] = stat.astype(packet.dtype)
        return c

    lax.fori_loop(0, insts, finish, 0)


UNROLL = 16
SETTLE = 16


def attend(old_block, lengths, meta, queries, keys, values, other_k, other_v, dk, dv, insts):
    requests, draft, width = queries.shape
    head_dim = keys.shape[2]
    qrows = draft * width // head_dim
    rows = requests // insts
    anyspace = pl.BlockSpec(memory_space=pl.ANY)
    smem = pl.BlockSpec(memory_space=pltpu.SMEM)
    vmem = pl.BlockSpec(memory_space=pltpu.VMEM)
    bf16 = jnp.bfloat16
    state = pltpu.VMEM((requests, qrows, head_dim), jnp.float32)
    return pl.pallas_call(
        attend_body,
        in_specs=[smem] * 3 + [anyspace] * 7,
        out_specs=vmem,
        out_shape=jax.ShapeDtypeStruct((insts, (rows + 1) * qrows, head_dim), bf16),
        scratch_shapes=[pltpu.VMEM(queries.shape, bf16)]
        + [pltpu.VMEM((rows, draft, head_dim), bf16)] * 2
        + [pltpu.VMEM(keys.shape, bf16)] * 4
        + [
            pltpu.VMEM((keys.shape[0], qrows, head_dim), jnp.float32),
            pltpu.VMEM((rows, qrows, head_dim), jnp.float32),
            state,
            state,
            state,
            pltpu.SMEM((TOTAL,), jnp.int32),
            pltpu.SMEM((TOTAL,), jnp.int32),
            pltpu.SemaphoreType.DMA((7,)),
        ],
        name="attend",
    )(old_block, lengths, meta, queries, keys, values, other_k, other_v, dk, dv)


TOTAL = 256


def join_body(got, out):
    insts, _, head_dim = got.shape
    rows = out.shape[1]
    draft = out.shape[2]
    heads = out.shape[3] // head_dim
    qrows = draft * heads
    lane = lax.broadcasted_iota(jnp.int32, (qrows, head_dim), 1)
    stats = [got[s, rows * qrows :, :].astype(jnp.float32) for s in range(insts)]
    for a in range(rows):
        mine = (lane % rows == a) & (lane < 3 * rows)
        level = [
            jnp.sum(jnp.where(mine, stat, 0.0), axis=1, keepdims=True) for stat in stats
        ]
        top = level[0]
        for x in level[1:]:
            top = jnp.maximum(top, x)
        total = jnp.zeros((qrows, 1), jnp.float32)
        acc = jnp.zeros((qrows, head_dim), jnp.float32)
        for s in range(insts):
            share = jnp.exp(level[s] - top)
            total = total + share
            acc = acc + share * got[s, a * qrows : (a + 1) * qrows, :].astype(jnp.float32)
        res = (acc / total).astype(out.dtype)
        for d in range(insts):
            for h in range(heads):
                out[d, a, :, h * head_dim : (h + 1) * head_dim] = res[h * draft : (h + 1) * draft]


def join(got, rows, draft, width):
    insts = got.shape[0]
    vmem = pl.BlockSpec(memory_space=pltpu.VMEM)
    return pl.pallas_call(
        join_body,
        in_specs=[vmem],
        out_specs=vmem,
        out_shape=jax.ShapeDtypeStruct((insts, rows, draft, width), got.dtype),
        name="join",
    )(got)


def spread(x):
    return lax.all_to_all(x, "inst", split_axis=0, concat_axis=0, tiled=True)


def move_and_attend(
    old_keys, old_values, old_block, new_slot, lengths, queries, draft_keys, draft_values
):
    insts = lax.axis_size("inst")
    _, entries, half, head_dim = old_keys.shape
    keys = old_keys.reshape(-1, half, head_dim)
    values = old_values.reshape(-1, half, head_dim)
    blocks = new_slot.shape[0]
    requests = queries.shape[0]
    rows = requests // insts
    swap = [(i, i ^ 1) for i in range(lax.axis_size("head"))]
    other_k = lax.ppermute(keys, "head", swap)
    other_v = lax.ppermute(values, "head", swap)

    table = table_of(blocks // insts, rows, half, head_dim)
    out_k, out_v = pack(old_block, new_slot, table, keys, values, insts, SENT_K, SENT_V)
    queries, out_k, out_v = lax.optimization_barrier((queries, out_k, out_v))
    shape = (blocks // insts, entries, half, head_dim)
    far2 = across(out_v[0])
    from_left = right(out_k[0])
    from_right = left(out_k[1])
    far = across(out_v[1])
    kept_k, kept_v = pack(old_block, new_slot, table, keys, values, insts, KEPT_K, KEPT_V)
    near = across(kept_v[0])
    packet = attend(
        old_block, lengths, table, queries, keys, values, other_k, other_v,
        draft_keys, draft_values, insts,
    )
    packet, rest_k, rest_v = lax.optimization_barrier((packet, kept_k, kept_v[1:]))
    moved_keys = move_keys(from_left, from_right, rest_k).reshape(shape)
    moved_values = move_values(far2, far, near, rest_v).reshape(shape)
    got = spread(packet)
    mine = join(got, rows, queries.shape[1], queries.shape[2])
    attended = spread(mine).reshape(queries.shape)
    return moved_keys, moved_values, attended


def solution(mesh):
    placed = (
        P("inst", "head", None, None),
        P("inst", "head", None, None),
        P("inst"),
        P(),
        P(),
        P(None, None, "head"),
        P("inst", None, None),
        P("inst", None, None),
    )
    return jax.shard_map(
        move_and_attend,
        mesh=mesh,
        in_specs=placed,
        out_specs=(
            P("inst", "head", None, None),
            P("inst", "head", None, None),
            P(None, None, "head"),
        ),
        check_vma=False,
    )
```

```python
import functools
import math

import jax
import jax.numpy as jnp
from jax import lax
from jax.experimental import pallas as pl
from jax.experimental.pallas import tpu as pltpu
from jax.sharding import PartitionSpec as P


BLK = 128
masked = -1e30


COLS = 4
SENT_K = ((4, 3), (5, 6))
SENT_V = ((5,), (3, 7))
KEPT_K = ((2,), (7,), (0,), (1,))
KEPT_V = ((1,), (4,), (2,), (6,), (0,))


def pack_body(groups_k, groups_v, old_block, new_slot, base, keys, values, *rest):
    count = len(groups_k) + len(groups_v)
    outs = rest[:count]
    vk, vv, zeros, origin, sems, load_sem = rest[count:]
    slots = keys.shape[0]
    total = new_slot.shape[0]
    per = zeros.shape[0]
    is_source = old_block[0] >= 0
    jobs = [(vk, out, group) for out, group in zip(outs, groups_k)]
    jobs += [(vv, out, group) for out, group in zip(outs[len(groups_k) :], groups_v)]

    @pl.when(is_source)
    def _():
        load_k = pltpu.make_async_copy(keys, vk, load_sem.at[0])
        load_v = pltpu.make_async_copy(values, vv, load_sem.at[1])
        load_k.start()
        load_v.start()
        zeros[0] = jnp.zeros(zeros.shape[1:], zeros.dtype)

        def clear(t, c):
            origin[t] = -1
            return c

        lax.fori_loop(0, total, clear, 0, unroll=8)

        def note(i, c):
            origin[new_slot[jnp.maximum(old_block[i], 0)]] = i
            return c

        lax.fori_loop(0, slots, note, 0, unroll=8)
        load_k.wait()
        load_v.wait()
        for at, (cache, out, group) in enumerate(jobs):
            for g, p in enumerate(group):
                start = base[p]

                def send(j, c, cache=cache, out=out, at=at, g=g, start=start):
                    i = origin[start + j]

                    @pl.when(i >= 0)
                    def _():
                        pltpu.make_async_copy(cache.at[i], out.at[g * per + j], sems.at[at]).start()

                    @pl.when(i < 0)
                    def _():
                        pltpu.make_async_copy(zeros.at[0], out.at[g * per + j], sems.at[at]).start()

                    return c

                lax.fori_loop(0, per, send, 0, unroll=4)

    @pl.when(jnp.logical_not(is_source))
    def _():
        zeros[...] = jnp.zeros(zeros.shape, zeros.dtype)
        for at, (cache, out, group) in enumerate(jobs):
            for g in range(len(group)):
                pltpu.make_async_copy(zeros, out.at[pl.ds(g * per, per)], sems.at[at]).start()

    for at, (cache, out, group) in enumerate(jobs):
        pltpu.make_async_copy(out, out, sems.at[at]).wait()


def table_of(per, rows, half, head_dim):
    insts = lax.axis_size("inst")
    inst = lax.axis_index("inst")
    me_head = lax.axis_index("head")
    step = jnp.arange(16, dtype=jnp.int32)
    away = (inst // COLS) ^ (step % 2)
    column = (inst % COLS + step // 2) % COLS
    base = (away * COLS + column) * per
    rest = jnp.where(
        step == insts,
        inst * rows,
        jnp.where(step == insts + 1, me_head % 2 * half, me_head // 2 * head_dim),
    )
    return jnp.where(step < insts, base, rest)


def pack(old_block, new_slot, base, keys, values, insts, groups_k, groups_v):
    total = new_slot.shape[0]
    per = total // insts
    groups = groups_k + groups_v
    anyspace = pl.BlockSpec(memory_space=pl.ANY)
    smem = pl.BlockSpec(memory_space=pltpu.SMEM)
    got = pl.pallas_call(
        functools.partial(pack_body, groups_k, groups_v),
        in_specs=[smem, smem, smem, anyspace, anyspace],
        out_specs=[anyspace] * len(groups),
        out_shape=[
            jax.ShapeDtypeStruct((per * len(g),) + keys.shape[1:], keys.dtype) for g in groups
        ],
        scratch_shapes=[
            pltpu.VMEM(keys.shape, keys.dtype),
            pltpu.VMEM(keys.shape, keys.dtype),
            pltpu.VMEM((per,) + keys.shape[1:], keys.dtype),
            pltpu.SMEM((total,), jnp.int32),
            pltpu.SemaphoreType.DMA((len(groups),)),
            pltpu.SemaphoreType.DMA((2,)),
        ],
    )(old_block, new_slot, base, keys, values)
    return got[: len(groups_k)], got[len(groups_k) :]


def right(x):
    rows = lax.axis_size("inst") // COLS
    route = [(r * COLS + c, r * COLS + (c + 1) % COLS) for r in range(rows) for c in range(COLS)]
    return lax.ppermute(x, "inst", route)


def left(x):
    rows = lax.axis_size("inst") // COLS
    route = [(r * COLS + (c + 1) % COLS, r * COLS + c) for r in range(rows) for c in range(COLS)]
    return lax.ppermute(x, "inst", route)


def across(x):
    return lax.ppermute(x, "inst", [(i, i ^ COLS) for i in range(lax.axis_size("inst"))])


def move_keys(from_left, from_right, groups):
    k1n, k3f, k0n, k0f = groups
    per = k1n.shape[0]
    a2 = right(k1n + from_left[:per])
    b2 = left(k3f + from_right[:per])
    b2, from_left = lax.optimization_barrier((b2, from_left))
    crossed = across(k0f + from_left[per:] + b2)
    return k0n + from_right[per:] + a2 + crossed


def move_values(got2, got, y0, groups):
    v2n, v1n, v3n, v0n = groups
    per = v1n.shape[0]
    cut = per // 2
    from_left = right(v2n[:cut] + got2[:cut])
    from_right = left(v2n[cut:] + got2[cut:])
    rest = jnp.zeros((per - cut,) + v1n.shape[1:], v1n.dtype)
    a2 = right(v1n + got[:per] + jnp.concatenate([from_left, rest]))
    b2 = left(v3n + got[per:] + jnp.concatenate([rest, from_right]))
    return v0n + y0 + a2 + b2


def dot_t(x, y):
    return lax.dot_general(x, y, (((1,), (1,)), ((), ())), preferred_element_type=jnp.float32)


def attend_body(
    old_block, lengths, meta, q, k, v, ok, ov, dks, dvs, packet,
    vq, dk, dv, vk, vv, vok, vov, scores, drafted, peak, total, acc, owner, live, sems,
):
    requests, draft, width = vq.shape
    head_dim = vk.shape[2]
    half = vk.shape[1]
    slots = vk.shape[0]
    heads = width // head_dim
    qrows = draft * heads
    insts = packet.shape[0]
    rows = requests // insts
    inv_root = 1.0 / math.sqrt(head_dim)
    is_source = old_block[0] >= 0
    first = meta[insts]
    shift = meta[insts + 1]
    kv = pl.ds(pl.multiple_of(meta[insts + 2], head_dim), head_dim)
    early = [
        pltpu.make_async_copy(q, vq, sems.at[0]),
        pltpu.make_async_copy(dks.at[:, :, kv], dk, sems.at[5]),
        pltpu.make_async_copy(dvs.at[:, :, kv], dv, sems.at[6]),
    ]
    for load in early:
        load.start()
    loads = [
        pltpu.make_async_copy(x, y, sems.at[1 + n])
        for n, (x, y) in enumerate(((k, vk), (ok, vok), (v, vv), (ov, vov)))
    ]

    @pl.when(is_source)
    def _():
        for load in loads:
            load.start()

        def per_request(r, g):
            size = lengths[r]

            def per_block(j, c):
                owner[g + j] = r
                live[g + j] = jnp.minimum(size - j * BLK, BLK)
                return c

            n = (size + BLK - 1) // BLK
            lax.fori_loop(0, n, per_block, 0)
            return g + n

        lax.fori_loop(0, requests, per_request, 0)

    def q_of(r):
        return jnp.concatenate(
            [vq[r, :, h * head_dim : (h + 1) * head_dim] for h in range(heads)], axis=0
        )

    lane = lax.broadcasted_iota(jnp.int32, (qrows, head_dim), 1)
    row = lax.broadcasted_iota(jnp.int32, (qrows, head_dim), 0)
    place = (lane + shift) % (2 * half)
    causal = lane <= row % draft
    blank = jnp.full((qrows, head_dim), masked, jnp.float32)

    def reset(r, c):
        peak[r] = blank
        return c

    lax.fori_loop(0, requests, reset, 0, unroll=4)
    for load in early:
        load.wait()
    pad = jnp.zeros((2 * half - draft, head_dim), dk.dtype)
    for a in range(rows):
        s = dot_t(q_of(first + a), jnp.concatenate([dk[a], pad], axis=0)) * inv_root
        s = jnp.where(causal, s, masked)
        drafted[a] = s
        peak[first + a] = s

    @pl.when(is_source)
    def _():
        loads[0].wait()
        loads[1].wait()

        def score(n, c):
            found = []
            for u in range(UNROLL):
                i = n * UNROLL + u
                g = jnp.maximum(old_block[i], 0)
                r = owner[g]
                key = jnp.concatenate([vk[i], vok[i]], axis=0)
                s = dot_t(q_of(r), key) * inv_root
                found.append((i, r, jnp.where(place < live[g], s, masked)))
            for i, r, s in found:
                scores[i] = s
                peak[r] = jnp.maximum(peak[r], s)
            return c

        lax.fori_loop(0, slots // UNROLL, score, 0)

    def settle(r, c):
        peak[r] = jnp.broadcast_to(jnp.max(peak[r], axis=1, keepdims=True), (qrows, head_dim))
        total[r] = jnp.zeros((qrows, head_dim), jnp.float32)
        acc[r] = jnp.zeros((qrows, head_dim), jnp.float32)
        return c

    lax.fori_loop(0, requests, settle, 0, unroll=SETTLE)
    for a in range(rows):
        w = jnp.exp(drafted[a] - peak[first + a])
        total[first + a] = w
        acc[first + a] = jnp.dot(
            w.astype(dv.dtype),
            jnp.concatenate([dv[a], pad], axis=0),
            preferred_element_type=jnp.float32,
        )

    @pl.when(is_source)
    def _():
        loads[2].wait()
        loads[3].wait()

        def gather(n, c):
            found = []
            for u in range(UNROLL):
                i = n * UNROLL + u
                r = owner[jnp.maximum(old_block[i], 0)]
                w = jnp.exp(scores[i] - peak[r])
                value = jnp.concatenate([vv[i], vov[i]], axis=0)
                out = jnp.dot(w.astype(vv.dtype), value, preferred_element_type=jnp.float32)
                found.append((r, w, out))
            for r, w, out in found:
                total[r] += w
                acc[r] += out
            return c

        lax.fori_loop(0, slots // UNROLL, gather, 0)

    def finish(d, c):
        sums = jnp.zeros((qrows, head_dim), jnp.float32)
        tops = jnp.zeros((qrows, head_dim), jnp.float32)
        for a in range(rows):
            r = d * rows + a
            l = jnp.sum(total[r], axis=1, keepdims=True)
            scale = 1.0 / jnp.where(l > 0, l, 1.0)
            packet[d, a * qrows : (a + 1) * qrows, :] = (acc[r] * scale).astype(packet.dtype)
            sums = jnp.where(lane % rows == a, l, sums)
            tops = jnp.where(lane % rows == a, peak[r], tops)
        level = jnp.where(sums > 0, tops + jnp.log(jnp.where(sums > 0, sums, 1.0)), masked)
        hi = level.astype(jnp.bfloat16).astype(jnp.float32)
        mid = (level - hi).astype(jnp.bfloat16).astype(jnp.float32)
        stat = jnp.where(lane < rows, hi, jnp.where(lane < 2 * rows, mid, level - hi - mid))
        packet[d, rows * qrows :, :] = stat.astype(packet.dtype)
        return c

    lax.fori_loop(0, insts, finish, 0)


UNROLL = 32
SETTLE = 16


def attend(old_block, lengths, meta, queries, keys, values, other_k, other_v, dk, dv, insts):
    requests, draft, width = queries.shape
    head_dim = keys.shape[2]
    qrows = draft * width // head_dim
    rows = requests // insts
    anyspace = pl.BlockSpec(memory_space=pl.ANY)
    smem = pl.BlockSpec(memory_space=pltpu.SMEM)
    vmem = pl.BlockSpec(memory_space=pltpu.VMEM)
    bf16 = jnp.bfloat16
    state = pltpu.VMEM((requests, qrows, head_dim), jnp.float32)
    return pl.pallas_call(
        attend_body,
        in_specs=[smem] * 3 + [anyspace] * 7,
        out_specs=vmem,
        out_shape=jax.ShapeDtypeStruct((insts, (rows + 1) * qrows, head_dim), bf16),
        scratch_shapes=[pltpu.VMEM(queries.shape, bf16)]
        + [pltpu.VMEM((rows, draft, head_dim), bf16)] * 2
        + [pltpu.VMEM(keys.shape, bf16)] * 4
        + [
            pltpu.VMEM((keys.shape[0], qrows, head_dim), jnp.float32),
            pltpu.VMEM((rows, qrows, head_dim), jnp.float32),
            state,
            state,
            state,
            pltpu.SMEM((TOTAL,), jnp.int32),
            pltpu.SMEM((TOTAL,), jnp.int32),
            pltpu.SemaphoreType.DMA((7,)),
        ],
        name="attend",
    )(old_block, lengths, meta, queries, keys, values, other_k, other_v, dk, dv)


TOTAL = 256


def join_body(got, out):
    insts, _, head_dim = got.shape
    rows, draft, width = out.shape
    heads = width // head_dim
    qrows = draft * heads
    lane = lax.broadcasted_iota(jnp.int32, (qrows, head_dim), 1)
    stats = [got[s, rows * qrows :, :].astype(jnp.float32) for s in range(insts)]
    for a in range(rows):
        mine = (lane % rows == a) & (lane < 3 * rows)
        level = [
            jnp.sum(jnp.where(mine, stat, 0.0), axis=1, keepdims=True) for stat in stats
        ]
        top = level[0]
        for x in level[1:]:
            top = jnp.maximum(top, x)
        total = jnp.zeros((qrows, 1), jnp.float32)
        acc = jnp.zeros((qrows, head_dim), jnp.float32)
        for s in range(insts):
            share = jnp.exp(level[s] - top)
            total = total + share
            acc = acc + share * got[s, a * qrows : (a + 1) * qrows, :].astype(jnp.float32)
        res = (acc / total).astype(out.dtype)
        for h in range(heads):
            out[a, :, h * head_dim : (h + 1) * head_dim] = res[h * draft : (h + 1) * draft]


def join(got, rows, draft, width):
    vmem = pl.BlockSpec(memory_space=pltpu.VMEM)
    return pl.pallas_call(
        join_body,
        in_specs=[vmem],
        out_specs=vmem,
        out_shape=jax.ShapeDtypeStruct((rows, draft, width), got.dtype),
        name="join",
    )(got)


def place_body(per, table, pair, east, far_own, far_other, west, out, sems):
    rows = far_own.shape[0]
    pieces = (
        pair.at[:rows], pair.at[rows:], east.at[:rows], east.at[rows:],
        far_own, far_other, west.at[:rows], west.at[rows:],
    )
    copies = [
        pltpu.make_async_copy(
            piece, out.at[pl.ds(table[p] // per * rows, rows)], sems.at[p]
        )
        for p, piece in enumerate(pieces)
    ]
    for copy in copies:
        copy.start()
    for copy in copies:
        copy.wait()


def results(mine, table, per, shape):
    rows = mine.shape[0]
    other = across(mine)
    pair = jnp.concatenate([mine, other])
    west = right(pair)
    east = left(pair)
    far_own = right(west[:rows])
    far_other = left(east[rows:])
    vmem = pl.BlockSpec(memory_space=pltpu.VMEM)
    return pl.pallas_call(
        functools.partial(place_body, per),
        in_specs=[pl.BlockSpec(memory_space=pltpu.SMEM)] + [vmem] * 5,
        out_specs=pl.BlockSpec(memory_space=pl.ANY),
        out_shape=jax.ShapeDtypeStruct(shape, mine.dtype),
        scratch_shapes=[pltpu.SemaphoreType.DMA((8,))],
        name="place",
    )(table, pair, east, far_own, far_other, west)


def spread(x):
    return lax.all_to_all(x, "inst", split_axis=0, concat_axis=0, tiled=True)


def move_and_attend(
    old_keys, old_values, old_block, new_slot, lengths, queries, draft_keys, draft_values
):
    insts = lax.axis_size("inst")
    _, entries, half, head_dim = old_keys.shape
    keys = old_keys.reshape(-1, half, head_dim)
    values = old_values.reshape(-1, half, head_dim)
    blocks = new_slot.shape[0]
    requests = queries.shape[0]
    rows = requests // insts
    swap = [(i, i ^ 1) for i in range(lax.axis_size("head"))]
    other_k = lax.ppermute(keys, "head", swap)
    other_v = lax.ppermute(values, "head", swap)

    table = table_of(blocks // insts, rows, half, head_dim)
    out_k, out_v = pack(
        old_block, new_slot, table, keys, values, insts, SENT_K + KEPT_K, SENT_V + KEPT_V
    )
    queries, out_k, out_v = lax.optimization_barrier((queries, out_k, out_v))
    shape = (blocks // insts, entries, half, head_dim)
    far2 = across(out_v[0])
    from_left = right(out_k[0])
    from_right = left(out_k[1])
    far = across(out_v[1])
    kept_k, kept_v = out_k[len(SENT_K) :], out_v[len(SENT_V) :]
    near = across(kept_v[0])
    packet = attend(
        old_block, lengths, table, queries, keys, values, other_k, other_v,
        draft_keys, draft_values, insts,
    )
    packet, rest_k, rest_v = lax.optimization_barrier((packet, kept_k, kept_v[1:]))
    moved_keys = move_keys(from_left, from_right, rest_k).reshape(shape)
    moved_values = move_values(far2, far, near, rest_v).reshape(shape)
    got = spread(packet)
    mine = join(got, rows, queries.shape[1], queries.shape[2])
    attended = results(mine, table, blocks // insts, queries.shape)
    return moved_keys, moved_values, attended


def solution(mesh):
    placed = (
        P("inst", "head", None, None),
        P("inst", "head", None, None),
        P("inst"),
        P(),
        P(),
        P(None, None, "head"),
        P("inst", None, None),
        P("inst", None, None),
    )
    return jax.shard_map(
        move_and_attend,
        mesh=mesh,
        in_specs=placed,
        out_specs=(
            P("inst", "head", None, None),
            P("inst", "head", None, None),
            P(None, None, "head"),
        ),
        check_vma=False,
    )
```

```python
import functools
import math

import jax
import jax.numpy as jnp
from jax import lax
from jax.experimental import pallas as pl
from jax.experimental.pallas import tpu as pltpu
from jax.sharding import PartitionSpec as P


BLK = 128
masked = -1e30


COLS = 4
SENT_K = ((4, 3), (5, 6))
SENT_V = ((5,), (3, 7))
KEPT_K = ((2,), (7,), (0,), (1,))
KEPT_V = ((1,), (4,), (2,), (6,), (0,))


def pack_body(groups_k, groups_v, old_block, new_slot, base, keys, values, *rest):
    count = len(groups_k) + len(groups_v)
    outs = rest[:count]
    vk, vv, zeros, origin, sems, load_sem = rest[count:]
    slots = keys.shape[0]
    total = new_slot.shape[0]
    per = zeros.shape[0]
    is_source = old_block[0] >= 0
    jobs = [(vk, out, group) for out, group in zip(outs, groups_k)]
    jobs += [(vv, out, group) for out, group in zip(outs[len(groups_k) :], groups_v)]

    @pl.when(is_source)
    def _():
        load_k = pltpu.make_async_copy(keys, vk, load_sem.at[0])
        load_v = pltpu.make_async_copy(values, vv, load_sem.at[1])
        load_k.start()
        load_v.start()
        zeros[0] = jnp.zeros(zeros.shape[1:], zeros.dtype)

        def clear(t, c):
            origin[t] = -1
            return c

        lax.fori_loop(0, total, clear, 0, unroll=8)

        def note(i, c):
            origin[new_slot[jnp.maximum(old_block[i], 0)]] = i
            return c

        lax.fori_loop(0, slots, note, 0, unroll=8)
        load_k.wait()
        load_v.wait()
        for at, (cache, out, group) in enumerate(jobs):
            for g, p in enumerate(group):
                start = base[p]

                def send(j, c, cache=cache, out=out, at=at, g=g, start=start):
                    i = origin[start + j]

                    @pl.when(i >= 0)
                    def _():
                        pltpu.make_async_copy(cache.at[i], out.at[g * per + j], sems.at[at]).start()

                    @pl.when(i < 0)
                    def _():
                        pltpu.make_async_copy(zeros.at[0], out.at[g * per + j], sems.at[at]).start()

                    return c

                lax.fori_loop(0, per, send, 0, unroll=4)

    @pl.when(jnp.logical_not(is_source))
    def _():
        zeros[...] = jnp.zeros(zeros.shape, zeros.dtype)
        for at, (cache, out, group) in enumerate(jobs):
            for g in range(len(group)):
                pltpu.make_async_copy(zeros, out.at[pl.ds(g * per, per)], sems.at[at]).start()

    for at, (cache, out, group) in enumerate(jobs):
        pltpu.make_async_copy(out, out, sems.at[at]).wait()


def table_of(per, rows, half, head_dim):
    insts = lax.axis_size("inst")
    inst = lax.axis_index("inst")
    me_head = lax.axis_index("head")
    step = jnp.arange(16, dtype=jnp.int32)
    away = (inst // COLS) ^ (step % 2)
    column = (inst % COLS + step // 2) % COLS
    base = (away * COLS + column) * per
    rest = jnp.where(
        step == insts,
        inst * rows,
        jnp.where(step == insts + 1, me_head % 2 * half, me_head // 2 * head_dim),
    )
    return jnp.where(step < insts, base, rest)


def pack(old_block, new_slot, base, keys, values, insts, groups_k, groups_v):
    total = new_slot.shape[0]
    per = total // insts
    groups = groups_k + groups_v
    anyspace = pl.BlockSpec(memory_space=pl.ANY)
    smem = pl.BlockSpec(memory_space=pltpu.SMEM)
    got = pl.pallas_call(
        functools.partial(pack_body, groups_k, groups_v),
        in_specs=[smem, smem, smem, anyspace, anyspace],
        out_specs=[anyspace] * len(groups),
        out_shape=[
            jax.ShapeDtypeStruct((per * len(g),) + keys.shape[1:], keys.dtype) for g in groups
        ],
        scratch_shapes=[
            pltpu.VMEM(keys.shape, keys.dtype),
            pltpu.VMEM(keys.shape, keys.dtype),
            pltpu.VMEM((per,) + keys.shape[1:], keys.dtype),
            pltpu.SMEM((total,), jnp.int32),
            pltpu.SemaphoreType.DMA((len(groups),)),
            pltpu.SemaphoreType.DMA((2,)),
        ],
    )(old_block, new_slot, base, keys, values)
    return got[: len(groups_k)], got[len(groups_k) :]


def right(x):
    rows = lax.axis_size("inst") // COLS
    route = [(r * COLS + c, r * COLS + (c + 1) % COLS) for r in range(rows) for c in range(COLS)]
    return lax.ppermute(x, "inst", route)


def left(x):
    rows = lax.axis_size("inst") // COLS
    route = [(r * COLS + (c + 1) % COLS, r * COLS + c) for r in range(rows) for c in range(COLS)]
    return lax.ppermute(x, "inst", route)


def across(x):
    return lax.ppermute(x, "inst", [(i, i ^ COLS) for i in range(lax.axis_size("inst"))])


def move_keys(from_left, from_right, groups):
    k1n, k3f, k0n, k0f = groups
    per = k1n.shape[0]
    a2 = right(k1n + from_left[:per])
    b2 = left(k3f + from_right[:per])
    b2, from_left = lax.optimization_barrier((b2, from_left))
    crossed = across(k0f + from_left[per:] + b2)
    return k0n + from_right[per:] + a2 + crossed


def move_values(got2, got, y0, groups):
    v2n, v1n, v3n, v0n = groups
    per = v1n.shape[0]
    cut = per // 2
    from_left = right(v2n[:cut] + got2[:cut])
    from_right = left(v2n[cut:] + got2[cut:])
    rest = jnp.zeros((per - cut,) + v1n.shape[1:], v1n.dtype)
    a2 = right(v1n + got[:per] + jnp.concatenate([from_left, rest]))
    b2 = left(v3n + got[per:] + jnp.concatenate([rest, from_right]))
    return v0n + y0 + a2 + b2


def dot_t(x, y):
    return lax.dot_general(x, y, (((1,), (1,)), ((), ())), preferred_element_type=jnp.float32)


def attend_body(
    old_block, lengths, meta, q, k, v, ok, ov, dks, dvs, packet,
    vq, dk, dv, vk, vv, vok, vov, scores, drafted, peak, total, acc, owner, live, sems,
):
    requests, draft, width = vq.shape
    head_dim = vk.shape[2]
    half = vk.shape[1]
    slots = vk.shape[0]
    heads = width // head_dim
    qrows = draft * heads
    insts = packet.shape[0]
    rows = requests // insts
    inv_root = 1.0 / math.sqrt(head_dim)
    is_source = old_block[0] >= 0
    first = meta[insts]
    shift = meta[insts + 1]
    kv = pl.ds(pl.multiple_of(meta[insts + 2], head_dim), head_dim)
    early = [
        pltpu.make_async_copy(q, vq, sems.at[0]),
        pltpu.make_async_copy(dks.at[:, :, kv], dk, sems.at[5]),
        pltpu.make_async_copy(dvs.at[:, :, kv], dv, sems.at[6]),
    ]
    for load in early:
        load.start()
    loads = [
        pltpu.make_async_copy(x, y, sems.at[1 + n])
        for n, (x, y) in enumerate(((k, vk), (ok, vok), (v, vv), (ov, vov)))
    ]

    @pl.when(is_source)
    def _():
        for load in loads:
            load.start()

        def per_request(r, g):
            size = lengths[r]

            def per_block(j, c):
                owner[g + j] = r
                live[g + j] = jnp.minimum(size - j * BLK, BLK)
                return c

            n = (size + BLK - 1) // BLK
            lax.fori_loop(0, n, per_block, 0)
            return g + n

        lax.fori_loop(0, requests, per_request, 0)

    def q_of(r):
        return jnp.concatenate(
            [vq[r, :, h * head_dim : (h + 1) * head_dim] for h in range(heads)], axis=0
        )

    lane = lax.broadcasted_iota(jnp.int32, (qrows, head_dim), 1)
    row = lax.broadcasted_iota(jnp.int32, (qrows, head_dim), 0)
    place = (lane + shift) % (2 * half)
    causal = lane <= row % draft
    blank = jnp.full((qrows, head_dim), masked, jnp.float32)

    def reset(r, c):
        peak[r] = blank
        return c

    lax.fori_loop(0, requests, reset, 0, unroll=4)
    for load in early:
        load.wait()
    pad = jnp.zeros((2 * half - draft, head_dim), dk.dtype)
    for a in range(rows):
        s = dot_t(q_of(first + a), jnp.concatenate([dk[a], pad], axis=0)) * inv_root
        s = jnp.where(causal, s, masked)
        drafted[a] = s
        peak[first + a] = s

    @pl.when(is_source)
    def _():
        loads[0].wait()
        loads[1].wait()

        def score(n, c):
            found = []
            for u in range(UNROLL):
                i = n * UNROLL + u
                g = jnp.maximum(old_block[i], 0)
                r = owner[g]
                key = jnp.concatenate([vk[i], vok[i]], axis=0)
                s = dot_t(q_of(r), key) * inv_root
                found.append((i, r, jnp.where(place < live[g], s, masked)))
            for i, r, s in found:
                scores[i] = s
                peak[r] = jnp.maximum(peak[r], s)
            return c

        lax.fori_loop(0, slots // UNROLL, score, 0)

    def settle(r, c):
        peak[r] = jnp.broadcast_to(jnp.max(peak[r], axis=1, keepdims=True), (qrows, head_dim))
        total[r] = jnp.zeros((qrows, head_dim), jnp.float32)
        acc[r] = jnp.zeros((qrows, head_dim), jnp.float32)
        return c

    lax.fori_loop(0, requests, settle, 0, unroll=SETTLE)
    for a in range(rows):
        w = jnp.exp(drafted[a] - peak[first + a])
        total[first + a] = w
        acc[first + a] = jnp.dot(
            w.astype(dv.dtype),
            jnp.concatenate([dv[a], pad], axis=0),
            preferred_element_type=jnp.float32,
        )

    @pl.when(is_source)
    def _():
        loads[2].wait()
        loads[3].wait()

        def gather(n, c):
            found = []
            for u in range(UNROLL):
                i = n * UNROLL + u
                r = owner[jnp.maximum(old_block[i], 0)]
                w = jnp.exp(scores[i] - peak[r])
                value = jnp.concatenate([vv[i], vov[i]], axis=0)
                out = jnp.dot(w.astype(vv.dtype), value, preferred_element_type=jnp.float32)
                found.append((r, w, out))
            for r, w, out in found:
                total[r] += w
                acc[r] += out
            return c

        lax.fori_loop(0, slots // UNROLL, gather, 0)

    def finish(d, c):
        sums = jnp.zeros((qrows, head_dim), jnp.float32)
        tops = jnp.zeros((qrows, head_dim), jnp.float32)
        for a in range(rows):
            r = d * rows + a
            l = jnp.sum(total[r], axis=1, keepdims=True)
            scale = 1.0 / jnp.where(l > 0, l, 1.0)
            packet[d, a * qrows : (a + 1) * qrows, :] = (acc[r] * scale).astype(packet.dtype)
            sums = jnp.where(lane % rows == a, l, sums)
            tops = jnp.where(lane % rows == a, peak[r], tops)
        level = jnp.where(sums > 0, tops + jnp.log(jnp.where(sums > 0, sums, 1.0)), masked)
        hi = level.astype(jnp.bfloat16).astype(jnp.float32)
        mid = (level - hi).astype(jnp.bfloat16).astype(jnp.float32)
        stat = jnp.where(lane < rows, hi, jnp.where(lane < 2 * rows, mid, level - hi - mid))
        packet[d, rows * qrows :, :] = stat.astype(packet.dtype)
        return c

    lax.fori_loop(0, insts, finish, 0)


UNROLL = 32
SETTLE = 16


def attend(old_block, lengths, meta, queries, keys, values, other_k, other_v, dk, dv, insts):
    requests, draft, width = queries.shape
    head_dim = keys.shape[2]
    qrows = draft * width // head_dim
    rows = requests // insts
    anyspace = pl.BlockSpec(memory_space=pl.ANY)
    smem = pl.BlockSpec(memory_space=pltpu.SMEM)
    vmem = pl.BlockSpec(memory_space=pltpu.VMEM)
    bf16 = jnp.bfloat16
    state = pltpu.VMEM((requests, qrows, head_dim), jnp.float32)
    return pl.pallas_call(
        attend_body,
        in_specs=[smem] * 3 + [anyspace] * 7,
        out_specs=vmem,
        out_shape=jax.ShapeDtypeStruct((insts, (rows + 1) * qrows, head_dim), bf16),
        scratch_shapes=[pltpu.VMEM(queries.shape, bf16)]
        + [pltpu.VMEM((rows, draft, head_dim), bf16)] * 2
        + [pltpu.VMEM(keys.shape, bf16)] * 4
        + [
            pltpu.VMEM((keys.shape[0], qrows, head_dim), jnp.float32),
            pltpu.VMEM((rows, qrows, head_dim), jnp.float32),
            state,
            state,
            state,
            pltpu.SMEM((TOTAL,), jnp.int32),
            pltpu.SMEM((TOTAL,), jnp.int32),
            pltpu.SemaphoreType.DMA((7,)),
        ],
        name="attend",
    )(old_block, lengths, meta, queries, keys, values, other_k, other_v, dk, dv)


TOTAL = 256


def join_body(got, out):
    insts, _, head_dim = got.shape
    rows = out.shape[1]
    draft = out.shape[2]
    heads = out.shape[3] // head_dim
    qrows = draft * heads
    lane = lax.broadcasted_iota(jnp.int32, (qrows, head_dim), 1)
    stats = [got[s, rows * qrows :, :].astype(jnp.float32) for s in range(insts)]
    for a in range(rows):
        mine = (lane % rows == a) & (lane < 3 * rows)
        level = [
            jnp.sum(jnp.where(mine, stat, 0.0), axis=1, keepdims=True) for stat in stats
        ]
        top = level[0]
        for x in level[1:]:
            top = jnp.maximum(top, x)
        total = jnp.zeros((qrows, 1), jnp.float32)
        acc = jnp.zeros((qrows, head_dim), jnp.float32)
        for s in range(insts):
            share = jnp.exp(level[s] - top)
            total = total + share
            acc = acc + share * got[s, a * qrows : (a + 1) * qrows, :].astype(jnp.float32)
        res = (acc / total).astype(out.dtype)
        for d in range(insts):
            for h in range(heads):
                out[d, a, :, h * head_dim : (h + 1) * head_dim] = res[h * draft : (h + 1) * draft]


def join(got, rows, draft, width):
    insts = got.shape[0]
    vmem = pl.BlockSpec(memory_space=pltpu.VMEM)
    return pl.pallas_call(
        join_body,
        in_specs=[vmem],
        out_specs=vmem,
        out_shape=jax.ShapeDtypeStruct((insts, rows, draft, width), got.dtype),
        name="join",
    )(got)


def spread(x):
    return lax.all_to_all(x, "inst", split_axis=0, concat_axis=0, tiled=True)


def move_and_attend(
    old_keys, old_values, old_block, new_slot, lengths, queries, draft_keys, draft_values
):
    insts = lax.axis_size("inst")
    _, entries, half, head_dim = old_keys.shape
    keys = old_keys.reshape(-1, half, head_dim)
    values = old_values.reshape(-1, half, head_dim)
    blocks = new_slot.shape[0]
    requests = queries.shape[0]
    rows = requests // insts
    swap = [(i, i ^ 1) for i in range(lax.axis_size("head"))]
    other_k = lax.ppermute(keys, "head", swap)
    other_v = lax.ppermute(values, "head", swap)

    table = table_of(blocks // insts, rows, half, head_dim)
    out_k, out_v = pack(
        old_block, new_slot, table, keys, values, insts, SENT_K + KEPT_K, SENT_V + KEPT_V
    )
    queries, out_k, out_v = lax.optimization_barrier((queries, out_k, out_v))
    shape = (blocks // insts, entries, half, head_dim)
    far2 = across(out_v[0])
    from_left = right(out_k[0])
    from_right = left(out_k[1])
    far = across(out_v[1])
    kept_k, kept_v = out_k[len(SENT_K) :], out_v[len(SENT_V) :]
    near = across(kept_v[0])
    packet = attend(
        old_block, lengths, table, queries, keys, values, other_k, other_v,
        draft_keys, draft_values, insts,
    )
    packet, rest_k, rest_v = lax.optimization_barrier((packet, kept_k, kept_v[1:]))
    moved_keys = move_keys(from_left, from_right, rest_k).reshape(shape)
    moved_values = move_values(far2, far, near, rest_v).reshape(shape)
    got = spread(packet)
    mine = join(got, rows, queries.shape[1], queries.shape[2])
    attended = spread(mine).reshape(queries.shape)
    return moved_keys, moved_values, attended


def solution(mesh):
    placed = (
        P("inst", "head", None, None),
        P("inst", "head", None, None),
        P("inst"),
        P(),
        P(),
        P(None, None, "head"),
        P("inst", None, None),
        P("inst", None, None),
    )
    return jax.shard_map(
        move_and_attend,
        mesh=mesh,
        in_specs=placed,
        out_specs=(
            P("inst", "head", None, None),
            P("inst", "head", None, None),
            P(None, None, "head"),
        ),
        check_vma=False,
    )
```

```python
import functools
import math

import jax
import jax.numpy as jnp
from jax import lax
from jax.experimental import pallas as pl
from jax.experimental.pallas import tpu as pltpu
from jax.sharding import PartitionSpec as P


BLK = 128
masked = -1e30


COLS = 4
SENT_K = ((4, 3), (5, 6))
SENT_V = ((5,), (3,), (7,))
KEPT_K = ((2,), (7,), (0,), (1,))
KEPT_V = ((1,), (4,), (2,), (6,), (0,))


def pack_body(groups_k, groups_v, old_block, new_slot, base, keys, values, *rest):
    count = len(groups_k) + len(groups_v)
    outs = rest[:count]
    vk, vv, zeros, origin, sems, load_sem = rest[count:]
    slots = keys.shape[0]
    total = new_slot.shape[0]
    per = zeros.shape[0]
    is_source = old_block[0] >= 0
    jobs = [(vk, out, group) for out, group in zip(outs, groups_k)]
    jobs += [(vv, out, group) for out, group in zip(outs[len(groups_k) :], groups_v)]
    places = {}
    for at, (cache, out, group) in enumerate(jobs):
        for g, p in enumerate(group):
            places.setdefault(p, []).append((cache, out, at, g * per))

    @pl.when(is_source)
    def _():
        load_k = pltpu.make_async_copy(keys, vk.at[pl.ds(0, slots)], load_sem.at[0])
        load_v = pltpu.make_async_copy(values, vv.at[pl.ds(0, slots)], load_sem.at[1])
        load_k.start()
        load_v.start()
        vk[slots] = jnp.zeros(zeros.shape[1:], zeros.dtype)
        vv[slots] = jnp.zeros(zeros.shape[1:], zeros.dtype)

        def clear(t, c):
            origin[t] = slots
            return c

        lax.fori_loop(0, total, clear, 0, unroll=16)

        def note(i, c):
            origin[new_slot[jnp.maximum(old_block[i], 0)]] = i
            return c

        lax.fori_loop(0, slots, note, 0, unroll=16)
        load_k.wait()
        load_v.wait()
        for p in sorted(places):
            start = base[p]

            def send(j, c, p=p, start=start):
                i = origin[start + j]
                for cache, out, at, first in places[p]:
                    pltpu.make_async_copy(cache.at[i], out.at[first + j], sems.at[at]).start()
                return c

            lax.fori_loop(0, per, send, 0, unroll=8)

    @pl.when(jnp.logical_not(is_source))
    def _():
        zeros[...] = jnp.zeros(zeros.shape, zeros.dtype)
        for at, (cache, out, group) in enumerate(jobs):
            for g in range(len(group)):
                pltpu.make_async_copy(zeros, out.at[pl.ds(g * per, per)], sems.at[at]).start()

    for at, (cache, out, group) in enumerate(jobs):
        pltpu.make_async_copy(out, out, sems.at[at]).wait()


def table_of(per, rows, half, head_dim):
    insts = lax.axis_size("inst")
    inst = lax.axis_index("inst")
    me_head = lax.axis_index("head")
    step = jnp.arange(16, dtype=jnp.int32)
    away = (inst // COLS) ^ (step % 2)
    column = (inst % COLS + step // 2) % COLS
    base = (away * COLS + column) * per
    rest = jnp.where(
        step == insts,
        inst * rows,
        jnp.where(step == insts + 1, me_head % 2 * half, me_head // 2 * head_dim),
    )
    return jnp.where(step < insts, base, rest)


def pack(old_block, new_slot, base, keys, values, insts, groups_k, groups_v):
    total = new_slot.shape[0]
    per = total // insts
    groups = groups_k + groups_v
    anyspace = pl.BlockSpec(memory_space=pl.ANY)
    smem = pl.BlockSpec(memory_space=pltpu.SMEM)
    got = pl.pallas_call(
        functools.partial(pack_body, groups_k, groups_v),
        in_specs=[smem, smem, smem, anyspace, anyspace],
        out_specs=[anyspace] * len(groups),
        out_shape=[
            jax.ShapeDtypeStruct((per * len(g),) + keys.shape[1:], keys.dtype) for g in groups
        ],
        scratch_shapes=[
            pltpu.VMEM((keys.shape[0] + 1,) + keys.shape[1:], keys.dtype),
            pltpu.VMEM((keys.shape[0] + 1,) + keys.shape[1:], keys.dtype),
            pltpu.VMEM((per,) + keys.shape[1:], keys.dtype),
            pltpu.SMEM((total,), jnp.int32),
            pltpu.SemaphoreType.DMA((len(groups),)),
            pltpu.SemaphoreType.DMA((2,)),
        ],
    )(old_block, new_slot, base, keys, values)
    return got[: len(groups_k)], got[len(groups_k) :]


def right(x):
    rows = lax.axis_size("inst") // COLS
    route = [(r * COLS + c, r * COLS + (c + 1) % COLS) for r in range(rows) for c in range(COLS)]
    return lax.ppermute(x, "inst", route)


def left(x):
    rows = lax.axis_size("inst") // COLS
    route = [(r * COLS + (c + 1) % COLS, r * COLS + c) for r in range(rows) for c in range(COLS)]
    return lax.ppermute(x, "inst", route)


def across(x):
    return lax.ppermute(x, "inst", [(i, i ^ COLS) for i in range(lax.axis_size("inst"))])


def move_keys(from_left, from_right, groups):
    k1n, k3f, k0n, k0f = groups
    per = k1n.shape[0]
    a2 = right(k1n + from_left[:per])
    b2 = left(k3f + from_right[:per])
    b2, from_left = lax.optimization_barrier((b2, from_left))
    crossed = across(k0f + from_left[per:] + b2)
    return k0n + from_right[per:] + a2 + crossed


def move_values(got2, got1, got3, y0, groups):
    v2n, v1n, v3n, v0n = groups
    per = v1n.shape[0]
    cut = per // 2
    from_left = right(v2n[:cut] + got2[:cut])
    from_right = left(v2n[cut:] + got2[cut:])
    rest = jnp.zeros((per - cut,) + v1n.shape[1:], v1n.dtype)
    a2 = right(v1n + got1 + jnp.concatenate([from_left, rest]))
    b2 = left(v3n + got3 + jnp.concatenate([rest, from_right]))
    return v0n + y0 + a2 + b2


def dot_t(x, y):
    return lax.dot_general(x, y, (((1,), (1,)), ((), ())), preferred_element_type=jnp.float32)


def attend_body(
    old_block, lengths, meta, q, k, v, ok, ov, dks, dvs, packet,
    vq, dk, dv, vk, vv, vok, vov, scores, drafted, peak, total, acc, owner, live, sems,
):
    requests, draft, width = vq.shape
    head_dim = vk.shape[2]
    half = vk.shape[1]
    slots = vk.shape[0]
    heads = width // head_dim
    qrows = draft * heads
    insts = packet.shape[0]
    rows = requests // insts
    inv_root = 1.0 / math.sqrt(head_dim)
    is_source = old_block[0] >= 0
    first = meta[insts]
    shift = meta[insts + 1]
    kv = pl.ds(pl.multiple_of(meta[insts + 2], head_dim), head_dim)
    early = [
        pltpu.make_async_copy(q, vq, sems.at[0]),
        pltpu.make_async_copy(dks.at[:, :, kv], dk, sems.at[5]),
        pltpu.make_async_copy(dvs.at[:, :, kv], dv, sems.at[6]),
    ]
    for load in early:
        load.start()
    loads = [
        pltpu.make_async_copy(x, y, sems.at[1 + n])
        for n, (x, y) in enumerate(((k, vk), (ok, vok), (v, vv), (ov, vov)))
    ]

    @pl.when(is_source)
    def _():
        for load in loads:
            load.start()

        def per_request(r, g):
            size = lengths[r]

            def per_block(j, c):
                owner[g + j] = r
                live[g + j] = jnp.minimum(size - j * BLK, BLK)
                return c

            n = (size + BLK - 1) // BLK
            lax.fori_loop(0, n, per_block, 0)
            return g + n

        lax.fori_loop(0, requests, per_request, 0)

    def q_of(r):
        return jnp.concatenate(
            [vq[r, :, h * head_dim : (h + 1) * head_dim] for h in range(heads)], axis=0
        )

    lane = lax.broadcasted_iota(jnp.int32, (qrows, head_dim), 1)
    row = lax.broadcasted_iota(jnp.int32, (qrows, head_dim), 0)
    place = (lane + shift) % (2 * half)
    fold = head_dim // heads
    causal = lane <= row % draft
    blank = jnp.full((qrows, head_dim), masked, jnp.float32)

    def reset(r, c):
        peak[r] = blank
        return c

    lax.fori_loop(0, requests, reset, 0, unroll=4)
    for load in early:
        load.wait()
    pad = jnp.zeros((2 * half - draft, head_dim), dk.dtype)
    for a in range(rows):
        s = dot_t(q_of(first + a), jnp.concatenate([dk[a], pad], axis=0)) * inv_root
        s = jnp.where(causal, s, masked)
        drafted[a] = s
        peak[first + a] = s

    @pl.when(is_source)
    def _():
        loads[0].wait()
        loads[1].wait()

        def score(n, c):
            found = []
            for u in range(UNROLL):
                i = n * UNROLL + u
                g = jnp.maximum(old_block[i], 0)
                r = owner[g]
                key = jnp.concatenate([vk[i], vok[i]], axis=0)
                s = dot_t(q_of(r), key) * inv_root
                found.append((i, r, jnp.where(place < live[g], s, masked)))
            for i, r, s in found:
                scores[i] = s
                peak[r] = jnp.maximum(peak[r], s)
            return c

        lax.fori_loop(0, slots // UNROLL, score, 0)

    def settle(r, c):
        peak[r] = jnp.broadcast_to(jnp.max(peak[r], axis=1, keepdims=True), (qrows, head_dim))
        total[r] = jnp.zeros((qrows, head_dim), jnp.float32)
        acc[r] = jnp.zeros((qrows, head_dim), jnp.float32)
        return c

    lax.fori_loop(0, requests, settle, 0, unroll=SETTLE)
    for a in range(rows):
        w = jnp.exp(drafted[a] - peak[first + a])
        total[first + a] = w
        acc[first + a] = jnp.dot(
            w.astype(dv.dtype),
            jnp.concatenate([dv[a], pad], axis=0),
            preferred_element_type=jnp.float32,
        )

    @pl.when(is_source)
    def _():
        loads[2].wait()
        loads[3].wait()

        def gather(n, c):
            found = []
            for u in range(UNROLL):
                i = n * UNROLL + u
                r = owner[jnp.maximum(old_block[i], 0)]
                w = jnp.exp(scores[i] - peak[r])
                value = jnp.concatenate([vv[i], vov[i]], axis=0)
                out = jnp.dot(w.astype(vv.dtype), value, preferred_element_type=jnp.float32)
                found.append((r, w, out))
            for r, w, out in found:
                total[r] += w
                acc[r] += out
            return c

        lax.fori_loop(0, slots // UNROLL, gather, 0)

    def finish(d, c):
        sums = jnp.zeros((qrows, head_dim), jnp.float32)
        tops = jnp.zeros((qrows, head_dim), jnp.float32)
        for a in range(rows):
            r = d * rows + a
            l = jnp.sum(total[r], axis=1, keepdims=True)
            scale = 1.0 / jnp.where(l > 0, l, 1.0)
            packet[d, a * qrows : (a + 1) * qrows, :] = (acc[r] * scale).astype(packet.dtype)
            sums = jnp.where(lane % rows == a, l, sums)
            tops = jnp.where(lane % rows == a, peak[r], tops)
        level = jnp.where(sums > 0, tops + jnp.log(jnp.where(sums > 0, sums, 1.0)), masked)
        hi = level.astype(jnp.bfloat16).astype(jnp.float32)
        mid = (level - hi).astype(jnp.bfloat16).astype(jnp.float32)
        stat = jnp.where(lane < rows, hi, jnp.where(lane < 2 * rows, mid, level - hi - mid))
        stat = jnp.where(lane < 3 * rows, stat, 0.0)
        folded = stat[:draft]
        for h in range(1, heads):
            folded += pltpu.roll(stat[h * draft : (h + 1) * draft], h * fold, 1)
        packet[d, rows * qrows :, :] = folded.astype(packet.dtype)
        return c

    lax.fori_loop(0, insts, finish, 0)


UNROLL = 32
SETTLE = 16


def attend(old_block, lengths, meta, queries, keys, values, other_k, other_v, dk, dv, insts):
    requests, draft, width = queries.shape
    head_dim = keys.shape[2]
    qrows = draft * width // head_dim
    rows = requests // insts
    anyspace = pl.BlockSpec(memory_space=pl.ANY)
    smem = pl.BlockSpec(memory_space=pltpu.SMEM)
    vmem = pl.BlockSpec(memory_space=pltpu.VMEM)
    bf16 = jnp.bfloat16
    state = pltpu.VMEM((requests, qrows, head_dim), jnp.float32)
    return pl.pallas_call(
        attend_body,
        in_specs=[smem] * 3 + [anyspace] * 7,
        out_specs=vmem,
        out_shape=jax.ShapeDtypeStruct((insts, rows * qrows + draft, head_dim), bf16),
        scratch_shapes=[pltpu.VMEM(queries.shape, bf16)]
        + [pltpu.VMEM((rows, draft, head_dim), bf16)] * 2
        + [pltpu.VMEM(keys.shape, bf16)] * 4
        + [
            pltpu.VMEM((keys.shape[0], qrows, head_dim), jnp.float32),
            pltpu.VMEM((rows, qrows, head_dim), jnp.float32),
            state,
            state,
            state,
            pltpu.SMEM((TOTAL,), jnp.int32),
            pltpu.SMEM((TOTAL,), jnp.int32),
            pltpu.SemaphoreType.DMA((7,)),
        ],
        name="attend",
    )(old_block, lengths, meta, queries, keys, values, other_k, other_v, dk, dv)


TOTAL = 256


def join_body(arrived, out, got, sem):
    load = pltpu.make_async_copy(arrived, got, sem)
    load.start()
    insts, _, head_dim = got.shape
    rows = out.shape[1]
    draft = out.shape[2]
    heads = out.shape[3] // head_dim
    qrows = draft * heads
    fold = head_dim // heads
    lane = lax.broadcasted_iota(jnp.int32, (draft, head_dim), 1)
    load.wait()
    stats = [got[s, rows * qrows :, :].astype(jnp.float32) for s in range(insts)]
    for a in range(rows):
        mine = [
            (lane % rows == a) & (lane >= h * fold) & (lane < h * fold + 3 * rows)
            for h in range(heads)
        ]
        level = [
            jnp.concatenate(
                [jnp.sum(jnp.where(m, stat, 0.0), axis=1, keepdims=True) for m in mine], axis=0
            )
            for stat in stats
        ]
        top = level[0]
        for x in level[1:]:
            top = jnp.maximum(top, x)
        total = jnp.zeros((qrows, 1), jnp.float32)
        acc = jnp.zeros((qrows, head_dim), jnp.float32)
        for s in range(insts):
            share = jnp.exp(level[s] - top)
            total = total + share
            acc = acc + share * got[s, a * qrows : (a + 1) * qrows, :].astype(jnp.float32)
        res = (acc / total).astype(out.dtype)
        for d in range(insts):
            for h in range(heads):
                out[d, a, :, h * head_dim : (h + 1) * head_dim] = res[h * draft : (h + 1) * draft]


def join(got, rows, draft, width):
    insts = got.shape[0]
    vmem = pl.BlockSpec(memory_space=pltpu.VMEM)
    return pl.pallas_call(
        join_body,
        in_specs=[pl.BlockSpec(memory_space=pl.ANY)],
        out_specs=vmem,
        out_shape=jax.ShapeDtypeStruct((insts, rows, draft, width), got.dtype),
        scratch_shapes=[pltpu.VMEM(got.shape, got.dtype), pltpu.SemaphoreType.DMA],
        name="join",
    )(got)


def spread(x):
    return lax.all_to_all(x, "inst", split_axis=0, concat_axis=0, tiled=True)


def move_and_attend(
    old_keys, old_values, old_block, new_slot, lengths, queries, draft_keys, draft_values
):
    insts = lax.axis_size("inst")
    _, entries, half, head_dim = old_keys.shape
    keys = old_keys.reshape(-1, half, head_dim)
    values = old_values.reshape(-1, half, head_dim)
    blocks = new_slot.shape[0]
    requests = queries.shape[0]
    rows = requests // insts
    swap = [(i, i ^ 1) for i in range(lax.axis_size("head"))]
    other_k = lax.ppermute(keys, "head", swap)
    other_v = lax.ppermute(values, "head", swap)

    table = table_of(blocks // insts, rows, half, head_dim)
    out_k, out_v = pack(
        old_block, new_slot, table, keys, values, insts, SENT_K + KEPT_K, SENT_V + KEPT_V
    )
    queries, out_k, out_v = lax.optimization_barrier((queries, out_k, out_v))
    shape = (blocks // insts, entries, half, head_dim)
    far2 = across(out_v[0])
    from_left = right(out_k[0])
    from_right = left(out_k[1])
    far1 = across(out_v[1])
    far3 = across(out_v[2])
    kept_k, kept_v = out_k[len(SENT_K) :], out_v[len(SENT_V) :]
    near = across(kept_v[0])
    packet = attend(
        old_block, lengths, table, queries, keys, values, other_k, other_v,
        draft_keys, draft_values, insts,
    )
    packet, rest_k, rest_v = lax.optimization_barrier((packet, kept_k, kept_v[1:]))
    moved_keys = move_keys(from_left, from_right, rest_k).reshape(shape)
    moved_values = move_values(far2, far1, far3, near, rest_v).reshape(shape)
    got = spread(packet)
    mine = join(got, rows, queries.shape[1], queries.shape[2])
    attended = spread(mine).reshape(queries.shape)
    return moved_keys, moved_values, attended


def solution(mesh):
    placed = (
        P("inst", "head", None, None),
        P("inst", "head", None, None),
        P("inst"),
        P(),
        P(),
        P(None, None, "head"),
        P("inst", None, None),
        P("inst", None, None),
    )
    return jax.shard_map(
        move_and_attend,
        mesh=mesh,
        in_specs=placed,
        out_specs=(
            P("inst", "head", None, None),
            P("inst", "head", None, None),
            P(None, None, "head"),
        ),
        check_vma=False,
    )
```

```python
import functools
import math

import jax
import jax.numpy as jnp
from jax import lax
from jax.experimental import pallas as pl
from jax.experimental.pallas import tpu as pltpu
from jax.sharding import PartitionSpec as P


BLK = 128
masked = -1e30


COLS = 4
SENT_K = ((4, 3), (5, 6))
SENT_V = ((5,), (3,), (7,))
KEPT_K = ((2,), (7,), (0,), (1,))
KEPT_V = ((1,), (4,), (2,), (6,), (0,))


def pack_body(groups_k, groups_v, old_block, new_slot, base, keys, values, *rest):
    count = len(groups_k) + len(groups_v)
    outs = rest[:count]
    vk, vv, zeros, origin, sems, load_sem = rest[count:]
    slots = keys.shape[0]
    total = new_slot.shape[0]
    per = zeros.shape[0]
    is_source = old_block[0] >= 0
    jobs = [(vk, out, group) for out, group in zip(outs, groups_k)]
    jobs += [(vv, out, group) for out, group in zip(outs[len(groups_k) :], groups_v)]
    places = {}
    for at, (cache, out, group) in enumerate(jobs):
        for g, p in enumerate(group):
            places.setdefault(p, []).append((cache, out, at, g * per))

    @pl.when(is_source)
    def _():
        load_k = pltpu.make_async_copy(keys, vk.at[pl.ds(0, slots)], load_sem.at[0])
        load_v = pltpu.make_async_copy(values, vv.at[pl.ds(0, slots)], load_sem.at[1])
        load_k.start()
        load_v.start()
        vk[slots] = jnp.zeros(zeros.shape[1:], zeros.dtype)
        vv[slots] = jnp.zeros(zeros.shape[1:], zeros.dtype)

        def clear(t, c):
            origin[t] = slots
            return c

        lax.fori_loop(0, total, clear, 0, unroll=16)

        def note(i, c):
            origin[new_slot[jnp.maximum(old_block[i], 0)]] = i
            return c

        lax.fori_loop(0, slots, note, 0, unroll=16)
        load_k.wait()
        load_v.wait()
        for p in sorted(places):
            start = base[p]

            def send(j, c, p=p, start=start):
                i = origin[start + j]
                for cache, out, at, first in places[p]:
                    pltpu.make_async_copy(cache.at[i], out.at[first + j], sems.at[at]).start()
                return c

            lax.fori_loop(0, per, send, 0, unroll=8)

    @pl.when(jnp.logical_not(is_source))
    def _():
        zeros[...] = jnp.zeros(zeros.shape, zeros.dtype)
        for at, (cache, out, group) in enumerate(jobs):
            for g in range(len(group)):
                pltpu.make_async_copy(zeros, out.at[pl.ds(g * per, per)], sems.at[at]).start()

    for at, (cache, out, group) in enumerate(jobs):
        pltpu.make_async_copy(out, out, sems.at[at]).wait()


def table_of(per, rows, half, head_dim):
    insts = lax.axis_size("inst")
    inst = lax.axis_index("inst")
    me_head = lax.axis_index("head")
    step = jnp.arange(16, dtype=jnp.int32)
    away = (inst // COLS) ^ (step % 2)
    column = (inst % COLS + step // 2) % COLS
    base = (away * COLS + column) * per
    rest = jnp.where(
        step == insts,
        inst * rows,
        jnp.where(step == insts + 1, me_head % 2 * half, me_head // 2 * head_dim),
    )
    return jnp.where(step < insts, base, rest)


def pack(old_block, new_slot, base, keys, values, insts, groups_k, groups_v):
    total = new_slot.shape[0]
    per = total // insts
    groups = groups_k + groups_v
    anyspace = pl.BlockSpec(memory_space=pl.ANY)
    smem = pl.BlockSpec(memory_space=pltpu.SMEM)
    got = pl.pallas_call(
        functools.partial(pack_body, groups_k, groups_v),
        in_specs=[smem, smem, smem, anyspace, anyspace],
        out_specs=[anyspace] * len(groups),
        out_shape=[
            jax.ShapeDtypeStruct((per * len(g),) + keys.shape[1:], keys.dtype) for g in groups
        ],
        scratch_shapes=[
            pltpu.VMEM((keys.shape[0] + 1,) + keys.shape[1:], keys.dtype),
            pltpu.VMEM((keys.shape[0] + 1,) + keys.shape[1:], keys.dtype),
            pltpu.VMEM((per,) + keys.shape[1:], keys.dtype),
            pltpu.SMEM((total,), jnp.int32),
            pltpu.SemaphoreType.DMA((len(groups),)),
            pltpu.SemaphoreType.DMA((2,)),
        ],
    )(old_block, new_slot, base, keys, values)
    return got[: len(groups_k)], got[len(groups_k) :]


def right(x):
    rows = lax.axis_size("inst") // COLS
    route = [(r * COLS + c, r * COLS + (c + 1) % COLS) for r in range(rows) for c in range(COLS)]
    return lax.ppermute(x, "inst", route)


def left(x):
    rows = lax.axis_size("inst") // COLS
    route = [(r * COLS + (c + 1) % COLS, r * COLS + c) for r in range(rows) for c in range(COLS)]
    return lax.ppermute(x, "inst", route)


def across(x):
    return lax.ppermute(x, "inst", [(i, i ^ COLS) for i in range(lax.axis_size("inst"))])


def move_keys(from_left, from_right, groups):
    k1n, k3f, k0n, k0f = groups
    per = k1n.shape[0]
    a2 = right(k1n + from_left[:per])
    b2 = left(k3f + from_right[:per])
    b2, from_left = lax.optimization_barrier((b2, from_left))
    crossed = across(k0f + from_left[per:] + b2)
    return k0n + from_right[per:] + a2 + crossed


def move_values(got2, got1, got3, y0, groups):
    v2n, v1n, v3n, v0n = groups
    per = v1n.shape[0]
    cut = per // 2
    from_left = right(v2n[:cut] + got2[:cut])
    from_right = left(v2n[cut:] + got2[cut:])
    rest = jnp.zeros((per - cut,) + v1n.shape[1:], v1n.dtype)
    a2 = right(v1n + got1 + jnp.concatenate([from_left, rest]))
    b2 = left(v3n + got3 + jnp.concatenate([rest, from_right]))
    return v0n + y0 + a2 + b2


def dot_t(x, y):
    return lax.dot_general(x, y, (((1,), (1,)), ((), ())), preferred_element_type=jnp.float32)


def attend_body(
    old_block, lengths, meta, q, k, v, ok, ov, dks, dvs, packet,
    vq, dk, dv, vk, vv, vok, vov, scores, drafted, peak, total, acc, owner, live, sems,
):
    requests, draft, width = vq.shape
    head_dim = vk.shape[2]
    half = vk.shape[1]
    slots = vk.shape[0]
    heads = width // head_dim
    qrows = draft * heads
    insts = packet.shape[0]
    rows = requests // insts
    inv_root = 1.0 / math.sqrt(head_dim)
    is_source = old_block[0] >= 0
    first = meta[insts]
    shift = meta[insts + 1]
    kv = pl.ds(pl.multiple_of(meta[insts + 2], head_dim), head_dim)
    early = [
        pltpu.make_async_copy(q, vq, sems.at[0]),
        pltpu.make_async_copy(dks.at[:, :, kv], dk, sems.at[5]),
        pltpu.make_async_copy(dvs.at[:, :, kv], dv, sems.at[6]),
    ]
    for load in early:
        load.start()
    loads = [
        pltpu.make_async_copy(x, y, sems.at[1 + n])
        for n, (x, y) in enumerate(((k, vk), (ok, vok), (v, vv), (ov, vov)))
    ]

    @pl.when(is_source)
    def _():
        for load in loads:
            load.start()

        def per_request(r, g):
            size = lengths[r]

            def per_block(j, c):
                owner[g + j] = r
                live[g + j] = jnp.minimum(size - j * BLK, BLK)
                return c

            n = (size + BLK - 1) // BLK
            lax.fori_loop(0, n, per_block, 0)
            return g + n

        lax.fori_loop(0, requests, per_request, 0)

    def q_of(r):
        return jnp.concatenate(
            [vq[r, :, h * head_dim : (h + 1) * head_dim] for h in range(heads)], axis=0
        )

    lane = lax.broadcasted_iota(jnp.int32, (qrows, head_dim), 1)
    row = lax.broadcasted_iota(jnp.int32, (qrows, head_dim), 0)
    place = (lane + shift) % (2 * half)
    fold = head_dim // heads
    causal = lane <= row % draft
    blank = jnp.full((qrows, head_dim), masked, jnp.float32)

    def reset(r, c):
        peak[r] = blank
        return c

    lax.fori_loop(0, requests, reset, 0, unroll=4)
    for load in early:
        load.wait()
    pad = jnp.zeros((2 * half - draft, head_dim), dk.dtype)
    for a in range(rows):
        s = dot_t(q_of(first + a), jnp.concatenate([dk[a], pad], axis=0)) * inv_root
        s = jnp.where(causal, s, masked)
        drafted[a] = s
        peak[first + a] = s

    @pl.when(is_source)
    def _():
        loads[0].wait()
        loads[1].wait()

        def score(n, c):
            found = []
            for u in range(UNROLL):
                i = n * UNROLL + u
                g = jnp.maximum(old_block[i], 0)
                r = owner[g]
                key = jnp.concatenate([vk[i], vok[i]], axis=0)
                s = dot_t(q_of(r), key) * inv_root
                found.append((i, r, jnp.where(place < live[g], s, masked)))
            for i, r, s in found:
                scores[i] = s
                peak[r] = jnp.maximum(peak[r], s)
            return c

        lax.fori_loop(0, slots // UNROLL, score, 0)

    def settle(r, c):
        peak[r] = jnp.broadcast_to(jnp.max(peak[r], axis=1, keepdims=True), (qrows, head_dim))
        total[r] = jnp.zeros((qrows, head_dim), jnp.float32)
        acc[r] = jnp.zeros((qrows, head_dim), jnp.float32)
        return c

    lax.fori_loop(0, requests, settle, 0, unroll=SETTLE)
    for a in range(rows):
        w = jnp.exp(drafted[a] - peak[first + a])
        total[first + a] = w
        acc[first + a] = jnp.dot(
            w.astype(dv.dtype),
            jnp.concatenate([dv[a], pad], axis=0),
            preferred_element_type=jnp.float32,
        )

    @pl.when(is_source)
    def _():
        loads[2].wait()
        loads[3].wait()

        def gather(n, c):
            found = []
            for u in range(UNROLL):
                i = n * UNROLL + u
                r = owner[jnp.maximum(old_block[i], 0)]
                w = jnp.exp(scores[i] - peak[r])
                value = jnp.concatenate([vv[i], vov[i]], axis=0)
                out = jnp.dot(w.astype(vv.dtype), value, preferred_element_type=jnp.float32)
                found.append((r, w, out))
            for r, w, out in found:
                total[r] += w
                acc[r] += out
            return c

        lax.fori_loop(0, slots // UNROLL, gather, 0)

    def finish(d, c):
        sums = jnp.zeros((qrows, head_dim), jnp.float32)
        tops = jnp.zeros((qrows, head_dim), jnp.float32)
        for a in range(rows):
            r = d * rows + a
            l = jnp.sum(total[r], axis=1, keepdims=True)
            scale = 1.0 / jnp.where(l > 0, l, 1.0)
            packet[d, a * qrows : (a + 1) * qrows, :] = (acc[r] * scale).astype(packet.dtype)
            sums = jnp.where(lane % rows == a, l, sums)
            tops = jnp.where(lane % rows == a, peak[r], tops)
        level = jnp.where(sums > 0, tops + jnp.log(jnp.where(sums > 0, sums, 1.0)), masked)
        hi = level.astype(jnp.bfloat16).astype(jnp.float32)
        mid = (level - hi).astype(jnp.bfloat16).astype(jnp.float32)
        stat = jnp.where(lane < rows, hi, jnp.where(lane < 2 * rows, mid, level - hi - mid))
        stat = jnp.where(lane < 3 * rows, stat, 0.0)
        folded = stat[:draft]
        for h in range(1, heads):
            folded += pltpu.roll(stat[h * draft : (h + 1) * draft], h * fold, 1)
        packet[d, rows * qrows :, :] = folded.astype(packet.dtype)
        return c

    lax.fori_loop(0, insts, finish, 0)


UNROLL = 32
SETTLE = 16


def attend(old_block, lengths, meta, queries, keys, values, other_k, other_v, dk, dv, insts):
    requests, draft, width = queries.shape
    head_dim = keys.shape[2]
    qrows = draft * width // head_dim
    rows = requests // insts
    anyspace = pl.BlockSpec(memory_space=pl.ANY)
    smem = pl.BlockSpec(memory_space=pltpu.SMEM)
    vmem = pl.BlockSpec(memory_space=pltpu.VMEM)
    bf16 = jnp.bfloat16
    state = pltpu.VMEM((requests, qrows, head_dim), jnp.float32)
    return pl.pallas_call(
        attend_body,
        in_specs=[smem] * 3 + [anyspace] * 7,
        out_specs=vmem,
        out_shape=jax.ShapeDtypeStruct((insts, rows * qrows + draft, head_dim), bf16),
        scratch_shapes=[pltpu.VMEM(queries.shape, bf16)]
        + [pltpu.VMEM((rows, draft, head_dim), bf16)] * 2
        + [pltpu.VMEM(keys.shape, bf16)] * 4
        + [
            pltpu.VMEM((keys.shape[0], qrows, head_dim), jnp.float32),
            pltpu.VMEM((rows, qrows, head_dim), jnp.float32),
            state,
            state,
            state,
            pltpu.SMEM((TOTAL,), jnp.int32),
            pltpu.SMEM((TOTAL,), jnp.int32),
            pltpu.SemaphoreType.DMA((7,)),
        ],
        name="attend",
    )(old_block, lengths, meta, queries, keys, values, other_k, other_v, dk, dv)


TOTAL = 256


def join_body(arrived, out, got, sem):
    load = pltpu.make_async_copy(arrived, got, sem)
    load.start()
    insts, _, head_dim = got.shape
    rows, draft, width = out.shape
    heads = width // head_dim
    qrows = draft * heads
    fold = head_dim // heads
    lane = lax.broadcasted_iota(jnp.int32, (draft, head_dim), 1)
    load.wait()
    stats = [got[s, rows * qrows :, :].astype(jnp.float32) for s in range(insts)]
    for a in range(rows):
        mine = [
            (lane % rows == a) & (lane >= h * fold) & (lane < h * fold + 3 * rows)
            for h in range(heads)
        ]
        level = [
            jnp.concatenate(
                [jnp.sum(jnp.where(m, stat, 0.0), axis=1, keepdims=True) for m in mine], axis=0
            )
            for stat in stats
        ]
        top = level[0]
        for x in level[1:]:
            top = jnp.maximum(top, x)
        total = jnp.zeros((qrows, 1), jnp.float32)
        acc = jnp.zeros((qrows, head_dim), jnp.float32)
        for s in range(insts):
            share = jnp.exp(level[s] - top)
            total = total + share
            acc = acc + share * got[s, a * qrows : (a + 1) * qrows, :].astype(jnp.float32)
        res = (acc / total).astype(out.dtype)
        for h in range(heads):
            out[a, :, h * head_dim : (h + 1) * head_dim] = res[h * draft : (h + 1) * draft]


def join(got, rows, draft, width):
    vmem = pl.BlockSpec(memory_space=pltpu.VMEM)
    return pl.pallas_call(
        join_body,
        in_specs=[pl.BlockSpec(memory_space=pl.ANY)],
        out_specs=vmem,
        out_shape=jax.ShapeDtypeStruct((rows, draft, width), got.dtype),
        scratch_shapes=[pltpu.VMEM(got.shape, got.dtype), pltpu.SemaphoreType.DMA],
        name="join",
    )(got)


def place_body(per, table, pair, east, far_own, far_other, west, out, sems):
    rows = far_own.shape[0]
    pieces = (
        pair.at[:rows], pair.at[rows:], east.at[:rows], east.at[rows:],
        far_own, far_other, west.at[:rows], west.at[rows:],
    )
    copies = [
        pltpu.make_async_copy(
            piece, out.at[pl.ds(table[p] // per * rows, rows)], sems.at[p]
        )
        for p, piece in enumerate(pieces)
    ]
    for copy in copies:
        copy.start()
    for copy in copies:
        copy.wait()


def results(mine, table, per, shape):
    rows = mine.shape[0]
    other = across(mine)
    pair = jnp.concatenate([mine, other])
    west = right(pair)
    east = left(pair)
    far_own = right(west[:rows])
    far_other = left(east[rows:])
    vmem = pl.BlockSpec(memory_space=pltpu.VMEM)
    return pl.pallas_call(
        functools.partial(place_body, per),
        in_specs=[pl.BlockSpec(memory_space=pltpu.SMEM)] + [vmem] * 5,
        out_specs=pl.BlockSpec(memory_space=pl.ANY),
        out_shape=jax.ShapeDtypeStruct(shape, mine.dtype),
        scratch_shapes=[pltpu.SemaphoreType.DMA((8,))],
        name="place",
    )(table, pair, east, far_own, far_other, west)


def spread(x):
    return lax.all_to_all(x, "inst", split_axis=0, concat_axis=0, tiled=True)


def move_and_attend(
    old_keys, old_values, old_block, new_slot, lengths, queries, draft_keys, draft_values
):
    insts = lax.axis_size("inst")
    _, entries, half, head_dim = old_keys.shape
    keys = old_keys.reshape(-1, half, head_dim)
    values = old_values.reshape(-1, half, head_dim)
    blocks = new_slot.shape[0]
    requests = queries.shape[0]
    rows = requests // insts
    swap = [(i, i ^ 1) for i in range(lax.axis_size("head"))]
    other_k = lax.ppermute(keys, "head", swap)
    other_v = lax.ppermute(values, "head", swap)

    table = table_of(blocks // insts, rows, half, head_dim)
    out_k, out_v = pack(
        old_block, new_slot, table, keys, values, insts, SENT_K + KEPT_K, SENT_V + KEPT_V
    )
    queries, out_k, out_v = lax.optimization_barrier((queries, out_k, out_v))
    shape = (blocks // insts, entries, half, head_dim)
    far2 = across(out_v[0])
    from_left = right(out_k[0])
    from_right = left(out_k[1])
    far1 = across(out_v[1])
    far3 = across(out_v[2])
    kept_k, kept_v = out_k[len(SENT_K) :], out_v[len(SENT_V) :]
    near = across(kept_v[0])
    packet = attend(
        old_block, lengths, table, queries, keys, values, other_k, other_v,
        draft_keys, draft_values, insts,
    )
    packet, rest_k, rest_v = lax.optimization_barrier((packet, kept_k, kept_v[1:]))
    moved_keys = move_keys(from_left, from_right, rest_k).reshape(shape)
    moved_values = move_values(far2, far1, far3, near, rest_v).reshape(shape)
    got = spread(packet)
    mine = join(got, rows, queries.shape[1], queries.shape[2])
    attended = results(mine, table, blocks // insts, queries.shape)
    return moved_keys, moved_values, attended


def solution(mesh):
    placed = (
        P("inst", "head", None, None),
        P("inst", "head", None, None),
        P("inst"),
        P(),
        P(),
        P(None, None, "head"),
        P("inst", None, None),
        P("inst", None, None),
    )
    return jax.shard_map(
        move_and_attend,
        mesh=mesh,
        in_specs=placed,
        out_specs=(
            P("inst", "head", None, None),
            P("inst", "head", None, None),
            P(None, None, "head"),
        ),
        check_vma=False,
    )
```

```python
import functools
import math

import jax
import jax.numpy as jnp
from jax import lax
from jax.experimental import pallas as pl
from jax.experimental.pallas import tpu as pltpu
from jax.sharding import PartitionSpec as P


BLK = 128
masked = -1e30


COLS = 4
SENT_K = ((4, 3), (5, 6))
SENT_V = ((5,), (3, 7))
KEPT_K = ((2,), (7,), (0,), (1,))
KEPT_V = ((1,), (4,), (2,), (6,), (0,))


def pack_body(groups_k, groups_v, old_block, new_slot, base, keys, values, *rest):
    count = len(groups_k) + len(groups_v)
    outs = rest[:count]
    vk, vv, zeros, origin, sems, load_sem = rest[count:]
    slots = keys.shape[0]
    total = new_slot.shape[0]
    per = zeros.shape[0]
    is_source = old_block[0] >= 0
    jobs = [(vk, out, group) for out, group in zip(outs, groups_k)]
    jobs += [(vv, out, group) for out, group in zip(outs[len(groups_k) :], groups_v)]
    places = {}
    for at, (cache, out, group) in enumerate(jobs):
        for g, p in enumerate(group):
            places.setdefault(p, []).append((cache, out, at, g * per))

    @pl.when(is_source)
    def _():
        load_k = pltpu.make_async_copy(keys, vk.at[pl.ds(0, slots)], load_sem.at[0])
        load_v = pltpu.make_async_copy(values, vv.at[pl.ds(0, slots)], load_sem.at[1])
        load_k.start()
        load_v.start()
        vk[slots] = jnp.zeros(zeros.shape[1:], zeros.dtype)
        vv[slots] = jnp.zeros(zeros.shape[1:], zeros.dtype)

        def clear(t, c):
            origin[t] = slots
            return c

        lax.fori_loop(0, total, clear, 0, unroll=16)

        def note(i, c):
            origin[new_slot[jnp.maximum(old_block[i], 0)]] = i
            return c

        lax.fori_loop(0, slots, note, 0, unroll=16)
        load_k.wait()
        load_v.wait()
        for p in sorted(places):
            start = base[p]

            def send(j, c, p=p, start=start):
                i = origin[start + j]
                for cache, out, at, first in places[p]:
                    pltpu.make_async_copy(cache.at[i], out.at[first + j], sems.at[at]).start()
                return c

            lax.fori_loop(0, per, send, 0, unroll=8)

    @pl.when(jnp.logical_not(is_source))
    def _():
        zeros[...] = jnp.zeros(zeros.shape, zeros.dtype)
        for at, (cache, out, group) in enumerate(jobs):
            for g in range(len(group)):
                pltpu.make_async_copy(zeros, out.at[pl.ds(g * per, per)], sems.at[at]).start()

    for at, (cache, out, group) in enumerate(jobs):
        pltpu.make_async_copy(out, out, sems.at[at]).wait()


def table_of(per, rows, half, head_dim):
    insts = lax.axis_size("inst")
    inst = lax.axis_index("inst")
    me_head = lax.axis_index("head")
    step = jnp.arange(16, dtype=jnp.int32)
    away = (inst // COLS) ^ (step % 2)
    column = (inst % COLS + step // 2) % COLS
    base = (away * COLS + column) * per
    rest = jnp.where(
        step == insts,
        inst * rows,
        jnp.where(step == insts + 1, me_head % 2 * half, me_head // 2 * head_dim),
    )
    return jnp.where(step < insts, base, rest)


def pack(old_block, new_slot, base, keys, values, insts, groups_k, groups_v):
    total = new_slot.shape[0]
    per = total // insts
    groups = groups_k + groups_v
    anyspace = pl.BlockSpec(memory_space=pl.ANY)
    smem = pl.BlockSpec(memory_space=pltpu.SMEM)
    got = pl.pallas_call(
        functools.partial(pack_body, groups_k, groups_v),
        in_specs=[smem, smem, smem, anyspace, anyspace],
        out_specs=[anyspace] * len(groups),
        out_shape=[
            jax.ShapeDtypeStruct((per * len(g),) + keys.shape[1:], keys.dtype) for g in groups
        ],
        scratch_shapes=[
            pltpu.VMEM((keys.shape[0] + 1,) + keys.shape[1:], keys.dtype),
            pltpu.VMEM((keys.shape[0] + 1,) + keys.shape[1:], keys.dtype),
            pltpu.VMEM((per,) + keys.shape[1:], keys.dtype),
            pltpu.SMEM((total,), jnp.int32),
            pltpu.SemaphoreType.DMA((len(groups),)),
            pltpu.SemaphoreType.DMA((2,)),
        ],
    )(old_block, new_slot, base, keys, values)
    return got[: len(groups_k)], got[len(groups_k) :]


def right(x):
    rows = lax.axis_size("inst") // COLS
    route = [(r * COLS + c, r * COLS + (c + 1) % COLS) for r in range(rows) for c in range(COLS)]
    return lax.ppermute(x, "inst", route)


def left(x):
    rows = lax.axis_size("inst") // COLS
    route = [(r * COLS + (c + 1) % COLS, r * COLS + c) for r in range(rows) for c in range(COLS)]
    return lax.ppermute(x, "inst", route)


def across(x):
    return lax.ppermute(x, "inst", [(i, i ^ COLS) for i in range(lax.axis_size("inst"))])


def move_keys(from_left, from_right, groups):
    k1n, k3f, k0n, k0f = groups
    per = k1n.shape[0]
    a2 = right(k1n + from_left[:per])
    b2 = left(k3f + from_right[:per])
    b2, from_left = lax.optimization_barrier((b2, from_left))
    crossed = across(k0f + from_left[per:] + b2)
    return k0n + from_right[per:] + a2 + crossed


def move_values(got2, got, y0, groups):
    v2n, v1n, v3n, v0n = groups
    per = v1n.shape[0]
    cut = per // 2
    from_left = right(v2n[:cut] + got2[:cut])
    from_right = left(v2n[cut:] + got2[cut:])
    rest = jnp.zeros((per - cut,) + v1n.shape[1:], v1n.dtype)
    a2 = right(v1n + got[:per] + jnp.concatenate([from_left, rest]))
    b2 = left(v3n + got[per:] + jnp.concatenate([rest, from_right]))
    return v0n + y0 + a2 + b2


def dot_t(x, y):
    return lax.dot_general(x, y, (((1,), (1,)), ((), ())), preferred_element_type=jnp.float32)


def attend_body(
    old_block, lengths, meta, q, k, v, ok, ov, dks, dvs, packet,
    vq, dk, dv, vk, vv, vok, vov, scores, drafted, peak, total, acc, owner, live, sems,
):
    requests, draft, width = vq.shape
    head_dim = vk.shape[2]
    half = vk.shape[1]
    slots = vk.shape[0]
    heads = width // head_dim
    qrows = draft * heads
    insts = packet.shape[0]
    rows = requests // insts
    inv_root = 1.0 / math.sqrt(head_dim)
    is_source = old_block[0] >= 0
    first = meta[insts]
    shift = meta[insts + 1]
    kv = pl.ds(pl.multiple_of(meta[insts + 2], head_dim), head_dim)
    early = [
        pltpu.make_async_copy(q, vq, sems.at[0]),
        pltpu.make_async_copy(dks.at[:, :, kv], dk, sems.at[5]),
        pltpu.make_async_copy(dvs.at[:, :, kv], dv, sems.at[6]),
    ]
    for load in early:
        load.start()
    loads = [
        pltpu.make_async_copy(x, y, sems.at[1 + n])
        for n, (x, y) in enumerate(((k, vk), (ok, vok), (v, vv), (ov, vov)))
    ]

    @pl.when(is_source)
    def _():
        for load in loads:
            load.start()

        def per_request(r, g):
            size = lengths[r]

            def per_block(j, c):
                owner[g + j] = r
                live[g + j] = jnp.minimum(size - j * BLK, BLK)
                return c

            n = (size + BLK - 1) // BLK
            lax.fori_loop(0, n, per_block, 0)
            return g + n

        lax.fori_loop(0, requests, per_request, 0)

    def q_of(r):
        return jnp.concatenate(
            [vq[r, :, h * head_dim : (h + 1) * head_dim] for h in range(heads)], axis=0
        )

    lane = lax.broadcasted_iota(jnp.int32, (qrows, head_dim), 1)
    row = lax.broadcasted_iota(jnp.int32, (qrows, head_dim), 0)
    place = (lane + shift) % (2 * half)
    fold = head_dim // heads
    causal = lane <= row % draft
    blank = jnp.full((qrows, head_dim), masked, jnp.float32)

    def reset(r, c):
        peak[r] = blank
        return c

    lax.fori_loop(0, requests, reset, 0, unroll=4)
    for load in early:
        load.wait()
    pad = jnp.zeros((2 * half - draft, head_dim), dk.dtype)
    for a in range(rows):
        s = dot_t(q_of(first + a), jnp.concatenate([dk[a], pad], axis=0)) * inv_root
        s = jnp.where(causal, s, masked)
        drafted[a] = s
        peak[first + a] = s

    @pl.when(is_source)
    def _():
        loads[0].wait()
        loads[1].wait()

        def score(n, c):
            found = []
            for u in range(UNROLL):
                i = n * UNROLL + u
                g = jnp.maximum(old_block[i], 0)
                r = owner[g]
                key = jnp.concatenate([vk[i], vok[i]], axis=0)
                s = dot_t(q_of(r), key) * inv_root
                found.append((i, r, jnp.where(place < live[g], s, masked)))
            for i, r, s in found:
                scores[i] = s
                peak[r] = jnp.maximum(peak[r], s)
            return c

        lax.fori_loop(0, slots // UNROLL, score, 0)

    def settle(r, c):
        peak[r] = jnp.broadcast_to(jnp.max(peak[r], axis=1, keepdims=True), (qrows, head_dim))
        total[r] = jnp.zeros((qrows, head_dim), jnp.float32)
        acc[r] = jnp.zeros((qrows, head_dim), jnp.float32)
        return c

    lax.fori_loop(0, requests, settle, 0, unroll=SETTLE)
    for a in range(rows):
        w = jnp.exp(drafted[a] - peak[first + a])
        total[first + a] = w
        acc[first + a] = jnp.dot(
            w.astype(dv.dtype),
            jnp.concatenate([dv[a], pad], axis=0),
            preferred_element_type=jnp.float32,
        )

    @pl.when(is_source)
    def _():
        loads[2].wait()
        loads[3].wait()

        def gather(n, c):
            found = []
            for u in range(UNROLL):
                i = n * UNROLL + u
                r = owner[jnp.maximum(old_block[i], 0)]
                w = jnp.exp(scores[i] - peak[r])
                value = jnp.concatenate([vv[i], vov[i]], axis=0)
                out = jnp.dot(w.astype(vv.dtype), value, preferred_element_type=jnp.float32)
                found.append((r, w, out))
            for r, w, out in found:
                total[r] += w
                acc[r] += out
            return c

        lax.fori_loop(0, slots // UNROLL, gather, 0)

    def finish(d, c):
        sums = jnp.zeros((qrows, head_dim), jnp.float32)
        tops = jnp.zeros((qrows, head_dim), jnp.float32)
        for a in range(rows):
            r = d * rows + a
            l = jnp.sum(total[r], axis=1, keepdims=True)
            scale = 1.0 / jnp.where(l > 0, l, 1.0)
            packet[d, a * qrows : (a + 1) * qrows, :] = (acc[r] * scale).astype(packet.dtype)
            sums = jnp.where(lane % rows == a, l, sums)
            tops = jnp.where(lane % rows == a, peak[r], tops)
        level = jnp.where(sums > 0, tops + jnp.log(jnp.where(sums > 0, sums, 1.0)), masked)
        hi = level.astype(jnp.bfloat16).astype(jnp.float32)
        mid = (level - hi).astype(jnp.bfloat16).astype(jnp.float32)
        stat = jnp.where(lane < rows, hi, jnp.where(lane < 2 * rows, mid, level - hi - mid))
        stat = jnp.where(lane < 3 * rows, stat, 0.0)
        folded = stat[:draft]
        for h in range(1, heads):
            folded += pltpu.roll(stat[h * draft : (h + 1) * draft], h * fold, 1)
        packet[d, rows * qrows :, :] = folded.astype(packet.dtype)
        return c

    lax.fori_loop(0, insts, finish, 0)


UNROLL = 32
SETTLE = 16


def attend(old_block, lengths, meta, queries, keys, values, other_k, other_v, dk, dv, insts):
    requests, draft, width = queries.shape
    head_dim = keys.shape[2]
    qrows = draft * width // head_dim
    rows = requests // insts
    anyspace = pl.BlockSpec(memory_space=pl.ANY)
    smem = pl.BlockSpec(memory_space=pltpu.SMEM)
    vmem = pl.BlockSpec(memory_space=pltpu.VMEM)
    bf16 = jnp.bfloat16
    state = pltpu.VMEM((requests, qrows, head_dim), jnp.float32)
    return pl.pallas_call(
        attend_body,
        in_specs=[smem] * 3 + [anyspace] * 7,
        out_specs=vmem,
        out_shape=jax.ShapeDtypeStruct((insts, rows * qrows + draft, head_dim), bf16),
        scratch_shapes=[pltpu.VMEM(queries.shape, bf16)]
        + [pltpu.VMEM((rows, draft, head_dim), bf16)] * 2
        + [pltpu.VMEM(keys.shape, bf16)] * 4
        + [
            pltpu.VMEM((keys.shape[0], qrows, head_dim), jnp.float32),
            pltpu.VMEM((rows, qrows, head_dim), jnp.float32),
            state,
            state,
            state,
            pltpu.SMEM((TOTAL,), jnp.int32),
            pltpu.SMEM((TOTAL,), jnp.int32),
            pltpu.SemaphoreType.DMA((7,)),
        ],
        name="attend",
    )(old_block, lengths, meta, queries, keys, values, other_k, other_v, dk, dv)


TOTAL = 256


def join_body(arrived, out, got, sem):
    load = pltpu.make_async_copy(arrived, got, sem)
    load.start()
    insts, _, head_dim = got.shape
    rows = out.shape[1]
    draft = out.shape[2]
    heads = out.shape[3] // head_dim
    qrows = draft * heads
    fold = head_dim // heads
    lane = lax.broadcasted_iota(jnp.int32, (draft, head_dim), 1)
    load.wait()
    stats = [got[s, rows * qrows :, :].astype(jnp.float32) for s in range(insts)]
    for a in range(rows):
        mine = [
            (lane % rows == a) & (lane >= h * fold) & (lane < h * fold + 3 * rows)
            for h in range(heads)
        ]
        level = [
            jnp.concatenate(
                [jnp.sum(jnp.where(m, stat, 0.0), axis=1, keepdims=True) for m in mine], axis=0
            )
            for stat in stats
        ]
        top = level[0]
        for x in level[1:]:
            top = jnp.maximum(top, x)
        total = jnp.zeros((qrows, 1), jnp.float32)
        acc = jnp.zeros((qrows, head_dim), jnp.float32)
        for s in range(insts):
            share = jnp.exp(level[s] - top)
            total = total + share
            acc = acc + share * got[s, a * qrows : (a + 1) * qrows, :].astype(jnp.float32)
        res = (acc / total).astype(out.dtype)
        for d in range(insts):
            for h in range(heads):
                out[d, a, :, h * head_dim : (h + 1) * head_dim] = res[h * draft : (h + 1) * draft]


def join(got, rows, draft, width):
    insts = got.shape[0]
    vmem = pl.BlockSpec(memory_space=pltpu.VMEM)
    return pl.pallas_call(
        join_body,
        in_specs=[pl.BlockSpec(memory_space=pl.ANY)],
        out_specs=vmem,
        out_shape=jax.ShapeDtypeStruct((insts, rows, draft, width), got.dtype),
        scratch_shapes=[pltpu.VMEM(got.shape, got.dtype), pltpu.SemaphoreType.DMA],
        name="join",
    )(got)


def spread(x):
    return lax.all_to_all(x, "inst", split_axis=0, concat_axis=0, tiled=True)


def move_and_attend(
    old_keys, old_values, old_block, new_slot, lengths, queries, draft_keys, draft_values
):
    insts = lax.axis_size("inst")
    _, entries, half, head_dim = old_keys.shape
    keys = old_keys.reshape(-1, half, head_dim)
    values = old_values.reshape(-1, half, head_dim)
    blocks = new_slot.shape[0]
    requests = queries.shape[0]
    rows = requests // insts
    swap = [(i, i ^ 1) for i in range(lax.axis_size("head"))]
    other_k = lax.ppermute(keys, "head", swap)
    other_v = lax.ppermute(values, "head", swap)

    table = table_of(blocks // insts, rows, half, head_dim)
    out_k, out_v = pack(
        old_block, new_slot, table, keys, values, insts, SENT_K + KEPT_K, SENT_V + KEPT_V
    )
    queries, out_k, out_v = lax.optimization_barrier((queries, out_k, out_v))
    shape = (blocks // insts, entries, half, head_dim)
    far2 = across(out_v[0])
    from_left = right(out_k[0])
    from_right = left(out_k[1])
    far = across(out_v[1])
    kept_k, kept_v = out_k[len(SENT_K) :], out_v[len(SENT_V) :]
    near = across(kept_v[0])
    packet = attend(
        old_block, lengths, table, queries, keys, values, other_k, other_v,
        draft_keys, draft_values, insts,
    )
    packet, rest_k, rest_v = lax.optimization_barrier((packet, kept_k, kept_v[1:]))
    moved_keys = move_keys(from_left, from_right, rest_k).reshape(shape)
    moved_values = move_values(far2, far, near, rest_v).reshape(shape)
    got = spread(packet)
    mine = join(got, rows, queries.shape[1], queries.shape[2])
    attended = spread(mine).reshape(queries.shape)
    return moved_keys, moved_values, attended


def solution(mesh):
    placed = (
        P("inst", "head", None, None),
        P("inst", "head", None, None),
        P("inst"),
        P(),
        P(),
        P(None, None, "head"),
        P("inst", None, None),
        P("inst", None, None),
    )
    return jax.shard_map(
        move_and_attend,
        mesh=mesh,
        in_specs=placed,
        out_specs=(
            P("inst", "head", None, None),
            P("inst", "head", None, None),
            P(None, None, "head"),
        ),
        check_vma=False,
    )
```
